128 devices in a mesh: dp: 1, cp: 128 (over z, y, x, core).
Axes of the slice: x: 4, y: 4, z: 4, core: 2. Of those that a mesh axis runs over, the one named last changes fastest.
Arguments:
- x_in: bfloat16 [24576, 1536], P(('dp', 'cp'))
- dy_in: bfloat16 [24576, 1536], P(('dp', 'cp'))
- doc_id: int32 [24576], P(('dp', 'cp'))
- w_q: bfloat16 [1536, 6, 128], replicated
- w_k: bfloat16 [1536, 1, 128], replicated
- w_v: bfloat16 [1536, 1, 128], replicated
- w_o: bfloat16 [6, 128, 1536], replicated
Outputs:
- output 1: bfloat16 [24576, 1536], P(('dp', 'cp'))
- output 2: bfloat16 [24576, 1536], P(('dp', 'cp'))
All inputs are finite; a program needn't handle non-finite values.
Results may differ from the reference program's by a relative error of at most 0.0094371.
Values are sent between devices in bfloat16 or wider.
A program may use at most 1 GiB of HBM per device.

```python
import jax
import jax.numpy as jnp
from jax import lax

D_MODEL = 1536
Q_HEADS = 6
KV_HEADS = 1
HEAD_DIM = 128
TOK_DEV = 192
GROUP_DEVS = 128
SEQ_LEN = GROUP_DEVS * TOK_DEV
PIECE_LEN = TOK_DEV // 2
QUERY_GROUP = Q_HEADS // KV_HEADS
DOC_CUTS = max(1, GROUP_DEVS // 2)
NEG_BIG = -1.0e30


def stored_positions():
    row_idx = jnp.arange(SEQ_LEN, dtype=jnp.int32)
    owner_dev = row_idx // TOK_DEV
    offset = row_idx % TOK_DEV
    piece_idx = jnp.where(offset < PIECE_LEN, owner_dev, 2 * GROUP_DEVS - 1 - owner_dev)
    return piece_idx * PIECE_LEN + offset % PIECE_LEN


def setup_inputs(seed: int = 0, part: int = 0) -> dict:
    part_key = jax.random.fold_in(jax.random.key(seed), part)
    key_x, key_dy, key_doc = jax.random.split(part_key, 3)
    key_q, key_k, key_v, key_o = jax.random.split(jax.random.key(seed + 1), 4)
    in_scale = D_MODEL ** -0.5
    out_scale = (Q_HEADS * HEAD_DIM) ** -0.5
    x_in = jax.random.normal(key_x, (SEQ_LEN, D_MODEL), jnp.float32).astype(jnp.bfloat16)
    dy_in = jax.random.normal(key_dy, (SEQ_LEN, D_MODEL), jnp.float32).astype(jnp.bfloat16)
    cut_pos = jax.random.randint(key_doc, (DOC_CUTS,), 1, SEQ_LEN, dtype=jnp.int32)
    doc_id = jnp.sum((stored_positions()[:, None] >= cut_pos[None, :]).astype(jnp.int32), axis=1)
    w_q = (jax.random.normal(key_q, (D_MODEL, Q_HEADS, HEAD_DIM), jnp.float32) * in_scale).astype(jnp.bfloat16)
    w_k = (jax.random.normal(key_k, (D_MODEL, KV_HEADS, HEAD_DIM), jnp.float32) * in_scale).astype(jnp.bfloat16)
    w_v = (jax.random.normal(key_v, (D_MODEL, KV_HEADS, HEAD_DIM), jnp.float32) * in_scale).astype(jnp.bfloat16)
    w_o = (jax.random.normal(key_o, (Q_HEADS, HEAD_DIM, D_MODEL), jnp.float32) * out_scale).astype(jnp.bfloat16)
    return {'x_in': x_in, 'dy_in': dy_in, 'doc_id': doc_id, 'w_q': w_q, 'w_k': w_k, 'w_v': w_v, 'w_o': w_o}


def reference(x_in, dy_in, doc_id, w_q, w_k, w_v, w_o):
    score_scale = HEAD_DIM ** -0.5
    all_pos = stored_positions()
    wq_flat = w_q.reshape(D_MODEL, Q_HEADS * HEAD_DIM)
    wk_flat = w_k.reshape(D_MODEL, KV_HEADS * HEAD_DIM)
    wv_flat = w_v.reshape(D_MODEL, KV_HEADS * HEAD_DIM)
    wo_flat = w_o.reshape(Q_HEADS * HEAD_DIM, D_MODEL)
    q_all = jnp.dot(x_in, wq_flat, preferred_element_type=jnp.float32).astype(jnp.bfloat16)
    q_all = q_all.reshape(SEQ_LEN, KV_HEADS, QUERY_GROUP, HEAD_DIM)
    k_all = jnp.dot(x_in, wk_flat, preferred_element_type=jnp.float32).astype(jnp.bfloat16)
    v_all = jnp.dot(x_in, wv_flat, preferred_element_type=jnp.float32).astype(jnp.bfloat16)
    k_wide = k_all.reshape(SEQ_LEN, KV_HEADS, HEAD_DIM).astype(jnp.float32)
    v_wide = v_all.reshape(SEQ_LEN, KV_HEADS, HEAD_DIM).astype(jnp.float32)
    do_all = jnp.dot(dy_in, wo_flat.T, preferred_element_type=jnp.float32).astype(jnp.bfloat16)
    do_all = do_all.reshape(SEQ_LEN, KV_HEADS, QUERY_GROUP, HEAD_DIM)

    def block_step(grad_acc, block_idx):
        dk_acc, dv_acc = grad_acc
        row_start = block_idx * TOK_DEV
        q_blk = lax.dynamic_slice_in_dim(q_all, row_start, TOK_DEV, 0).astype(jnp.float32)
        do_blk = lax.dynamic_slice_in_dim(do_all, row_start, TOK_DEV, 0).astype(jnp.float32)
        pos_blk = lax.dynamic_slice_in_dim(all_pos, row_start, TOK_DEV, 0)
        doc_blk = lax.dynamic_slice_in_dim(doc_id, row_start, TOK_DEV, 0)
        visible = (all_pos[None, :] <= pos_blk[:, None]) & (doc_id[None, :] == doc_blk[:, None])
        scores = jnp.einsum('tkge,ske->tkgs', q_blk, k_wide) * score_scale
        scores = jnp.where(visible[:, None, None, :], scores, NEG_BIG)
        log_norm = jax.nn.logsumexp(scores, axis=-1, keepdims=True)
        prob_blk = jnp.exp(scores - log_norm).astype(jnp.bfloat16).astype(jnp.float32)
        out_blk = jnp.einsum('tkgs,ske->tkge', prob_blk, v_wide).astype(jnp.bfloat16).astype(jnp.float32)
        delta_row = jnp.sum(do_blk * out_blk, axis=-1, keepdims=True)
        d_prob = jnp.einsum('tkge,ske->tkgs', do_blk, v_wide)
        d_score = (prob_blk * (d_prob - delta_row)).astype(jnp.bfloat16).astype(jnp.float32)
        dq_blk = (jnp.einsum('tkgs,ske->tkge', d_score, k_wide) * score_scale).astype(jnp.bfloat16)
        dk_acc = dk_acc + jnp.einsum('tkgs,tkge->ske', d_score, q_blk) * score_scale
        dv_acc = dv_acc + jnp.einsum('tkgs,tkge->ske', prob_blk, do_blk)
        return (dk_acc, dv_acc), (out_blk.astype(jnp.bfloat16), dq_blk)

    zero_grad = jnp.zeros((SEQ_LEN, KV_HEADS, HEAD_DIM), jnp.float32)
    grad_sums, block_outs = lax.scan(block_step, (zero_grad, zero_grad), jnp.arange(GROUP_DEVS))
    dk_sum, dv_sum = grad_sums
    out_blocks, dq_blocks = block_outs
    out_all = out_blocks.reshape(SEQ_LEN, Q_HEADS * HEAD_DIM)
    dq_all = dq_blocks.reshape(SEQ_LEN, Q_HEADS * HEAD_DIM)
    y_out = jnp.dot(out_all, wo_flat, preferred_element_type=jnp.float32).astype(jnp.bfloat16)
    dk_bf = dk_sum.astype(jnp.bfloat16).reshape(SEQ_LEN, KV_HEADS * HEAD_DIM)
    dv_bf = dv_sum.astype(jnp.bfloat16).reshape(SEQ_LEN, KV_HEADS * HEAD_DIM)
    dx_wide = (jnp.dot(dq_all, wq_flat.T, preferred_element_type=jnp.float32)
               + jnp.dot(dk_bf, wk_flat.T, preferred_element_type=jnp.float32)
               + jnp.dot(dv_bf, wv_flat.T, preferred_element_type=jnp.float32))
    dx_out = dx_wide.astype(jnp.bfloat16)
    return y_out, dx_out
```

```python
import functools

import jax
import jax.numpy as jnp
from jax import lax
from jax.experimental import pallas as pl
from jax.experimental.pallas import tpu as pltpu
from jax.sharding import PartitionSpec as P

NEG_BIG = -1.0e30
MESH = pl.DeviceIdType.MESH
NEAR, FAR = 12, 24
F32, BF16 = jnp.float32, jnp.bfloat16
HBM = pl.BlockSpec(memory_space=pl.ANY)
VMEM = pl.BlockSpec(memory_space=pltpu.VMEM)
SMEM = pl.BlockSpec(memory_space=pltpu.SMEM)
VMEM_LIMIT = 60 * 1024 * 1024


def dot(a, b):
    return jnp.dot(a, b, preferred_element_type=F32)


def dot_nt(a, b):
    return lax.dot_general(a, b, (((1,), (1,)), ((), ())), preferred_element_type=F32)


def dot_tn(a, b):
    return lax.dot_general(a, b, (((0,), (0,)), ((), ())), preferred_element_type=F32)


def block_of(dev, n):
    return jnp.where(dev % 2 == 0, dev // 2, n - 1 - dev // 2)


def dev_of(blk, n):
    return jnp.where(blk < n // 2, 2 * blk, 2 * (n - 1 - blk) + 1)


def at(dev):
    return (lax.axis_index('dp'), dev)


def stages_of(n):
    out, stride = [(1, min(n, 8))], min(n, 8)
    while stride < n:
        size = min(4, n // stride)
        out.append((stride, size))
        stride *= size
    return out


def peer_of(me, stride, size, j):
    idx = (me // stride) % size
    return me - idx * stride + ((idx + j) % size) * stride


def remote(src, dst, send, recv, dev):
    return pltpu.make_async_remote_copy(src_ref=src, dst_ref=dst, send_sem=send, recv_sem=recv,
                                        device_id=at(dev), device_id_type=MESH)


def window_signal(barrier, blk, n, near):
    for d in range(1, near + 1):
        @pl.when(blk + d < n)
        def _():
            pl.semaphore_signal(barrier, inc=1, device_id=at(dev_of(blk + d, n)), device_id_type=MESH)

        @pl.when(blk - d >= 0)
        def _():
            pl.semaphore_signal(barrier, inc=1, device_id=at(dev_of(blk - d, n)), device_id_type=MESH)


def window_size(blk, n, near):
    return jnp.minimum(n - 1 - blk, near) + jnp.minimum(blk, near)


def project_kernel(n, near, x_ref, dy_ref, cnt_ref, wq_ref, wk_ref, wv_ref, wo_ref,
                   q_ref, do_ref, kvw_ref, tab_ref,
                   xs, dys, wq, wk, wv, wo, kv, loc_sem, swap_send, swap_recv, win_send, win_recv, tab_send, tab_recv):
    me = lax.axis_index('cp')
    core = me % 2
    partner = me + 1 - 2 * core
    blk = block_of(me, n)
    tok = x_ref.shape[0]
    half = tok // 2
    heads = wq_ref.shape[0]
    hd = wq_ref.shape[2]
    keep = pl.ds(pl.multiple_of(core * half, half), half)
    give = pl.ds(pl.multiple_of((1 - core) * half, half), half)
    loads = [pltpu.make_async_copy(src, dst, loc_sem.at[i]) for i, (src, dst) in enumerate((
        (x_ref.at[keep], xs.at[pl.ds(0, half)]), (wk_ref, wk), (wv_ref, wv), (wq_ref, wq),
        (dy_ref.at[keep], dys.at[pl.ds(0, half)]), (wo_ref, wo)))]
    for c in loads:
        c.start()
    barrier = pltpu.get_barrier_semaphore()
    stages = stages_of(n)
    peers = 0
    for stride, size in stages:
        for j in range(1, size):
            pl.semaphore_signal(barrier, inc=1, device_id=at(peer_of(me, stride, size, j)), device_id_type=MESH)
            peers += 1
    window_signal(barrier, blk, n, near)
    tab_ref[me] = cnt_ref[0]
    pl.semaphore_wait(barrier, peers + window_size(blk, n, near))

    swap_x = remote(x_ref.at[give], xs.at[pl.ds(half, half)], swap_send.at[0], swap_recv.at[0], partner)
    swap_dy = remote(dy_ref.at[give], dys.at[pl.ds(half, half)], swap_send.at[1], swap_recv.at[1], partner)
    swap_x.start()
    swap_dy.start()

    def stage_copies(s):
        stride, size = stages[s]
        rows = pl.ds(me - me % stride, stride)
        src = cnt_ref if s == 0 else tab_ref.at[rows]
        return [remote(src, tab_ref.at[rows], tab_send.at[8 * s + j], tab_recv.at[8 * s + j],
                       peer_of(me, stride, size, j)) for j in range(1, size)]

    tables = [stage_copies(s) for s in range(len(stages))]
    for c in tables[0]:
        c.start()
    for c in loads[:3]:
        c.wait()
    swap_x.wait_recv()
    kv[:, :hd] = dot(xs[...], wk[...]).astype(BF16)
    kv[:, hd:] = dot(xs[...], wv[...]).astype(BF16)
    loads[3].wait()

    def q_head(h):
        q_ref[pl.ds(h * tok, tok), :] = dot(xs[...], wq[h]).astype(BF16)

    q_head(0)
    q_head(1)
    own = pltpu.make_async_copy(kv, kvw_ref.at[pl.ds(0, tok)], loc_sem.at[6])
    own.start()
    sends = [remote(kv, kvw_ref.at[pl.ds(d * tok, tok)], win_send.at[d - 1], win_recv.at[d - 1],
                    dev_of(jnp.minimum(blk + d, n - 1), n)) for d in range(1, near + 1)]
    for d in range(1, near + 1):
        @pl.when(blk + d < n)
        def _():
            sends[d - 1].start()
    for s in range(1, len(stages)):
        for c in tables[s - 1]:
            c.wait()
        for c in tables[s]:
            c.start()
        for h in range(2 * s, min(2 * s + 2, heads)):
            q_head(h)
    for h in range(2 * len(stages), heads):
        q_head(h)
    loads[4].wait()
    loads[5].wait()
    swap_dy.wait_recv()
    for h in range(heads):
        do_ref[pl.ds(h * tok, tok), :] = dot_nt(dys[...], wo[pl.ds(h * hd, hd), :]).astype(BF16)
    for c in tables[-1]:
        c.wait()
    swap_x.wait_send()
    swap_dy.wait_send()
    own.wait()
    for d in range(1, near + 1):
        @pl.when(blk - d >= 0)
        def _():
            sends[d - 1].wait_recv()

        @pl.when(blk + d < n)
        def _():
            sends[d - 1].wait_send()


def gather_kernel(n, near, kvb_ref, kvw_ref, win_send, win_recv, loc_sem):
    me = lax.axis_index('cp')
    blk = block_of(me, n)
    tok = kvb_ref.shape[0]
    barrier = pltpu.get_barrier_semaphore()
    window_signal(barrier, blk, n, near)
    pl.semaphore_wait(barrier, window_size(blk, n, near))
    own = pltpu.make_async_copy(kvb_ref, kvw_ref.at[pl.ds(0, tok)], loc_sem.at[0])
    own.start()
    sends = [remote(kvb_ref, kvw_ref.at[pl.ds(d * tok, tok)], win_send.at[d - 1], win_recv.at[d - 1],
                    dev_of(jnp.minimum(blk + d, n - 1), n)) for d in range(1, near + 1)]
    for d in range(1, near + 1):
        @pl.when(blk + d < n)
        def _():
            sends[d - 1].start()
    own.wait()
    for d in range(1, near + 1):
        @pl.when(blk - d >= 0)
        def _():
            sends[d - 1].wait_recv()

        @pl.when(blk + d < n)
        def _():
            sends[d - 1].wait_send()


def attend_kernel(slots, tok, chunk, keep, nd_ref, start_ref, q_ref, do_ref, kv_ref, o_ref, dq_ref, dkv_ref,
                  q_t, do_t, o_t, dq_t, top, tot, delta, *saved):
    nd = nd_ref[0]
    cols = q_ref.shape[0]
    hd = q_ref.shape[1]
    scale = hd ** -0.5
    q_t[...] = q_ref[...].T
    do_t[...] = do_ref[...].T
    parts = [pl.ds(c * chunk, chunk) for c in range(cols // chunk)]

    def rows(d):
        return pl.ds(pl.multiple_of(d * tok, tok), tok)

    def scores(d, part, c):
        s = dot(kv_ref[rows(d), :hd], q_t[:, part]) * scale
        u = lax.broadcasted_iota(jnp.int32, (tok, chunk), 0) - d * tok
        t = (lax.broadcasted_iota(jnp.int32, (1, chunk), 1) + c * chunk) % tok
        return jnp.where((u >= start_ref[:, part]) & (u <= t), s, NEG_BIG)

    top[...] = jnp.full_like(top, NEG_BIG)
    tot[...] = jnp.zeros_like(tot)
    o_t[...] = jnp.zeros_like(o_t)
    dq_t[...] = jnp.zeros_like(dq_t)

    def find_top(d, _):
        for c, part in enumerate(parts):
            s = scores(d, part, c)
            if keep:
                saved[0][rows(d), part] = s
            top[:, part] = jnp.maximum(top[:, part], jnp.max(s, axis=0, keepdims=True))
        return 0

    def find_total(d, _):
        for c, part in enumerate(parts):
            s = saved[0][rows(d), part] if keep else scores(d, part, c)
            e = jnp.exp(s - top[:, part])
            if keep:
                saved[0][rows(d), part] = e
            tot[:, part] = tot[:, part] + jnp.sum(e, axis=0, keepdims=True)
        return 0

    def prob(d, part, c):
        e = saved[0][rows(d), part] if keep else jnp.exp(scores(d, part, c) - top[:, part])
        return (e * tot[:, part]).astype(BF16)

    def forward(d, _):
        for c, part in enumerate(parts):
            p = prob(d, part, c)
            if keep:
                saved[1][rows(d), part] = p
            o_t[:, part] += dot_tn(kv_ref[rows(d), hd:], p)
        return 0

    def backward(d, _):
        dk = jnp.zeros((tok, hd), F32)
        dv = jnp.zeros((tok, hd), F32)
        for c, part in enumerate(parts):
            p = saved[1][rows(d), part] if keep else prob(d, part, c)
            dp = dot(kv_ref[rows(d), hd:], do_t[:, part])
            ds = (p.astype(F32) * (dp - delta[:, part])).astype(BF16)
            dq_t[:, part] += dot_tn(kv_ref[rows(d), :hd], ds)
            dk += dot(ds, q_ref[part, :])
            dv += dot(p, do_ref[part, :])
        dkv_ref[rows(d), :hd] = dk * scale
        dkv_ref[rows(d), hd:] = dv
        return 0

    def clear(d, _):
        dkv_ref[rows(d), :] = jnp.zeros((tok, 2 * hd), F32)
        return 0

    lax.fori_loop(0, nd + 1, find_top, 0)
    lax.fori_loop(0, nd + 1, find_total, 0)
    tot[...] = 1.0 / tot[...]
    lax.fori_loop(0, nd + 1, forward, 0)
    o_bf = o_t[...].astype(BF16)
    delta[...] = jnp.sum(o_bf.astype(F32) * do_t[...].astype(F32), axis=0, keepdims=True)
    o_ref[...] = o_bf.T
    lax.fori_loop(0, nd + 1, backward, 0)
    dq_ref[...] = (dq_t[...] * scale).astype(BF16).T
    lax.fori_loop(nd + 1, slots, clear, 0)


def finish_kernel(n, near, dkv_ref, o_ref, dq_ref, wq_ref, wk_ref, wv_ref, wo_ref, y_ref, dx_ref,
                  acc, recv, o, dq, wq, wk, wv, wo, y_give, dx_give, dx_part, loc_sem, swap_send, swap_recv, *win_sems):
    me = lax.axis_index('cp')
    core = me % 2
    partner = me + 1 - 2 * core
    blk = block_of(me, n)
    tok = y_ref.shape[0]
    half = tok // 2
    heads, d_model, hd = wq_ref.shape
    mine = pl.ds(pl.multiple_of(core * half, half), half)
    loads = [pltpu.make_async_copy(src, dst, loc_sem.at[i]) for i, (src, dst) in enumerate((
        (o_ref, o), (wo_ref, wo), (dq_ref, dq), (wq_ref, wq), (dkv_ref.at[pl.ds(0, tok)], acc), (wk_ref, wk), (wv_ref, wv)))]
    for c in loads:
        c.start()
    barrier = pltpu.get_barrier_semaphore()
    pl.semaphore_signal(barrier, inc=1, device_id=at(partner), device_id_type=MESH)
    window_signal(barrier, blk, n, near)
    pl.semaphore_wait(barrier, 1 + window_size(blk, n, near))
    sends = [remote(dkv_ref.at[pl.ds(d * tok, tok)], recv.at[pl.ds((d - 1) * tok, tok)], win_sems[0].at[d - 1],
                    win_sems[1].at[d - 1], dev_of(jnp.maximum(blk - d, 0), n)) for d in range(1, near + 1)]
    for d in range(1, near + 1):
        @pl.when(blk - d >= 0)
        def _():
            sends[d - 1].start()
    loads[0].wait()
    loads[1].wait()
    o_cat = jnp.concatenate([o[pl.ds(h * tok, tok), :] for h in range(heads)], axis=1)
    y = dot(o_cat, wo[...]).astype(BF16)
    y_give[...] = y[half:]
    y_ref[mine, :] = y[:half]
    loads[2].wait()
    loads[3].wait()
    dx = dot_nt(dq[pl.ds(0, tok), :], wq[0])
    for h in range(1, heads):
        dx += dot_nt(dq[pl.ds(h * tok, tok), :], wq[h])
    dx_part[...] = dx
    swap_y = remote(y_give, y_ref.at[mine], swap_send.at[0], swap_recv.at[0], partner)
    swap_y.start()
    for c in loads[4:]:
        c.wait()
    for d in range(1, near + 1):
        @pl.when(blk + d < n)
        def _():
            sends[d - 1].wait_recv()
            acc[...] += recv[pl.ds((d - 1) * tok, tok), :]
    dkv = acc[...].astype(BF16)

    def dx_rows(lo):
        rows = slice(lo, lo + half)
        return (dx_part[pl.ds(lo, half), :] + dot_nt(dkv[rows, :hd], wk[...]) + dot_nt(dkv[rows, hd:], wv[...])).astype(BF16)

    dx_give[...] = dx_rows(half)
    dx_ref[mine, :] = dx_rows(0)
    swap_dx = remote(dx_give, dx_ref.at[mine], swap_send.at[1], swap_recv.at[1], partner)
    swap_dx.start()
    for d in range(1, near + 1):
        @pl.when(blk - d >= 0)
        def _():
            sends[d - 1].wait_send()
    swap_y.wait()
    swap_dx.wait()


def make_layer(n, near, far):
    dma = pltpu.SemaphoreType.DMA

    def comm(cid):
        return pltpu.CompilerParams(collective_id=cid, has_side_effects=True, vmem_limit_bytes=VMEM_LIMIT)

    def local_layer(x_in, dy_in, doc_id, w_q, w_k, w_v, w_o):
        tok, d_model = x_in.shape
        heads, hd = w_q.shape[1], w_q.shape[2]
        cols = heads * tok
        seq = tok * n
        me = lax.axis_index('cp')
        blk = block_of(me, n)
        wq = jnp.transpose(w_q, (1, 0, 2))
        wk = w_k.reshape(d_model, hd)
        wv = w_v.reshape(d_model, hd)
        wo = w_o.reshape(heads * hd, d_model)
        counts = jnp.sum((doc_id[:, None] < jnp.arange(128, dtype=jnp.int32)[None, :]).astype(jnp.int32), axis=0)
        n_stage = len(stages_of(n))
        q, do, kvw, table = pl.pallas_call(
            functools.partial(project_kernel, n, near),
            out_shape=(jax.ShapeDtypeStruct((cols, hd), BF16), jax.ShapeDtypeStruct((cols, hd), BF16),
                       jax.ShapeDtypeStruct(((near + 1) * tok, 2 * hd), BF16),
                       jax.ShapeDtypeStruct((n, 1, 128), jnp.int32)),
            in_specs=[HBM, HBM, VMEM, HBM, HBM, HBM, HBM],
            out_specs=(VMEM, VMEM, HBM, VMEM),
            scratch_shapes=[pltpu.VMEM((tok, d_model), BF16), pltpu.VMEM((tok, d_model), BF16),
                            pltpu.VMEM(wq.shape, BF16), pltpu.VMEM(wk.shape, BF16), pltpu.VMEM(wv.shape, BF16),
                            pltpu.VMEM(wo.shape, BF16), pltpu.VMEM((tok, 2 * hd), BF16),
                            dma((7,)), dma((2,)), dma((2,)), dma((near,)), dma((near,)),
                            dma((8 * n_stage,)), dma((8 * n_stage,))],
            compiler_params=comm(0),
            name='project',
        )(x_in, dy_in, counts.reshape(1, 1, 128), wq, wk, wv, wo)

        starts = jnp.sum(table, axis=(0, 1))
        ends = jnp.concatenate([starts[1:], jnp.full((1,), seq, jnp.int32)])
        spans = jnp.where(ends > starts, (ends - 1) // tok - starts // tok, 0)
        span = jnp.max(spans)
        pos = blk * tok + jnp.arange(tok, dtype=jnp.int32)
        first = jnp.max(jnp.where(starts[None, :] <= pos[:, None], starts[None, :], 0), axis=1)
        rel = jnp.tile(first - blk * tok, heads).reshape(1, cols)
        nd = (blk - first[0] // tok).reshape(1)

        def attend(kv, slots, keep):
            saved = [pltpu.VMEM((slots * tok, cols), F32), pltpu.VMEM((slots * tok, cols), BF16)] if keep else []
            return pl.pallas_call(
                functools.partial(attend_kernel, slots, tok, 384, keep),
                out_shape=(jax.ShapeDtypeStruct((cols, hd), BF16), jax.ShapeDtypeStruct((cols, hd), BF16),
                           jax.ShapeDtypeStruct((slots * tok, 2 * hd), F32)),
                in_specs=[SMEM, VMEM, VMEM, VMEM, VMEM],
                out_specs=(VMEM, VMEM, VMEM),
                scratch_shapes=[pltpu.VMEM((hd, cols), BF16), pltpu.VMEM((hd, cols), BF16),
                                pltpu.VMEM((hd, cols), F32), pltpu.VMEM((hd, cols), F32),
                                pltpu.VMEM((1, cols), F32), pltpu.VMEM((1, cols), F32), pltpu.VMEM((1, cols), F32)] + saved,
                compiler_params=pltpu.CompilerParams(vmem_limit_bytes=VMEM_LIMIT),
                name='attend',
            )(nd, rel, q, do, kv)

        def finish(dkv, o, dq, width, cid):
            return pl.pallas_call(
                functools.partial(finish_kernel, n, width),
                out_shape=(jax.ShapeDtypeStruct((tok, d_model), BF16), jax.ShapeDtypeStruct((tok, d_model), BF16)),
                in_specs=[HBM] * 7,
                out_specs=(VMEM, VMEM),
                scratch_shapes=[pltpu.VMEM((tok, 2 * hd), F32), pltpu.VMEM((max(width, 1) * tok, 2 * hd), F32),
                                pltpu.VMEM((cols, hd), BF16), pltpu.VMEM((cols, hd), BF16),
                                pltpu.VMEM(wq.shape, BF16), pltpu.VMEM(wk.shape, BF16), pltpu.VMEM(wv.shape, BF16),
                                pltpu.VMEM(wo.shape, BF16), pltpu.VMEM((tok // 2, d_model), BF16),
                                pltpu.VMEM((tok // 2, d_model), BF16), pltpu.VMEM((tok, d_model), F32),
                                dma((7,)), dma((2,)), dma((2,))] + ([dma((width,)), dma((width,))] if width else []),
                compiler_params=comm(cid),
                name='finish',
            )(dkv, o, dq, wq, wk, wv, wo)

        def with_near(kvw):
            o, dq, dkv = attend(kvw, near + 1, True)
            return finish(dkv, o, dq, near, 2)

        def with_far(kvw):
            kv = pl.pallas_call(
                functools.partial(gather_kernel, n, far),
                out_shape=jax.ShapeDtypeStruct(((far + 1) * tok, 2 * hd), BF16),
                in_specs=[HBM], out_specs=HBM,
                scratch_shapes=[dma((far,)), dma((far,)), dma((1,))],
                compiler_params=comm(1),
                name='gather',
            )(kvw[:tok])
            o, dq, dkv = attend(kv, far + 1, True)
            return finish(dkv, o, dq, far, 3)

        order = [2 * b if b < n // 2 else 2 * (n - 1 - b) + 1 for b in range(n)]
        up = [(order[b], order[(b + 1) % n]) for b in range(n)]
        down = [(dst, src) for src, dst in up]

        def with_all(kvw):
            def pull(d, state):
                held, kv = state
                held = lax.ppermute(held, 'cp', up)
                return held, lax.dynamic_update_slice_in_dim(kv, held, d * tok, 0)

            own = kvw[:tok]
            kv = lax.dynamic_update_slice_in_dim(jnp.zeros((n * tok, 2 * hd), BF16), own, 0, 0)
            kv = lax.fori_loop(1, n, pull, (own, kv))[1]
            o, dq, dkv = attend(kv, n, False)

            def push(step, acc):
                acc = acc + lax.dynamic_slice_in_dim(dkv, (n - 1 - step) * tok, tok, 0)
                return lax.ppermute(acc, 'cp', down)

            acc = lax.fori_loop(0, n - 1, push, jnp.zeros((tok, 2 * hd), F32))
            return finish(acc + dkv[:tok], o, dq, 0, 4)

        which = (span > near).astype(jnp.int32) + (span > far).astype(jnp.int32)
        return lax.switch(which, (with_near, with_far, with_all), kvw)

    return local_layer


def solution(mesh, near=NEAR, far=FAR):
    n = mesh.shape['cp']
    row_spec = P(('dp', 'cp'))
    full_spec = P()
    return jax.shard_map(make_layer(n, near, far), mesh=mesh,
                         in_specs=(row_spec, row_spec, row_spec, full_spec, full_spec, full_spec, full_spec),
                         out_specs=(row_spec, row_spec), check_vma=False)
```

```python
import functools

import jax
import jax.numpy as jnp
from jax import lax
from jax.experimental import pallas as pl
from jax.experimental.pallas import tpu as pltpu
from jax.sharding import PartitionSpec as P

NEG_BIG = -1.0e30
MESH = pl.DeviceIdType.MESH
WIDTHS, FAR, CHUNK = (8, 10, 12), 24, 384
F32, BF16 = jnp.float32, jnp.bfloat16
HBM = pl.BlockSpec(memory_space=pl.ANY)
VMEM = pl.BlockSpec(memory_space=pltpu.VMEM)
SMEM = pl.BlockSpec(memory_space=pltpu.SMEM)
VMEM_LIMIT = 60 * 1024 * 1024


def dot(a, b):
    return jnp.dot(a, b, preferred_element_type=F32)


def dot_nt(a, b):
    return lax.dot_general(a, b, (((1,), (1,)), ((), ())), preferred_element_type=F32)


def dot_tn(a, b):
    return lax.dot_general(a, b, (((0,), (0,)), ((), ())), preferred_element_type=F32)


def block_of(dev, n):
    return jnp.where(dev % 2 == 0, dev // 2, n - 1 - dev // 2)


def dev_of(blk, n):
    return jnp.where(blk < n // 2, 2 * blk, 2 * (n - 1 - blk) + 1)


def at(dev):
    return (lax.axis_index('dp'), dev)


def stages_of(n):
    out, stride = [(1, min(n, 8))], min(n, 8)
    while stride < n:
        size = min(4, n // stride)
        out.append((stride, size))
        stride *= size
    return out


def peer_of(me, stride, size, j):
    idx = (me // stride) % size
    return me - idx * stride + ((idx + j) % size) * stride


def remote(src, dst, send, recv, dev):
    return pltpu.make_async_remote_copy(src_ref=src, dst_ref=dst, send_sem=send, recv_sem=recv,
                                        device_id=at(dev), device_id_type=MESH)


def column(blk, n, reach):
    out = []
    for dy in range(1, reach + 1):
        out.append((blk - 4 * dy, blk - 4 * dy >= 0))
        out.append((blk + 4 * dy, blk + 4 * dy < n))
    return out


def signal(barrier, dev):
    pl.semaphore_signal(barrier, inc=1, device_id=at(dev), device_id_type=MESH)


def column_signal(barrier, blk, n, reach):
    for other, there in column(blk, n, reach):
        @pl.when(there)
        def _():
            signal(barrier, dev_of(other, n))


def column_size(blk, n, reach):
    return jnp.minimum((n - 1 - blk) // 4, reach) + jnp.minimum(blk // 4, reach)


class Gather:
    def __init__(self, n, blk, reach, k_ref, v_ref, sems):
        self.n, self.blk, self.reach = n, blk, reach
        place = blk % 4
        base = blk - place
        mates = [dev_of(base + (place + m) % 4, n) for m in range(1, 4)]
        later = [dev_of(jnp.minimum(blk + 4 * dy, n - 1), n) for dy in range(1, reach + 1)]
        depth = reach + 1
        col = pl.ds(place * depth, depth)
        k1s, k1r, k2s, k2r, v1s, v1r, v2s, v2r = sems
        self.k1 = [remote(k_ref.at[place], k_ref.at[place], k1s.at[m], k1r.at[m], mates[m]) for m in range(3)]
        self.k2 = [remote(k_ref.at[pl.ds(0, 4)], k_ref.at[pl.ds(4 * dy, 4)], k2s.at[dy - 1], k2r.at[dy - 1], later[dy - 1])
                   for dy in range(1, reach + 1)]
        self.v1 = [remote(v_ref.at[place * depth], v_ref.at[place * depth + dy], v1s.at[dy - 1], v1r.at[dy - 1], later[dy - 1])
                   for dy in range(1, reach + 1)]
        self.v2 = [remote(v_ref.at[col], v_ref.at[col], v2s.at[m], v2r.at[m], mates[m]) for m in range(3)]

    def sending(self, act):
        for dy in range(1, self.reach + 1):
            @pl.when(self.blk + 4 * dy < self.n)
            def _():
                act(dy - 1)

    def receiving(self, act):
        for dy in range(1, self.reach + 1):
            @pl.when(self.blk - 4 * dy >= 0)
            def _():
                act(dy - 1)

    def first(self):
        for c in self.k1:
            c.start()
        self.sending(lambda i: self.v1[i].start())

    def second(self):
        for c in self.k1:
            c.wait_recv()
        self.sending(lambda i: self.k2[i].start())
        self.receiving(lambda i: self.v1[i].wait_recv())
        for c in self.v2:
            c.start()

    def finish(self):
        for c in self.v2:
            c.wait_recv()
        self.receiving(lambda i: self.k2[i].wait_recv())
        for c in self.k1 + self.v2:
            c.wait_send()
        self.sending(lambda i: self.v1[i].wait_send())
        self.sending(lambda i: self.k2[i].wait_send())


def gather_sems(reach):
    dma = pltpu.SemaphoreType.DMA
    return [dma((k,)) for k in (3, 3, reach, reach, reach, reach, 3, 3)]


def project_kernel(n, reach, x_ref, dy_ref, cnt_ref, wq_ref, wk_ref, wv_ref, wo_ref,
                   q_ref, do_ref, k_ref, v_ref, tab_ref,
                   xs, dys, wq, wk, wv, wo, loc_sem, swap_send, swap_recv, tab_send, tab_recv, *win):
    me = lax.axis_index('cp')
    core = me % 2
    partner = me + 1 - 2 * core
    blk = block_of(me, n)
    place = blk % 4
    tok = x_ref.shape[0]
    half = tok // 2
    heads = wq_ref.shape[0]
    hd = wq_ref.shape[2]
    keep = pl.ds(pl.multiple_of(core * half, half), half)
    give = pl.ds(pl.multiple_of((1 - core) * half, half), half)
    loads = [pltpu.make_async_copy(src, dst, loc_sem.at[i]) for i, (src, dst) in enumerate((
        (x_ref.at[keep], xs.at[pl.ds(0, half)]), (wk_ref, wk), (wv_ref, wv), (wq_ref, wq),
        (dy_ref.at[keep], dys.at[pl.ds(0, half)]), (wo_ref, wo)))]
    for c in loads:
        c.start()
    barrier = pltpu.get_barrier_semaphore()
    stages = stages_of(n)
    peers = 0
    for stride, size in stages:
        for j in range(1, size):
            signal(barrier, peer_of(me, stride, size, j))
            peers += 1
    column_signal(barrier, blk, n, reach)
    tab_ref[me] = cnt_ref[0]
    pl.semaphore_wait(barrier, peers + column_size(blk, n, reach))

    swap_x = remote(x_ref.at[give], xs.at[pl.ds(half, half)], swap_send.at[0], swap_recv.at[0], partner)
    swap_dy = remote(dy_ref.at[give], dys.at[pl.ds(half, half)], swap_send.at[1], swap_recv.at[1], partner)
    swap_x.start()
    swap_dy.start()

    def stage_copies(s):
        stride, size = stages[s]
        rows = pl.ds(me - me % stride, stride)
        src = cnt_ref if s == 0 else tab_ref.at[rows]
        return [remote(src, tab_ref.at[rows], tab_send.at[8 * s + j], tab_recv.at[8 * s + j],
                       peer_of(me, stride, size, j)) for j in range(1, size)]

    tables = [stage_copies(s) for s in range(len(stages))]
    for c in tables[0]:
        c.start()
    for c in loads[:3]:
        c.wait()
    swap_x.wait_recv()
    k_ref[place] = dot(xs[...], wk[...]).astype(BF16)
    v_ref[place * (reach + 1)] = dot(xs[...], wv[...]).astype(BF16)
    loads[3].wait()

    def q_head(h):
        q_ref[pl.ds(h * tok, tok), :] = dot(xs[...], wq[h]).astype(BF16)

    q_head(0)
    q_head(1)
    gather = Gather(n, blk, reach, k_ref, v_ref, win)
    gather.first()
    for h in range(2, heads):
        q_head(h)
    gather.second()
    for s in range(1, len(stages)):
        for c in tables[s - 1]:
            c.wait()
        for c in tables[s]:
            c.start()
        if s == 1:
            loads[4].wait()
            loads[5].wait()
            swap_dy.wait_recv()
            for h in range(heads // 2):
                do_ref[pl.ds(h * tok, tok), :] = dot_nt(dys[...], wo[pl.ds(h * hd, hd), :]).astype(BF16)
    if len(stages) == 1:
        loads[4].wait()
        loads[5].wait()
        swap_dy.wait_recv()
    for h in range(heads // 2 if len(stages) > 1 else 0, heads):
        do_ref[pl.ds(h * tok, tok), :] = dot_nt(dys[...], wo[pl.ds(h * hd, hd), :]).astype(BF16)
    for c in tables[-1]:
        c.wait()
    swap_x.wait_send()
    swap_dy.wait_send()
    gather.finish()


def gather_kernel(n, reach, k_own_ref, v_own_ref, k_ref, v_ref, loc_sem, *win):
    me = lax.axis_index('cp')
    blk = block_of(me, n)
    place = blk % 4
    own = [pltpu.make_async_copy(k_own_ref, k_ref.at[place], loc_sem.at[0]),
           pltpu.make_async_copy(v_own_ref, v_ref.at[place * (reach + 1)], loc_sem.at[1])]
    for c in own:
        c.start()
    barrier = pltpu.get_barrier_semaphore()
    for m in range(1, 4):
        signal(barrier, dev_of(blk - place + (place + m) % 4, n))
    column_signal(barrier, blk, n, reach)
    pl.semaphore_wait(barrier, 3 + column_size(blk, n, reach))
    for c in own:
        c.wait()
    gather = Gather(n, blk, reach, k_ref, v_ref, win)
    gather.first()
    gather.second()
    gather.finish()


def attend_kernel(reach, chunk, keep, nd_ref, start_ref, q_ref, do_ref, k_ref, v_ref, o_ref, dq_ref, dk_ref, dv_ref,
                  q_t, do_t, o_t, dq_t, top, tot, delta, *saved):
    nd = nd_ref[0]
    place = nd_ref[1]
    slots, tok = k_ref.shape[0], k_ref.shape[1]
    cols = q_ref.shape[0]
    hd = q_ref.shape[1]
    scale = hd ** -0.5
    q_t[...] = q_ref[...].T
    do_t[...] = do_ref[...].T
    parts = [pl.ds(c * chunk, chunk) for c in range(cols // chunk)]

    def rows(d):
        return pl.ds(pl.multiple_of(d * tok, tok), tok)

    def k_slot(d):
        if not reach:
            return d
        back = (d + 3 - place) // 4
        return 4 * back + (place - d + 4 * back)

    def v_slot(d):
        if not reach:
            return d
        back = (d + 3 - place) // 4
        return (place - d + 4 * back) * (reach + 1) + back

    def scores(d, part, c):
        s = dot(k_ref[k_slot(d)], q_t[:, part]) * scale
        u = lax.broadcasted_iota(jnp.int32, (tok, chunk), 0) - d * tok
        t = (lax.broadcasted_iota(jnp.int32, (1, chunk), 1) + c * chunk) % tok
        return jnp.where((u >= start_ref[:, part]) & (u <= t), s, NEG_BIG)

    top[...] = jnp.full_like(top, NEG_BIG)
    tot[...] = jnp.zeros_like(tot)
    o_t[...] = jnp.zeros_like(o_t)
    dq_t[...] = jnp.zeros_like(dq_t)

    def find_top(d, _):
        for c, part in enumerate(parts):
            s = scores(d, part, c)
            if keep:
                saved[0][rows(d), part] = s
            top[:, part] = jnp.maximum(top[:, part], jnp.max(s, axis=0, keepdims=True))
        return 0

    def find_total(d, _):
        for c, part in enumerate(parts):
            s = saved[0][rows(d), part] if keep else scores(d, part, c)
            e = jnp.exp(s - top[:, part])
            if keep:
                saved[0][rows(d), part] = e
            tot[:, part] = tot[:, part] + jnp.sum(e, axis=0, keepdims=True)
        return 0

    def prob(d, part, c):
        e = saved[0][rows(d), part] if keep else jnp.exp(scores(d, part, c) - top[:, part])
        return (e * tot[:, part]).astype(BF16)

    def forward(d, _):
        for c, part in enumerate(parts):
            p = prob(d, part, c)
            if keep:
                saved[1][rows(d), part] = p
            o_t[:, part] += dot_tn(v_ref[v_slot(d)], p)
        return 0

    def backward(d, _):
        dk = jnp.zeros((tok, hd), F32)
        dv = jnp.zeros((tok, hd), F32)
        for c, part in enumerate(parts):
            p = saved[1][rows(d), part] if keep else prob(d, part, c)
            dp = dot(v_ref[v_slot(d)], do_t[:, part])
            ds = (p.astype(F32) * (dp - delta[:, part])).astype(BF16)
            dq_t[:, part] += dot_tn(k_ref[k_slot(d)], ds)
            dk += dot(ds, q_ref[part, :])
            dv += dot(p, do_ref[part, :])
        dk_ref[k_slot(d)] = dk * scale
        dv_ref[v_slot(d)] = dv
        return 0

    def clear(i, _):
        if not reach:
            dk_ref[nd + 1 + i] = jnp.zeros((tok, hd), F32)
            dv_ref[nd + 1 + i] = jnp.zeros((tok, hd), F32)
        else:
            d = place + 4 * (i // 4) - i % 4

            @pl.when((d < 0) | (d > nd))
            def _():
                dk_ref[i] = jnp.zeros((tok, hd), F32)
                dv_ref[(i % 4) * (reach + 1) + i // 4] = jnp.zeros((tok, hd), F32)
        return 0

    lax.fori_loop(0, nd + 1, find_top, 0)
    lax.fori_loop(0, nd + 1, find_total, 0)
    tot[...] = 1.0 / tot[...]
    lax.fori_loop(0, nd + 1, forward, 0)
    o_bf = o_t[...].astype(BF16)
    delta[...] = jnp.sum(o_bf.astype(F32) * do_t[...].astype(F32), axis=0, keepdims=True)
    o_ref[...] = o_bf.T
    lax.fori_loop(0, nd + 1, backward, 0)
    dq_ref[...] = (dq_t[...] * scale).astype(BF16).T
    lax.fori_loop(0, slots if reach else slots - 1 - nd, clear, 0)


def finish_kernel(n, reach, width, dk_ref, dv_ref, o_ref, dq_ref, wq_ref, wk_ref, wv_ref, wo_ref, y_ref, dx_ref,
                  acc_k, acc_v, o, dq, wq, wk, wv, wo, y_give, dx_give, dx_part, loc_sem, swap_send, swap_recv, *win):
    me = lax.axis_index('cp')
    core = me % 2
    partner = me + 1 - 2 * core
    blk = block_of(me, n)
    place = blk % 4
    base = blk - place
    tok = y_ref.shape[0]
    half = tok // 2
    heads, d_model, hd = wq_ref.shape
    rows = (width + 3) // 4
    depth = reach + 1
    mine = pl.ds(pl.multiple_of(core * half, half), half)
    col = pl.ds(place * depth, rows + 1)
    own_k = dk_ref.at[pl.ds(0, 4)] if reach else dk_ref
    own_v = dv_ref.at[col] if reach else dv_ref
    loads = [pltpu.make_async_copy(src, dst, loc_sem.at[i]) for i, (src, dst) in enumerate((
        (own_v, acc_v), (own_k, acc_k), (o_ref, o), (wo_ref, wo), (dq_ref, dq), (wq_ref, wq), (wk_ref, wk), (wv_ref, wv)))]
    for c in loads:
        c.start()
    barrier = pltpu.get_barrier_semaphore()
    signal(barrier, partner)
    if reach:
        for m in range(1, 4):
            signal(barrier, dev_of(base + (place + m) % 4, n))
        column_signal(barrier, blk, n, rows)
        pl.semaphore_wait(barrier, 4 + column_size(blk, n, rows))
        recv_k1, recv_k2, recv_v1, recv_v2, k1s, k1r, k2s, k2r, v1s, v1r, v2s, v2r = win
        mates = [(base + (place + m) % 4, (place + m) % 4) for m in range(1, 4)]
        earlier = [dev_of(jnp.maximum(blk - 4 * dy, 0), n) for dy in range(1, rows + 1)]
        first = [max(0, 4 * dy - width) for dy in range(1, rows + 1)]
        k1 = [remote(dk_ref.at[pl.ds(4 * dy + first[dy - 1], 4 - first[dy - 1])],
                     recv_k1.at[dy - 1, pl.ds(first[dy - 1], 4 - first[dy - 1])], k1s.at[dy - 1], k1r.at[dy - 1], earlier[dy - 1])
              for dy in range(1, rows + 1)]
        v1 = [remote(dv_ref.at[pl.ds(j * depth, rows + 1)], recv_v1.at[m], v1s.at[m], v1r.at[m], dev_of(b, n))
              for m, (b, j) in enumerate(mates)]
        k2 = [remote(acc_k.at[j], recv_k2.at[m], k2s.at[m], k2r.at[m], dev_of(b, n)) for m, (b, j) in enumerate(mates)]
        v2 = [remote(acc_v.at[dy], recv_v2.at[dy - 1], v2s.at[dy - 1], v2r.at[dy - 1], earlier[dy - 1])
              for dy in range(1, rows + 1)]
    else:
        pl.semaphore_wait(barrier, 1)

    def sending(act):
        for dy in range(1, rows + 1):
            @pl.when(blk - 4 * dy >= 0)
            def _():
                act(dy - 1)

    def receiving(act):
        for dy in range(1, rows + 1):
            @pl.when(blk + 4 * dy < n)
            def _():
                act(dy - 1)

    if reach:
        for c in v1:
            c.start()
        sending(lambda i: k1[i].start())
    for c in loads[2:4]:
        c.wait()
    o_cat = jnp.concatenate([o[pl.ds(h * tok, tok), :] for h in range(heads)], axis=1)
    y = dot(o_cat, wo[...]).astype(BF16)
    y_give[...] = y[half:]
    y_ref[mine, :] = y[:half]
    for c in loads[4:6]:
        c.wait()
    dx = dot_nt(dq[pl.ds(0, tok), :], wq[0])
    for h in range(1, heads):
        dx += dot_nt(dq[pl.ds(h * tok, tok), :], wq[h])
    dx_part[...] = dx
    swap_y = remote(y_give, y_ref.at[mine], swap_send.at[0], swap_recv.at[0], partner)
    swap_y.start()
    for c in loads[:2] + loads[6:]:
        c.wait()
    if reach:
        def add_k1(i):
            k1[i].wait_recv()
            acc_k[pl.ds(first[i], 4 - first[i])] += recv_k1[i, pl.ds(first[i], 4 - first[i])]

        def add_v2(i):
            v2[i].wait_recv()
            acc_v[0] += recv_v2[i]

        for m in range(3):
            v1[m].wait_recv()
            acc_v[...] += recv_v1[m]
        receiving(add_k1)
        sending(lambda i: v2[i].start())
        for c in k2:
            c.start()
        total_k = acc_k[place]
        for m in range(3):
            k2[m].wait_recv()
            total_k = total_k + recv_k2[m]
        receiving(add_v2)
    else:
        total_k = acc_k[0]
    dk = total_k.astype(BF16)
    dv = acc_v[0].astype(BF16)

    def dx_rows(lo):
        part = slice(lo, lo + half)
        return (dx_part[pl.ds(lo, half), :] + dot_nt(dk[part], wk[...]) + dot_nt(dv[part], wv[...])).astype(BF16)

    dx_give[...] = dx_rows(half)
    dx_ref[mine, :] = dx_rows(0)
    swap_dx = remote(dx_give, dx_ref.at[mine], swap_send.at[1], swap_recv.at[1], partner)
    swap_dx.start()
    if reach:
        for c in v1 + k2:
            c.wait_send()
        sending(lambda i: k1[i].wait_send())
        sending(lambda i: v2[i].wait_send())
    swap_y.wait()
    swap_dx.wait()


def make_layer(n, widths, far):
    dma = pltpu.SemaphoreType.DMA
    near = widths[-1]

    def comm(cid):
        return pltpu.CompilerParams(collective_id=cid, has_side_effects=True, vmem_limit_bytes=VMEM_LIMIT)

    def local_layer(x_in, dy_in, doc_id, w_q, w_k, w_v, w_o):
        tok, d_model = x_in.shape
        heads, hd = w_q.shape[1], w_q.shape[2]
        cols = heads * tok
        seq = tok * n
        me = lax.axis_index('cp')
        blk = block_of(me, n)
        place = blk % 4
        wq = jnp.transpose(w_q, (1, 0, 2))
        wk = w_k.reshape(d_model, hd)
        wv = w_v.reshape(d_model, hd)
        wo = w_o.reshape(heads * hd, d_model)
        counts = jnp.sum((doc_id[:, None] < jnp.arange(128, dtype=jnp.int32)[None, :]).astype(jnp.int32), axis=0)
        n_stage = len(stages_of(n))
        reach = (near + 3) // 4

        def window(reach, dtype=BF16):
            return jax.ShapeDtypeStruct((4 * (reach + 1), tok, hd), dtype)

        q, do, k_win, v_win, table = pl.pallas_call(
            functools.partial(project_kernel, n, reach),
            out_shape=(jax.ShapeDtypeStruct((cols, hd), BF16), jax.ShapeDtypeStruct((cols, hd), BF16),
                       window(reach), window(reach), jax.ShapeDtypeStruct((n, 1, 128), jnp.int32)),
            in_specs=[HBM, HBM, VMEM, HBM, HBM, HBM, HBM],
            out_specs=(VMEM, VMEM, VMEM, VMEM, VMEM),
            scratch_shapes=[pltpu.VMEM((tok, d_model), BF16), pltpu.VMEM((tok, d_model), BF16),
                            pltpu.VMEM(wq.shape, BF16), pltpu.VMEM(wk.shape, BF16), pltpu.VMEM(wv.shape, BF16),
                            pltpu.VMEM(wo.shape, BF16),
                            dma((6,)), dma((2,)), dma((2,)), dma((8 * n_stage,)), dma((8 * n_stage,))] + gather_sems(reach),
            compiler_params=comm(0),
            name='project',
        )(x_in, dy_in, counts.reshape(1, 1, 128), wq, wk, wv, wo)

        starts = jnp.sum(table, axis=(0, 1))
        ends = jnp.concatenate([starts[1:], jnp.full((1,), seq, jnp.int32)])
        spans = jnp.where(ends > starts, (ends - 1) // tok - starts // tok, 0)
        span = jnp.max(spans)
        pos = blk * tok + jnp.arange(tok, dtype=jnp.int32)
        first = jnp.max(jnp.where(starts[None, :] <= pos[:, None], starts[None, :], 0), axis=1)
        rel = jnp.tile(first - blk * tok, heads).reshape(1, cols)
        nd = jnp.stack([blk - first[0] // tok, place])

        def attend(k, v, width, reach):
            slots = k.shape[0]
            saved = [pltpu.VMEM(((width + 1) * tok, cols), F32), pltpu.VMEM(((width + 1) * tok, cols), BF16)] if width else []
            return pl.pallas_call(
                functools.partial(attend_kernel, reach, CHUNK, bool(width)),
                out_shape=(jax.ShapeDtypeStruct((cols, hd), BF16), jax.ShapeDtypeStruct((cols, hd), BF16),
                           jax.ShapeDtypeStruct(k.shape, F32), jax.ShapeDtypeStruct(k.shape, F32)),
                in_specs=[SMEM, VMEM, VMEM, VMEM, VMEM, VMEM],
                out_specs=(VMEM, VMEM, VMEM, VMEM),
                scratch_shapes=[pltpu.VMEM((hd, cols), BF16), pltpu.VMEM((hd, cols), BF16),
                                pltpu.VMEM((hd, cols), F32), pltpu.VMEM((hd, cols), F32),
                                pltpu.VMEM((1, cols), F32), pltpu.VMEM((1, cols), F32), pltpu.VMEM((1, cols), F32)] + saved,
                compiler_params=pltpu.CompilerParams(vmem_limit_bytes=VMEM_LIMIT),
                name='attend',
            )(nd, rel, q, do, k, v)

        def finish(dk, dv, o, dq, reach, width, cid):
            rows = (width + 3) // 4
            win = [pltpu.VMEM((rows, 4, tok, hd), F32), pltpu.VMEM((3, tok, hd), F32),
                   pltpu.VMEM((3, rows + 1, tok, hd), F32), pltpu.VMEM((rows, tok, hd), F32),
                   dma((rows,)), dma((rows,)), dma((3,)), dma((3,)), dma((3,)), dma((3,)), dma((rows,)), dma((rows,))]
            return pl.pallas_call(
                functools.partial(finish_kernel, n, reach, width),
                out_shape=(jax.ShapeDtypeStruct((tok, d_model), BF16), jax.ShapeDtypeStruct((tok, d_model), BF16)),
                in_specs=[HBM] * 8,
                out_specs=(VMEM, VMEM),
                scratch_shapes=[pltpu.VMEM((4 if reach else 1, tok, hd), F32), pltpu.VMEM((rows + 1, tok, hd), F32),
                                pltpu.VMEM((cols, hd), BF16), pltpu.VMEM((cols, hd), BF16),
                                pltpu.VMEM(wq.shape, BF16), pltpu.VMEM(wk.shape, BF16), pltpu.VMEM(wv.shape, BF16),
                                pltpu.VMEM(wo.shape, BF16), pltpu.VMEM((tok // 2, d_model), BF16),
                                pltpu.VMEM((tok // 2, d_model), BF16), pltpu.VMEM((tok, d_model), F32),
                                dma((8,)), dma((2,)), dma((2,))] + (win if reach else []),
                compiler_params=comm(cid),
                name='finish',
            )(dk, dv, o, dq, wq, wk, wv, wo)

        def with_near(width, cid):
            def run(k, v):
                o, dq, dk, dv = attend(k, v, near, reach)
                return finish(dk, dv, o, dq, reach, width, cid)
            return run

        def own(k, v):
            return (lax.dynamic_index_in_dim(k, place, 0, keepdims=False),
                    lax.dynamic_index_in_dim(v, place * (reach + 1), 0, keepdims=False))

        def with_far(k, v):
            reach = (far + 3) // 4
            k, v = pl.pallas_call(
                functools.partial(gather_kernel, n, reach),
                out_shape=(window(reach), window(reach)),
                in_specs=[HBM, HBM], out_specs=(HBM, HBM),
                scratch_shapes=[dma((2,))] + gather_sems(reach),
                compiler_params=comm(1),
                name='gather',
            )(*own(k, v))
            o, dq, dk, dv = attend(k, v, far, reach)
            return finish(dk, dv, o, dq, reach, far, 2)

        order = [2 * b if b < n // 2 else 2 * (n - 1 - b) + 1 for b in range(n)]
        up = [(order[b], order[(b + 1) % n]) for b in range(n)]
        down = [(dst, src) for src, dst in up]

        def with_all(k, v):
            def pull(d, state):
                held, k, v = state
                held = lax.ppermute(held, 'cp', up)
                return held, k.at[d].set(held[0]), v.at[d].set(held[1])

            held = jnp.stack(own(k, v))
            empty = jnp.zeros((n, tok, hd), BF16)
            _, k, v = lax.fori_loop(1, n, pull, (held, empty.at[0].set(held[0]), empty.at[0].set(held[1])))
            o, dq, dk, dv = attend(k, v, 0, 0)

            def push(step, acc):
                d = n - 1 - step
                acc = acc + jnp.stack([lax.dynamic_index_in_dim(dk, d, 0, keepdims=False),
                                       lax.dynamic_index_in_dim(dv, d, 0, keepdims=False)])
                return lax.ppermute(acc, 'cp', down)

            acc = lax.fori_loop(0, n - 1, push, jnp.zeros((2, tok, hd), F32))
            return finish((acc[0] + dk[0])[None], (acc[1] + dv[0])[None], o, dq, 0, 0, 3)

        which = sum((span > w).astype(jnp.int32) for w in (*widths, far))
        branches = [with_near(w, 4 + i) for i, w in enumerate(widths)] + [with_far, with_all]
        return lax.switch(which, branches, k_win, v_win)

    return local_layer


def solution(mesh, widths=WIDTHS, far=FAR):
    n = mesh.shape['cp']
    row_spec = P(('dp', 'cp'))
    full_spec = P()
    return jax.shard_map(make_layer(n, widths, far), mesh=mesh,
                         in_specs=(row_spec, row_spec, row_spec, full_spec, full_spec, full_spec, full_spec),
                         out_specs=(row_spec, row_spec), check_vma=False)
```

```python
import functools

import jax
import jax.numpy as jnp
from jax import lax
from jax.experimental import pallas as pl
from jax.experimental.pallas import tpu as pltpu
from jax.sharding import PartitionSpec as P

NEG_BIG = -1.0e30
GROUP = 4
MESH = pl.DeviceIdType.MESH
WIDTHS, FAR, CHUNK, WIDE = (8, 10, 12), 24, 256, 384
LOG2_E = 1.4426950408889634
F32, BF16 = jnp.float32, jnp.bfloat16
HBM = pl.BlockSpec(memory_space=pl.ANY)
VMEM = pl.BlockSpec(memory_space=pltpu.VMEM)
SMEM = pl.BlockSpec(memory_space=pltpu.SMEM)
VMEM_LIMIT = 60 * 1024 * 1024


def dot(a, b):
    return jnp.dot(a, b, preferred_element_type=F32)


def dot_nt(a, b):
    return lax.dot_general(a, b, (((1,), (1,)), ((), ())), preferred_element_type=F32)


def dot_tn(a, b):
    return lax.dot_general(a, b, (((0,), (0,)), ((), ())), preferred_element_type=F32)


def block_of(dev, n):
    return jnp.where(dev % 2 == 0, dev // 2, n - 1 - dev // 2)


def dev_of(blk, n):
    return jnp.where(blk < n // 2, 2 * blk, 2 * (n - 1 - blk) + 1)


def at(dev):
    return (lax.axis_index('dp'), dev)


def stages_of(n):
    out, stride = [(1, min(n, 8))], min(n, 8)
    while stride < n:
        size = min(4, n // stride)
        out.append((stride, size))
        stride *= size
    return out


def peer_of(me, stride, size, j):
    idx = (me // stride) % size
    return me - idx * stride + ((idx + j) % size) * stride


def remote(src, dst, send, recv, dev):
    return pltpu.make_async_remote_copy(src_ref=src, dst_ref=dst, send_sem=send, recv_sem=recv,
                                        device_id=at(dev), device_id_type=MESH)


def column(blk, n, reach):
    out = []
    for dy in range(1, reach + 1):
        out.append((blk - GROUP * dy, blk - GROUP * dy >= 0))
        out.append((blk + GROUP * dy, blk + GROUP * dy < n))
    return out


def signal(barrier, dev):
    pl.semaphore_signal(barrier, inc=1, device_id=at(dev), device_id_type=MESH)


def column_signal(barrier, blk, n, reach):
    for other, there in column(blk, n, reach):
        @pl.when(there)
        def _():
            signal(barrier, dev_of(other, n))


def column_size(blk, n, reach):
    return jnp.minimum((n - 1 - blk) // GROUP, reach) + jnp.minimum(blk // GROUP, reach)


class Moves:
    def __init__(self, send, recv):
        self.sems, self.copies = (send, recv), []

    def new(self, src, dst, dev, go=None, come=None):
        i = len(self.copies)
        self.copies.append((remote(src, dst, self.sems[0].at[i], self.sems[1].at[i], dev), go, come))
        return i

    def when(self, cond, act):
        if cond is None:
            act()
        else:
            pl.when(cond)(act)

    def start(self, i):
        copy, go, _ = self.copies[i]
        self.when(go, copy.start)

    def arrived(self, i, then=None):
        copy, _, come = self.copies[i]

        def act():
            copy.wait_recv()
            if then is not None:
                then()
        self.when(come, act)

    def sent(self):
        for copy, go, _ in self.copies:
            self.when(go, copy.wait_send)


class Gather:
    def __init__(self, n, blk, reach, k_ref, v_ref, send, recv):
        place = blk % GROUP
        base = blk - place
        depth = reach + 1
        self.m = m = Moves(send, recv)

        def mate(r):
            return dev_of(base + (place + r) % GROUP, n)

        def later(dy):
            return dev_of(jnp.minimum(blk + GROUP * dy, n - 1), n)

        def k_at(dy, r):
            return k_ref.at[GROUP * dy + (place + r) % GROUP]

        def v_at(r, dy):
            return v_ref.at[((place + r) % GROUP) * depth + dy]

        def up(dy):
            return blk + GROUP * dy < n

        def down(dy):
            return blk - GROUP * dy >= 0

        both = up(1) & down(1)
        mid = down(2)
        self.straight = [dy for dy in range(1, reach + 1) if dy != 2]
        self.k_x = {r: m.new(k_at(0, 0), k_at(0, 0), mate(r)) for r in (1, 3)}
        self.k_xx = m.new(k_at(0, 3), k_at(0, 3), mate(1))
        self.k_y = {(dy, r): m.new(k_at(0, r), k_at(dy, r), later(dy), up(dy), down(dy)) for dy in self.straight for r in range(GROUP)}
        self.v_y = {dy: m.new(v_at(0, 0), v_at(0, dy), later(dy), up(dy), down(dy)) for dy in self.straight}
        rows = [(0, None)] + [(dy, down(dy)) for dy in range(1, reach + 1)]
        self.v_x = {(dy, r): m.new(v_at(0, dy), v_at(0, dy), mate(r), c, c) for dy, c in rows for r in (1, 3)}
        self.v_xx = {dy: m.new(v_at(3, dy), v_at(3, dy), mate(1), c, c) for dy, c in rows}
        if reach > 1:
            self.k_yy = {r: m.new(k_at(1, r), k_at(2, r), later(1), both, mid) for r in range(GROUP)}
            self.v_yy = m.new(v_at(0, 1), v_at(0, 2), later(1), both, mid)
        self.reach = reach

    def own(self):
        m = self.m
        for r in (1, 3):
            m.start(self.k_x[r])
        self.k_on(0)
        for dy in self.straight:
            m.start(self.v_y[dy])
        self.v_on(0)

    def k_on(self, r):
        for dy in self.straight:
            self.m.start(self.k_y[dy, r])

    def v_on(self, dy):
        for r in (1, 3):
            self.m.start(self.v_x[dy, r])

    def hand_on(self):
        m = self.m
        m.arrived(self.k_x[1])
        m.start(self.k_xx)
        self.k_on(3)
        m.arrived(self.v_y[1])
        if self.reach > 1:
            m.start(self.v_yy)
        self.v_on(1)
        m.arrived(self.k_x[3])
        self.k_on(1)
        for dy in self.straight[1:]:
            m.arrived(self.v_y[dy])
            self.v_on(dy)
        m.arrived(self.v_x[0, 1])
        m.start(self.v_xx[0])
        m.arrived(self.k_y[1, 0])
        if self.reach > 1:
            m.start(self.k_yy[0])
        m.arrived(self.k_xx)
        self.k_on(2)
        if self.reach > 1:
            m.arrived(self.v_yy)
            self.v_on(2)

    def rest(self):
        m = self.m
        order = [1] + self.straight[1:] + ([2] if self.reach > 1 else [])
        for i in range(max(len(order), 3)):
            if i < len(order):
                m.arrived(self.v_x[order[i], 1])
                m.start(self.v_xx[order[i]])
            if i < 3:
                r = (3, 1, 2)[i]
                m.arrived(self.k_y[1, r])
                if self.reach > 1:
                    m.start(self.k_yy[r])

    def finish(self):
        m = self.m
        for dy in self.straight[1:]:
            for r in range(GROUP):
                m.arrived(self.k_y[dy, r])
        for dy in range(self.reach + 1):
            m.arrived(self.v_x[dy, 3])
            m.arrived(self.v_xx[dy])
        if self.reach > 1:
            for r in range(GROUP):
                m.arrived(self.k_yy[r])
        m.sent()


def gather_sems(reach):
    dma = pltpu.SemaphoreType.DMA
    return [dma((9 * reach + 12,)), dma((9 * reach + 12,))]


def place_documents(tab_ref, doc_ref, me):
    docs, tok = tab_ref.shape[-1], doc_ref.shape[-1]
    earlier = doc_ref[...] < lax.broadcasted_iota(jnp.int32, (docs, tok), 0)
    count = dot_nt(jnp.ones((8, tok), BF16), jnp.where(earlier, 1.0, 0.0).astype(BF16))
    tab_ref[me] = count[:1].astype(jnp.int32)


def find_documents(tab_ref, rel_ref, near_ref, which_ref, blk, tok, limits):
    n, _, docs = tab_ref.shape
    starts = jnp.sum(tab_ref[...], axis=0).astype(F32)
    lane = lax.broadcasted_iota(jnp.int32, (1, docs), 1)
    ends = jnp.where(lane == docs - 1, float(n * tok), pltpu.roll(starts, docs - 1, 1))

    def block(pos):
        return jnp.floor((pos + 0.5) * (1.0 / tok))

    span = jnp.max(jnp.where(ends > starts, block(ends - 1.0) - block(starts), 0.0)).astype(jnp.int32)
    which = jnp.int32(0)
    for w in limits:
        which = which + jnp.where(span > w, 1, 0)
    which_ref[0] = which
    cols = rel_ref.shape[1]
    pos = (lax.broadcasted_iota(jnp.int32, (1, cols), 1) % tok + blk * tok).astype(F32)
    column = jnp.broadcast_to(starts, (docs, docs)).T[:, :1]
    first = jnp.max(jnp.where(column <= pos, column, 0.0), axis=0, keepdims=True)
    rel_ref[...] = first.astype(jnp.int32) - blk * tok
    near_ref[0] = blk - block(jnp.min(first)).astype(jnp.int32)
    near_ref[1] = blk % GROUP


def project_kernel(n, reach, limits, x_ref, dy_ref, doc_ref, wq_ref, wk_ref, wv_ref, wo_ref,
                   q_ref, do_ref, k_ref, v_ref, rel_ref, near_ref, which_ref,
                   xs, dys, wq, wk, wv, wo, tab_ref, loc_sem, swap_send, swap_recv, tab_send, tab_recv, *win):
    me = lax.axis_index('cp')
    core = me % 2
    partner = me + 1 - 2 * core
    blk = block_of(me, n)
    place = blk % GROUP
    tok = x_ref.shape[0]
    half = tok // 2
    heads = wq_ref.shape[0]
    hd = wq_ref.shape[2]
    keep = pl.ds(pl.multiple_of(core * half, half), half)
    give = pl.ds(pl.multiple_of((1 - core) * half, half), half)
    loads = [pltpu.make_async_copy(src, dst, loc_sem.at[i]) for i, (src, dst) in enumerate((
        (x_ref.at[keep], xs.at[pl.ds(0, half)]), (wk_ref, wk), (wv_ref, wv), (wq_ref, wq),
        (dy_ref.at[keep], dys.at[pl.ds(0, half)]), (wo_ref, wo)))]
    for c in loads:
        c.start()
    barrier = pltpu.get_barrier_semaphore()
    stages = stages_of(n)
    peers = 0
    for stride, size in stages:
        for j in range(1, size):
            signal(barrier, peer_of(me, stride, size, j))
            peers += 1
    column_signal(barrier, blk, n, reach)
    place_documents(tab_ref, doc_ref, me)
    pl.semaphore_wait(barrier, peers + column_size(blk, n, reach))

    swap_x = remote(x_ref.at[give], xs.at[pl.ds(half, half)], swap_send.at[0], swap_recv.at[0], partner)
    swap_dy = remote(dy_ref.at[give], dys.at[pl.ds(half, half)], swap_send.at[1], swap_recv.at[1], partner)
    swap_x.start()
    swap_dy.start()

    def stage_copies(s):
        stride, size = stages[s]
        rows = pl.ds(me - me % stride, stride)
        return [remote(tab_ref.at[rows], tab_ref.at[rows], tab_send.at[8 * s + j], tab_recv.at[8 * s + j],
                       peer_of(me, stride, size, j)) for j in range(1, size)]

    tables = [stage_copies(s) for s in range(len(stages))]
    for c in tables[0]:
        c.start()
    for c in loads[:3]:
        c.wait()
    swap_x.wait_recv()
    k_ref[place] = dot(xs[...], wk[...]).astype(BF16)
    v_ref[place * (reach + 1)] = dot(xs[...], wv[...]).astype(BF16)
    loads[3].wait()

    def q_head(h):
        q_ref[pl.ds(h * tok, tok), :] = dot(xs[...], wq[h]).astype(BF16)

    q_head(0)
    q_head(1)
    gather = Gather(n, blk, reach, k_ref, v_ref, *win)
    gather.own()
    for h in range(2, heads):
        q_head(h)
    gather.hand_on()
    for s in range(1, len(stages)):
        for c in tables[s - 1]:
            c.wait()
        for c in tables[s]:
            c.start()
        if s == 1:
            loads[4].wait()
            loads[5].wait()
            swap_dy.wait_recv()
            for h in range(heads // 2):
                do_ref[pl.ds(h * tok, tok), :] = dot_nt(dys[...], wo[pl.ds(h * hd, hd), :]).astype(BF16)
    if len(stages) == 1:
        loads[4].wait()
        loads[5].wait()
        swap_dy.wait_recv()
    gather.rest()
    for h in range(heads // 2 if len(stages) > 1 else 0, heads):
        do_ref[pl.ds(h * tok, tok), :] = dot_nt(dys[...], wo[pl.ds(h * hd, hd), :]).astype(BF16)
    for c in tables[-1]:
        c.wait()
    find_documents(tab_ref, rel_ref, near_ref, which_ref, blk, tok, limits)
    swap_x.wait_send()
    swap_dy.wait_send()
    gather.finish()


def gather_kernel(n, reach, k_own_ref, v_own_ref, k_ref, v_ref, loc_sem, *win):
    me = lax.axis_index('cp')
    blk = block_of(me, n)
    place = blk % GROUP
    own = [pltpu.make_async_copy(k_own_ref, k_ref.at[place], loc_sem.at[0]),
           pltpu.make_async_copy(v_own_ref, v_ref.at[place * (reach + 1)], loc_sem.at[1])]
    for c in own:
        c.start()
    barrier = pltpu.get_barrier_semaphore()
    for m in range(1, GROUP):
        signal(barrier, dev_of(blk - place + (place + m) % GROUP, n))
    column_signal(barrier, blk, n, reach)
    pl.semaphore_wait(barrier, 3 + column_size(blk, n, reach))
    for c in own:
        c.wait()
    gather = Gather(n, blk, reach, k_ref, v_ref, *win)
    gather.own()
    gather.hand_on()
    gather.rest()
    gather.finish()


def attend_kernel(reach, keep, nd_ref, start_ref, q_ref, do_ref, k_ref, v_ref, o_ref, dq_ref, dk_ref, dv_ref,
                  q_t, do_t, o_t, dq_t, top, tot, delta, zero, dk_out, dv_out, out_sem, zero_sem, *saved):
    nd = nd_ref[0]
    place = nd_ref[1]
    slots, tok, hd = k_ref.shape
    cols = q_ref.shape[0]
    scale = hd ** -0.5
    base2 = scale * LOG2_E

    def slots_of(d):
        if not reach:
            return d, d
        back = (d + GROUP - 1 - place) // GROUP
        spot = place - d + GROUP * back
        return GROUP * back + spot, spot * (reach + 1) + back

    def rows(d):
        return pl.ds(pl.multiple_of(d * tok, tok), tok)

    zero[...] = jnp.zeros_like(zero)

    def each_empty(act):
        def step(i, _):
            if reach:
                d = place + GROUP * (i // GROUP) - i % GROUP
                empty = (d < 0) | (d > nd)
                where = (i, (i % GROUP) * (reach + 1) + i // GROUP)
            else:
                empty = i > nd
                where = (i, i)

            @pl.when(empty)
            def _():
                for ref, slot in zip((dk_ref, dv_ref), where):
                    act(pltpu.make_async_copy(zero, ref.at[slot], zero_sem))
            return 0
        lax.fori_loop(0, slots, step, 0)

    each_empty(lambda c: c.start())
    q_t[...] = q_ref[...].T
    do_t[...] = do_ref[...].T
    top[...] = jnp.full_like(top, NEG_BIG)
    tot[...] = jnp.zeros_like(tot)
    o_t[...] = jnp.zeros_like(o_t)
    dq_t[...] = jnp.zeros_like(dq_t)

    def split(size):
        return [(lo, min(size, cols - lo)) for lo in range(0, cols, size)]

    def scores(k, d, lo, size, own):
        part = pl.ds(lo, size)
        s = dot(k, q_t[:, part])
        u = lax.broadcasted_iota(jnp.int32, (tok, size), 0)
        visible = u >= start_ref[:, part] + d * tok
        if own:
            t = (lax.broadcasted_iota(jnp.int32, (1, size), 1) + lo) % tok
            visible = visible & (u <= t + d * tok)
        return jnp.where(visible, s, NEG_BIG)

    def weight(s, part):
        return jnp.exp2(s * base2 - top[:, part])

    def find_top(d, own):
        k = k_ref[slots_of(d)[0]]
        for lo, size in split(WIDE):
            part = pl.ds(lo, size)
            s = scores(k, d, lo, size, own)
            top[:, part] = jnp.maximum(top[:, part], jnp.max(s, axis=0, keepdims=True))
            if keep:
                saved[0][rows(d), part] = s

    def find_total(d, own):
        k = None if keep else k_ref[slots_of(d)[0]]
        for lo, size in split(WIDE):
            part = pl.ds(lo, size)
            e = weight(saved[0][rows(d), part] if keep else scores(k, d, lo, size, own), part)
            tot[:, part] += jnp.sum(e, axis=0, keepdims=True)
            if keep:
                saved[0][rows(d), part] = e

    def forward(d, own):
        vt = v_ref[slots_of(d)[1]].T
        k = None if keep else k_ref[slots_of(d)[0]]
        for lo, size in split(CHUNK):
            part = pl.ds(lo, size)
            e = saved[0][rows(d), part] if keep else weight(scores(k, d, lo, size, own), part)
            p = (e * tot[:, part]).astype(BF16)
            if keep:
                saved[1][rows(d), part] = p
            o_t[:, part] += dot(vt, p)

    def outputs(d):
        buf = d % 2
        return [pltpu.make_async_copy(out.at[buf], ref.at[slot], out_sem.at[i, buf])
                for i, (out, ref, slot) in enumerate(zip((dk_out, dv_out), (dk_ref, dv_ref), slots_of(d)))]

    def backward(d, own):
        @pl.when(d > 1)
        def _():
            for c in outputs(d - 2):
                c.wait()

        k, v = k_ref[slots_of(d)[0]], v_ref[slots_of(d)[1]]
        kt = k.T
        dk = dv = jnp.zeros((tok, hd), F32)
        for lo, size in split(WIDE):
            part = pl.ds(lo, size)
            if keep:
                p = saved[1][rows(d), part]
            else:
                p = (weight(scores(k, d, lo, size, own), part) * tot[:, part]).astype(BF16)
            dp = dot(v, do_t[:, part])
            ds = (p.astype(F32) * (dp - delta[:, part])).astype(BF16)
            dq_t[:, part] += dot(kt, ds)
            dk += dot(ds, q_ref[part, :])
            dv += dot(p, do_ref[part, :])
        dk_out[d % 2] = dk * scale
        dv_out[d % 2] = dv
        for c in outputs(d):
            c.start()

    def over_blocks(step, first):
        def body(d, _):
            step(d, not first)
            return 0

        if first:
            step(0, True)
        lax.fori_loop(int(first), nd + 1, body, 0)

    over_blocks(find_top, keep)
    top[...] = top[...] * base2
    over_blocks(find_total, False)
    tot[...] = 1.0 / tot[...]
    over_blocks(forward, False)
    o_bf = o_t[...].astype(BF16)
    delta[...] = jnp.sum(o_bf.astype(F32) * do_t[...].astype(F32), axis=0, keepdims=True)
    o_ref[...] = o_bf.T
    over_blocks(backward, False)
    dq_ref[...] = (dq_t[...] * scale).astype(BF16).T

    @pl.when(nd > 0)
    def _():
        for c in outputs(nd - 1):
            c.wait()

    for c in outputs(nd):
        c.wait()
    each_empty(lambda c: c.wait())


class Scatter:
    def __init__(self, n, blk, reach, width, dk_ref, dv_ref, acc_k, acc_v, bufs, sems):
        place = blk % GROUP
        base = blk - place
        depth = reach + 1
        self.place, self.acc_k, self.acc_v = place, acc_k, acc_v
        self.rows = rows = (width + 3) // GROUP
        self.near_k, self.in_k, self.in_k1, self.in_k3, self.in_kx, self.side_v, self.in_v, self.in_v1, self.in_v3 = bufs
        self.m = m = Moves(*sems)

        def mate(r):
            return dev_of(base + (place + r) % GROUP, n)

        def earlier(dy):
            return dev_of(jnp.maximum(blk - GROUP * dy, 0), n)

        def down(dy):
            return blk - GROUP * dy >= 0

        def up(dy):
            return blk + GROUP * dy < n

        both = up(1) & down(1)
        self.first = first = {dy: max(0, GROUP * dy - width) for dy in range(1, rows + 1)}
        self.straight = list(range(3, rows + 1))

        def span(dy, lead=0):
            return pl.ds(lead + first[dy], GROUP - first[dy])

        self.k_yy = m.new(dk_ref.at[span(2, 8)], self.in_k.at[span(2)], earlier(1), down(2), both) if rows > 1 else None
        self.k_y = {dy: m.new(dk_ref.at[span(dy, GROUP * dy)], self.in_k3.at[dy - 3, span(dy)], earlier(dy), down(dy), up(dy))
                    for dy in self.straight}
        self.k_y1 = m.new(self.near_k, self.in_k1, earlier(1), down(1), up(1))
        self.k_xx = m.new(acc_k.at[(place + 2) % GROUP], self.in_kx.at[0], mate(3))
        self.k_xu = m.new(acc_k.at[(place + 1) % GROUP], self.in_kx.at[1], mate(1))
        self.k_xd = m.new(acc_k.at[(place + 3) % GROUP], self.in_kx.at[2], mate(3))
        def col(r):
            return dv_ref.at[pl.ds(((place + r) % GROUP) * depth, rows + 1)]

        self.v_xx = m.new(col(2), self.in_v.at[0], mate(3))
        self.v_xu = m.new(col(1), self.in_v.at[1], mate(1))
        self.v_xd = m.new(self.side_v, self.in_v.at[2], mate(3))
        self.v_yy = m.new(acc_v.at[2], self.in_v1.at[0], earlier(1), down(2), both) if rows > 1 else None
        self.v_y = {dy: m.new(acc_v.at[dy], self.in_v3.at[dy - 3], earlier(dy), down(dy), up(dy)) for dy in self.straight}
        self.v_y1 = m.new(acc_v.at[1], self.in_v1.at[1], earlier(1), down(1), up(1))

    def start(self):
        m = self.m
        m.start(self.v_xx)
        if self.k_yy is not None:
            m.start(self.k_yy)
        m.start(self.v_xu)
        for dy in self.straight:
            m.start(self.k_y[dy])

    def run(self):
        m, acc_k, acc_v, first = self.m, self.acc_k, self.acc_v, self.first

        def add_far_k():
            rows = pl.ds(first[2], GROUP - first[2])
            self.near_k[rows] += self.in_k[rows]

        def add_k3(dy):
            rows = pl.ds(first[dy], GROUP - first[dy])
            acc_k[rows] += self.in_k3[dy - 3, rows]

        def add_k1():
            acc_k[...] += self.in_k1[...]

        def add_far_v():
            acc_v[1] += self.in_v1[0]

        def add_v1():
            acc_v[0] += self.in_v1[1]

        def add_v3(dy):
            acc_v[0] += self.in_v3[dy - 3]

        m.arrived(self.v_xx)
        self.side_v[...] += self.in_v[0]
        m.start(self.v_xd)
        if self.k_yy is not None:
            m.arrived(self.k_yy, add_far_k)
        m.start(self.k_y1)
        m.arrived(self.v_xu)
        acc_v[...] += self.in_v[1]
        for dy in self.straight:
            m.arrived(self.k_y[dy], functools.partial(add_k3, dy))
        m.arrived(self.v_xd)
        acc_v[...] += self.in_v[2]
        if self.v_yy is not None:
            m.start(self.v_yy)
        for dy in self.straight:
            m.start(self.v_y[dy])
        m.arrived(self.k_y1, add_k1)
        m.start(self.k_xx)
        m.start(self.k_xu)
        if self.v_yy is not None:
            m.arrived(self.v_yy, add_far_v)
        m.start(self.v_y1)
        m.arrived(self.k_xx)
        acc_k[(self.place + 3) % GROUP] += self.in_kx[0]
        m.start(self.k_xd)
        for dy in self.straight:
            m.arrived(self.v_y[dy], functools.partial(add_v3, dy))
        m.arrived(self.v_y1, add_v1)
        m.arrived(self.k_xu)
        m.arrived(self.k_xd)
        return acc_k[self.place] + self.in_kx[1] + self.in_kx[2]


def scatter_bufs(width, tok, hd):
    rows = (width + 3) // GROUP
    more = max(rows - 2, 1)
    dma = pltpu.SemaphoreType.DMA
    shapes = [(GROUP,), (GROUP,), (GROUP,), (more, GROUP), (3,), (rows + 1,), (3, rows + 1), (2,), (more,)]
    return [pltpu.VMEM((*shape, tok, hd), F32) for shape in shapes] + [dma((2 * rows + 8,)), dma((2 * rows + 8,))]


def finish_kernel(n, reach, width, dk_ref, dv_ref, o_ref, dq_ref, wq_ref, wk_ref, wv_ref, wo_ref, y_ref, dx_ref,
                  acc_k, acc_v, o, dq, wq, wk, wv, wo, y_give, dx_give, dx_part, loc_sem, swap_send, swap_recv, *win):
    me = lax.axis_index('cp')
    core = me % 2
    partner = me + 1 - 2 * core
    blk = block_of(me, n)
    place = blk % GROUP
    base = blk - place
    tok = y_ref.shape[0]
    half = tok // 2
    heads, d_model, hd = wq_ref.shape
    rows = (width + 3) // GROUP
    depth = reach + 1
    mine = pl.ds(pl.multiple_of(core * half, half), half)
    if reach:
        bufs, sems = win[:9], win[9:]
        terms = [(dv_ref.at[pl.ds(((place + 3) % GROUP) * depth, rows + 1)], bufs[5]), (dk_ref.at[pl.ds(4, GROUP)], bufs[0]),
                 (dv_ref.at[pl.ds(place * depth, rows + 1)], acc_v), (dk_ref.at[pl.ds(0, GROUP)], acc_k)]
    else:
        terms = [(dv_ref, acc_v), (dk_ref, acc_k)]
    pairs = terms + [(o_ref, o), (wo_ref, wo), (dq_ref, dq), (wq_ref, wq), (wk_ref, wk), (wv_ref, wv)]
    loads = [pltpu.make_async_copy(src, dst, loc_sem.at[i]) for i, (src, dst) in enumerate(pairs)]
    for c in loads:
        c.start()
    barrier = pltpu.get_barrier_semaphore()
    signal(barrier, partner)
    if reach:
        for r in (1, 3):
            signal(barrier, dev_of(base + (place + r) % GROUP, n))
        column_signal(barrier, blk, n, rows)
        pl.semaphore_wait(barrier, 3 + column_size(blk, n, rows))
        scatter = Scatter(n, blk, reach, width, dk_ref, dv_ref, acc_k, acc_v, bufs, sems)
        scatter.start()
    else:
        pl.semaphore_wait(barrier, 1)
    for c in loads[-6:-4]:
        c.wait()
    o_cat = jnp.concatenate([o[pl.ds(h * tok, tok), :] for h in range(heads)], axis=1)
    y = dot(o_cat, wo[...]).astype(BF16)
    y_give[...] = y[half:]
    y_ref[mine, :] = y[:half]
    for c in loads[-4:-2]:
        c.wait()
    dx = dot_nt(dq[pl.ds(0, tok), :], wq[0])
    for h in range(1, heads):
        dx += dot_nt(dq[pl.ds(h * tok, tok), :], wq[h])
    dx_part[...] = dx
    swap_y = remote(y_give, y_ref.at[mine], swap_send.at[0], swap_recv.at[0], partner)
    swap_y.start()
    for c in loads[:-6] + loads[-2:]:
        c.wait()
    total_k = scatter.run() if reach else acc_k[0]
    dk = total_k.astype(BF16)
    dv = acc_v[0].astype(BF16)

    def dx_rows(lo):
        part = slice(lo, lo + half)
        return (dx_part[pl.ds(lo, half), :] + dot_nt(dk[part], wk[...]) + dot_nt(dv[part], wv[...])).astype(BF16)

    dx_give[...] = dx_rows(half)
    dx_ref[mine, :] = dx_rows(0)
    swap_dx = remote(dx_give, dx_ref.at[mine], swap_send.at[1], swap_recv.at[1], partner)
    swap_dx.start()
    if reach:
        scatter.m.sent()
    swap_y.wait()
    swap_dx.wait()


def copy_kernel(y_ref, dx_ref, y_out, dx_out):
    y_out[...] = y_ref[...]
    dx_out[...] = dx_ref[...]


def make_layer(n, widths, far):
    dma = pltpu.SemaphoreType.DMA
    near = widths[-1]

    def comm(cid):
        return pltpu.CompilerParams(collective_id=cid, has_side_effects=True, vmem_limit_bytes=VMEM_LIMIT)

    def local_layer(x_in, dy_in, doc_id, w_q, w_k, w_v, w_o):
        tok, d_model = x_in.shape
        heads, hd = w_q.shape[1], w_q.shape[2]
        cols = heads * tok
        me = lax.axis_index('cp')
        blk = block_of(me, n)
        place = blk % GROUP
        wq = jnp.transpose(w_q, (1, 0, 2))
        wk = w_k.reshape(d_model, hd)
        wv = w_v.reshape(d_model, hd)
        wo = w_o.reshape(heads * hd, d_model)
        n_stage = len(stages_of(n))
        reach = (near + 3) // GROUP

        def window(reach, dtype=BF16):
            return jax.ShapeDtypeStruct((GROUP * (reach + 1), tok, hd), dtype)

        q, do, k_win, v_win, rel, nd, which = pl.pallas_call(
            functools.partial(project_kernel, n, reach, (*widths, far)),
            out_shape=(jax.ShapeDtypeStruct((cols, hd), BF16), jax.ShapeDtypeStruct((cols, hd), BF16),
                       window(reach), window(reach), jax.ShapeDtypeStruct((1, cols), jnp.int32),
                       jax.ShapeDtypeStruct((2,), jnp.int32), jax.ShapeDtypeStruct((1,), jnp.int32)),
            in_specs=[HBM, HBM, VMEM, HBM, HBM, HBM, HBM],
            out_specs=(VMEM, VMEM, VMEM, VMEM, VMEM, SMEM, SMEM),
            scratch_shapes=[pltpu.VMEM((tok, d_model), BF16), pltpu.VMEM((tok, d_model), BF16),
                            pltpu.VMEM(wq.shape, BF16), pltpu.VMEM(wk.shape, BF16), pltpu.VMEM(wv.shape, BF16),
                            pltpu.VMEM(wo.shape, BF16), pltpu.VMEM((n, 1, 128), jnp.int32),
                            dma((6,)), dma((2,)), dma((2,)), dma((8 * n_stage,)), dma((8 * n_stage,))] + gather_sems(reach),
            compiler_params=comm(0),
            name='project',
        )(x_in, dy_in, doc_id.reshape(1, tok), wq, wk, wv, wo)

        def attend(k, v, width, reach):
            saved = []
            if width:
                saved = [pltpu.VMEM(((width + 1) * tok, cols), F32), pltpu.VMEM(((width + 1) * tok, cols), BF16)]
            row = pltpu.VMEM((1, cols), F32)
            return pl.pallas_call(
                functools.partial(attend_kernel, reach, bool(width)),
                out_shape=(jax.ShapeDtypeStruct((cols, hd), BF16), jax.ShapeDtypeStruct((cols, hd), BF16),
                           jax.ShapeDtypeStruct(k.shape, F32), jax.ShapeDtypeStruct(k.shape, F32)),
                in_specs=[SMEM, VMEM, VMEM, VMEM, VMEM, VMEM],
                out_specs=(VMEM, VMEM, HBM, HBM),
                scratch_shapes=[pltpu.VMEM((hd, cols), BF16), pltpu.VMEM((hd, cols), BF16),
                                pltpu.VMEM((hd, cols), F32), pltpu.VMEM((hd, cols), F32),
                                row, row, row, pltpu.VMEM((tok, hd), F32), pltpu.VMEM((2, tok, hd), F32),
                                pltpu.VMEM((2, tok, hd), F32), dma((2, 2)), dma] + saved,
                compiler_params=pltpu.CompilerParams(vmem_limit_bytes=VMEM_LIMIT),
                name='attend',
            )(nd, rel, q, do, k, v)

        def finish(dk, dv, o, dq, reach, width, cid):
            rows = (width + 3) // GROUP
            win = scatter_bufs(width, tok, hd) if reach else []
            return pl.pallas_call(
                functools.partial(finish_kernel, n, reach, width),
                out_shape=(jax.ShapeDtypeStruct((tok, d_model), BF16), jax.ShapeDtypeStruct((tok, d_model), BF16)),
                in_specs=[HBM] * 8,
                out_specs=(VMEM, VMEM),
                scratch_shapes=[pltpu.VMEM((4 if reach else 1, tok, hd), F32), pltpu.VMEM((rows + 1, tok, hd), F32),
                                pltpu.VMEM((cols, hd), BF16), pltpu.VMEM((cols, hd), BF16),
                                pltpu.VMEM(wq.shape, BF16), pltpu.VMEM(wk.shape, BF16), pltpu.VMEM(wv.shape, BF16),
                                pltpu.VMEM(wo.shape, BF16), pltpu.VMEM((tok // 2, d_model), BF16),
                                pltpu.VMEM((tok // 2, d_model), BF16), pltpu.VMEM((tok, d_model), F32),
                                dma((10,)), dma((2,)), dma((2,))] + win,
                compiler_params=comm(cid),
                name='finish',
            )(dk, dv, o, dq, wq, wk, wv, wo)

        def with_near(width, cid):
            def run(k, v):
                o, dq, dk, dv = attend(k, v, near, reach)
                return finish(dk, dv, o, dq, reach, width, cid)
            return run

        def own(k, v):
            return (lax.dynamic_index_in_dim(k, place, 0, keepdims=False),
                    lax.dynamic_index_in_dim(v, place * (reach + 1), 0, keepdims=False))

        def with_far(k, v):
            reach = (far + 3) // GROUP
            k, v = pl.pallas_call(
                functools.partial(gather_kernel, n, reach),
                out_shape=(window(reach), window(reach)),
                in_specs=[HBM, HBM], out_specs=(HBM, HBM),
                scratch_shapes=[dma((2,))] + gather_sems(reach),
                compiler_params=comm(1),
                name='gather',
            )(*own(k, v))
            o, dq, dk, dv = attend(k, v, far, reach)
            return finish(dk, dv, o, dq, reach, far, 2)

        order = [2 * b if b < n // 2 else 2 * (n - 1 - b) + 1 for b in range(n)]
        up = [(order[b], order[(b + 1) % n]) for b in range(n)]
        down = [(dst, src) for src, dst in up]

        def with_all(k, v):
            def pull(d, state):
                held, k, v = state
                held = lax.ppermute(held, 'cp', up)
                return held, k.at[d].set(held[0]), v.at[d].set(held[1])

            held = jnp.stack(own(k, v))
            empty = jnp.zeros((n, tok, hd), BF16)
            _, k, v = lax.fori_loop(1, n, pull, (held, empty.at[0].set(held[0]), empty.at[0].set(held[1])))
            o, dq, dk, dv = attend(k, v, 0, 0)

            def push(step, acc):
                d = n - 1 - step
                acc = acc + jnp.stack([lax.dynamic_index_in_dim(dk, d, 0, keepdims=False),
                                       lax.dynamic_index_in_dim(dv, d, 0, keepdims=False)])
                return lax.ppermute(acc, 'cp', down)

            acc = lax.fori_loop(0, n - 1, push, jnp.zeros((2, tok, hd), F32))
            return finish((acc[0] + dk[0])[None], (acc[1] + dv[0])[None], o, dq, 0, 0, 3)

        branches = [with_near(w, 4 + i) for i, w in enumerate(widths)] + [with_far, with_all]
        y, dx = lax.switch(which[0], branches, k_win, v_win)
        part = pl.BlockSpec((tok // 4, d_model), lambda i: (i, 0))
        return pl.pallas_call(
            copy_kernel, grid=(4,), out_shape=(jax.ShapeDtypeStruct(y.shape, BF16),) * 2,
            in_specs=[part, part], out_specs=(part, part), name='copy')(y, dx)

    return local_layer


def solution(mesh, widths=WIDTHS, far=FAR):
    n = mesh.shape['cp']
    row_spec = P(('dp', 'cp'))
    full_spec = P()
    return jax.shard_map(make_layer(n, widths, far), mesh=mesh,
                         in_specs=(row_spec, row_spec, row_spec, full_spec, full_spec, full_spec, full_spec),
                         out_specs=(row_spec, row_spec), check_vma=False)
```

```python
import functools

import jax
import jax.numpy as jnp
from jax import lax
from jax.experimental import pallas as pl
from jax.experimental.pallas import tpu as pltpu
from jax.sharding import PartitionSpec as P

NEG_BIG = -1.0e30
GROUP = 4
MESH = pl.DeviceIdType.MESH
WIDTHS, FAR, CHUNK, WIDE = (8, 9, 10, 12), 24, 256, 384
LOG2_E = 1.4426950408889634
F32, BF16 = jnp.float32, jnp.bfloat16
HBM = pl.BlockSpec(memory_space=pl.ANY)
VMEM = pl.BlockSpec(memory_space=pltpu.VMEM)
SMEM = pl.BlockSpec(memory_space=pltpu.SMEM)
VMEM_LIMIT = 60 * 1024 * 1024


def dot(a, b):
    return jnp.dot(a, b, preferred_element_type=F32)


def dot_nt(a, b):
    return lax.dot_general(a, b, (((1,), (1,)), ((), ())), preferred_element_type=F32)


def dot_tn(a, b):
    return lax.dot_general(a, b, (((0,), (0,)), ((), ())), preferred_element_type=F32)


def block_of(dev, n):
    return jnp.where(dev % 2 == 0, dev // 2, n - 1 - dev // 2)


def dev_of(blk, n):
    return jnp.where(blk < n // 2, 2 * blk, 2 * (n - 1 - blk) + 1)


def at(dev):
    return (lax.axis_index('dp'), dev)


def stages_of(n):
    out, stride = [(1, min(n, 8))], min(n, 8)
    while stride < n:
        size = min(4, n // stride)
        out.append((stride, size))
        stride *= size
    return out


def peer_of(me, stride, size, j):
    idx = (me // stride) % size
    return me - idx * stride + ((idx + j) % size) * stride


def remote(src, dst, send, recv, dev):
    return pltpu.make_async_remote_copy(src_ref=src, dst_ref=dst, send_sem=send, recv_sem=recv,
                                        device_id=at(dev), device_id_type=MESH)


def column(blk, n, reach):
    out = []
    for dy in range(1, reach + 1):
        out.append((blk - GROUP * dy, blk - GROUP * dy >= 0))
        out.append((blk + GROUP * dy, blk + GROUP * dy < n))
    return out


def signal(barrier, dev):
    pl.semaphore_signal(barrier, inc=1, device_id=at(dev), device_id_type=MESH)


def column_signal(barrier, blk, n, reach):
    for other, there in column(blk, n, reach):
        @pl.when(there)
        def _():
            signal(barrier, dev_of(other, n))


def column_size(blk, n, reach):
    return jnp.minimum((n - 1 - blk) // GROUP, reach) + jnp.minimum(blk // GROUP, reach)


class Moves:
    def __init__(self, send, recv):
        self.sems, self.copies = (send, recv), []

    def new(self, src, dst, dev, go=None, come=None):
        i = len(self.copies)
        self.copies.append((remote(src, dst, self.sems[0].at[i], self.sems[1].at[i], dev), go, come))
        return i

    def when(self, cond, act):
        if cond is None:
            act()
        else:
            pl.when(cond)(act)

    def start(self, i):
        copy, go, _ = self.copies[i]
        self.when(go, copy.start)

    def arrived(self, i, then=None):
        copy, _, come = self.copies[i]

        def act():
            copy.wait_recv()
            if then is not None:
                then()
        self.when(come, act)

    def sent(self):
        for copy, go, _ in self.copies:
            self.when(go, copy.wait_send)


class Gather:
    def __init__(self, n, blk, reach, k_ref, v_ref, send, recv):
        place = blk % GROUP
        base = blk - place
        depth = reach + 1
        self.m = m = Moves(send, recv)

        def mate(r):
            return dev_of(base + (place + r) % GROUP, n)

        def later(dy):
            return dev_of(jnp.minimum(blk + GROUP * dy, n - 1), n)

        def k_at(dy, r):
            return k_ref.at[GROUP * dy + (place + r) % GROUP]

        def v_at(r, dy):
            return v_ref.at[((place + r) % GROUP) * depth + dy]

        def up(dy):
            return blk + GROUP * dy < n

        def down(dy):
            return blk - GROUP * dy >= 0

        both = up(1) & down(1)
        mid = down(2)
        self.straight = [dy for dy in range(1, reach + 1) if dy != 2]
        self.k_x = {r: m.new(k_at(0, 0), k_at(0, 0), mate(r)) for r in (1, 3)}
        self.k_xx = m.new(k_at(0, 3), k_at(0, 3), mate(1))
        self.k_y = {(dy, r): m.new(k_at(0, r), k_at(dy, r), later(dy), up(dy), down(dy)) for dy in self.straight for r in range(GROUP)}
        self.v_y = {dy: m.new(v_at(0, 0), v_at(0, dy), later(dy), up(dy), down(dy)) for dy in self.straight}
        rows = [(0, None)] + [(dy, down(dy)) for dy in range(1, reach + 1)]
        self.v_x = {(dy, r): m.new(v_at(0, dy), v_at(0, dy), mate(r), c, c) for dy, c in rows for r in (1, 3)}
        self.v_xx = {dy: m.new(v_at(3, dy), v_at(3, dy), mate(1), c, c) for dy, c in rows}
        if reach > 1:
            self.k_yy = {r: m.new(k_at(1, r), k_at(2, r), later(1), both, mid) for r in range(GROUP)}
            self.v_yy = m.new(v_at(0, 1), v_at(0, 2), later(1), both, mid)
        self.reach = reach

    def own(self):
        m = self.m
        for r in (1, 3):
            m.start(self.k_x[r])
        self.k_on(0)
        for dy in self.straight:
            m.start(self.v_y[dy])
        self.v_on(0)

    def k_on(self, r):
        for dy in self.straight:
            self.m.start(self.k_y[dy, r])

    def v_on(self, dy):
        for r in (1, 3):
            self.m.start(self.v_x[dy, r])

    def hand_on(self):
        m = self.m
        m.arrived(self.k_x[1])
        m.start(self.k_xx)
        self.k_on(3)
        m.arrived(self.v_y[1])
        if self.reach > 1:
            m.start(self.v_yy)
        self.v_on(1)
        m.arrived(self.k_x[3])
        self.k_on(1)
        for dy in self.straight[1:]:
            m.arrived(self.v_y[dy])
            self.v_on(dy)
        m.arrived(self.v_x[0, 1])
        m.start(self.v_xx[0])
        m.arrived(self.k_y[1, 0])
        if self.reach > 1:
            m.start(self.k_yy[0])
        m.arrived(self.k_xx)
        self.k_on(2)
        if self.reach > 1:
            m.arrived(self.v_yy)
            self.v_on(2)

    def rest(self):
        m = self.m
        order = [1] + self.straight[1:] + ([2] if self.reach > 1 else [])
        for i in range(max(len(order), 3)):
            if i < len(order):
                m.arrived(self.v_x[order[i], 1])
                m.start(self.v_xx[order[i]])
            if i < 3:
                r = (3, 1, 2)[i]
                m.arrived(self.k_y[1, r])
                if self.reach > 1:
                    m.start(self.k_yy[r])

    def finish(self):
        m = self.m
        for dy in self.straight[1:]:
            for r in range(GROUP):
                m.arrived(self.k_y[dy, r])
        for dy in range(self.reach + 1):
            m.arrived(self.v_x[dy, 3])
            m.arrived(self.v_xx[dy])
        if self.reach > 1:
            for r in range(GROUP):
                m.arrived(self.k_yy[r])
        m.sent()


def gather_sems(reach):
    dma = pltpu.SemaphoreType.DMA
    return [dma((9 * reach + 12,)), dma((9 * reach + 12,))]


def place_documents(tab_ref, doc_ref, me):
    docs, tok = tab_ref.shape[-1], doc_ref.shape[-1]
    earlier = doc_ref[...] < lax.broadcasted_iota(jnp.int32, (docs, tok), 0)
    count = dot_nt(jnp.ones((8, tok), BF16), jnp.where(earlier, 1.0, 0.0).astype(BF16))
    tab_ref[me] = count[:1].astype(jnp.int32)


def find_documents(tab_ref, rel_ref, near_ref, which_ref, blk, tok, limits):
    n, _, docs = tab_ref.shape
    starts = jnp.sum(tab_ref[...], axis=0).astype(F32)
    lane = lax.broadcasted_iota(jnp.int32, (1, docs), 1)
    ends = jnp.where(lane == docs - 1, float(n * tok), pltpu.roll(starts, docs - 1, 1))

    def block(pos):
        return jnp.floor((pos + 0.5) * (1.0 / tok))

    span = jnp.max(jnp.where(ends > starts, block(ends - 1.0) - block(starts), 0.0)).astype(jnp.int32)
    which = jnp.int32(0)
    for w in limits:
        which = which + jnp.where(span > w, 1, 0)
    which_ref[0] = which
    cols = rel_ref.shape[1]
    pos = (lax.broadcasted_iota(jnp.int32, (1, cols), 1) % tok + blk * tok).astype(F32)
    column = jnp.broadcast_to(starts, (docs, docs)).T[:, :1]
    first = jnp.max(jnp.where(column <= pos, column, 0.0), axis=0, keepdims=True)
    rel_ref[...] = first.astype(jnp.int32) - blk * tok
    near_ref[0] = blk - block(jnp.min(first)).astype(jnp.int32)
    near_ref[1] = blk % GROUP


def project_kernel(n, reach, limits, x_ref, dy_ref, doc_ref, wq_ref, wk_ref, wv_ref, wo_ref,
                   q_ref, do_ref, k_ref, v_ref, rel_ref, near_ref, which_ref,
                   xs, dys, wq, wk, wv, wo, own_kv, own_q, own_do, tab_ref, loc_sem, swap_send, swap_recv,
                   tab_send, tab_recv, *win):
    me = lax.axis_index('cp')
    core = me % 2
    partner = me + 1 - 2 * core
    blk = block_of(me, n)
    place = blk % GROUP
    tok = x_ref.shape[0]
    half = tok // 2
    heads, _, hd = wq_ref.shape
    depth = reach + 1
    keep = pl.ds(pl.multiple_of(core * half, half), half)
    give = pl.ds(pl.multiple_of((1 - core) * half, half), half)
    front, back = pl.ds(0, half), pl.ds(half, half)
    loads = [pltpu.make_async_copy(src, dst, loc_sem.at[i]) for i, (src, dst) in enumerate((
        (x_ref, xs), (wk_ref, wk), (wv_ref, wv), (wq_ref, wq), (dy_ref, dys), (wo_ref, wo)))]
    for c in loads:
        c.start()
    barrier = pltpu.get_barrier_semaphore()
    stages = stages_of(n)
    peers = 0
    for stride, size in stages:
        for j in range(1, size):
            signal(barrier, peer_of(me, stride, size, j))
            peers += 1
    column_signal(barrier, blk, n, reach)
    place_documents(tab_ref, doc_ref, me)

    def stage_copies(s):
        stride, size = stages[s]
        rows = pl.ds(me - me % stride, stride)
        return [remote(tab_ref.at[rows], tab_ref.at[rows], tab_send.at[8 * s + j], tab_recv.at[8 * s + j],
                       peer_of(me, stride, size, j)) for j in range(1, size)]

    def q_heads(some):
        for h in some:
            own_q[h] = dot(xs[...], wq[h]).astype(BF16)
            q_ref[h, front, :] = own_q[h, keep, :]

    tables = [stage_copies(s) for s in range(len(stages))]
    other = GROUP - 1 - place
    swaps = [remote(src, dst, swap_send.at[i], swap_recv.at[i], partner) for i, (src, dst) in enumerate((
        (own_kv.at[0, give], k_ref.at[other, back]), (own_kv.at[1, give], v_ref.at[other * depth, back]),
        (own_q.at[:, give], q_ref.at[:, back]), (own_do.at[:, give], do_ref.at[:, back])))]
    gather = Gather(n, blk, reach, k_ref, v_ref, *win)

    def next_table(s):
        if s < len(stages):
            for c in tables[s - 1]:
                c.wait()
            for c in tables[s]:
                c.start()

    for c in loads[:3]:
        c.wait()
    own_kv[0] = dot(xs[...], wk[...]).astype(BF16)
    own_kv[1] = dot(xs[...], wv[...]).astype(BF16)
    k_ref[place, front, :] = own_kv[0, keep, :]
    v_ref[place * depth, front, :] = own_kv[1, keep, :]
    loads[3].wait()
    q_heads(range(1))
    pl.semaphore_wait(barrier, peers + column_size(blk, n, reach))
    for c in swaps[:2] + tables[0]:
        c.start()
    q_heads(range(1, heads))
    for c in swaps[:2]:
        c.wait_recv()
    gather.own()
    loads[4].wait()
    loads[5].wait()
    for h in range(heads):
        own_do[h] = dot_nt(dys[...], wo[pl.ds(h * hd, hd), :]).astype(BF16)
        do_ref[h, front, :] = own_do[h, keep, :]
    swaps[2].start()
    next_table(1)
    gather.hand_on()
    swaps[3].start()
    next_table(2)
    gather.rest()
    for c in tables[-1]:
        c.wait()
    find_documents(tab_ref, rel_ref, near_ref, which_ref, blk, tok, limits)
    gather.finish()
    for c in swaps[2:]:
        c.wait_recv()
    for c in swaps:
        c.wait_send()


def gather_kernel(n, reach, k_own_ref, v_own_ref, k_ref, v_ref, loc_sem, *win):
    me = lax.axis_index('cp')
    blk = block_of(me, n)
    place = blk % GROUP
    own = [pltpu.make_async_copy(k_own_ref, k_ref.at[place], loc_sem.at[0]),
           pltpu.make_async_copy(v_own_ref, v_ref.at[place * (reach + 1)], loc_sem.at[1])]
    for c in own:
        c.start()
    barrier = pltpu.get_barrier_semaphore()
    for m in range(1, GROUP):
        signal(barrier, dev_of(blk - place + (place + m) % GROUP, n))
    column_signal(barrier, blk, n, reach)
    pl.semaphore_wait(barrier, 3 + column_size(blk, n, reach))
    for c in own:
        c.wait()
    gather = Gather(n, blk, reach, k_ref, v_ref, *win)
    gather.own()
    gather.hand_on()
    gather.rest()
    gather.finish()


def attend_kernel(reach, keep, nd_ref, start_ref, q_ref, do_ref, k_ref, v_ref, o_ref, dq_ref, dk_ref, dv_ref,
                  q_t, do_t, o_t, dq_t, top, tot, delta, zero, dk_out, dv_out, out_sem, zero_sem, *saved):
    nd = nd_ref[0]
    place = nd_ref[1]
    slots, tok, hd = k_ref.shape
    cols = q_ref.shape[0]
    scale = hd ** -0.5
    base2 = scale * LOG2_E

    def slots_of(d):
        if not reach:
            return d, d
        back = (d + GROUP - 1 - place) // GROUP
        spot = place - d + GROUP * back
        return GROUP * back + spot, spot * (reach + 1) + back

    def rows(d):
        return pl.ds(pl.multiple_of(d * tok, tok), tok)

    zero[...] = jnp.zeros_like(zero)

    def each_empty(act):
        def step(i, _):
            if reach:
                d = place + GROUP * (i // GROUP) - i % GROUP
                empty = (d < 0) | (d > nd)
                where = (i, (i % GROUP) * (reach + 1) + i // GROUP)
            else:
                empty = i > nd
                where = (i, i)

            @pl.when(empty)
            def _():
                for ref, slot in zip((dk_ref, dv_ref), where):
                    act(pltpu.make_async_copy(zero, ref.at[slot], zero_sem))
            return 0
        lax.fori_loop(0, slots, step, 0)

    each_empty(lambda c: c.start())
    q_t[...] = q_ref[...].T
    do_t[...] = do_ref[...].T
    top[...] = jnp.full_like(top, NEG_BIG)
    tot[...] = jnp.zeros_like(tot)
    o_t[...] = jnp.zeros_like(o_t)
    dq_t[...] = jnp.zeros_like(dq_t)

    def split(size):
        return [(lo, min(size, cols - lo)) for lo in range(0, cols, size)]

    def scores(k, d, lo, size, own):
        part = pl.ds(lo, size)
        s = dot(k, q_t[:, part])
        u = lax.broadcasted_iota(jnp.int32, (tok, size), 0)
        visible = u >= start_ref[:, part] + d * tok
        if own:
            t = (lax.broadcasted_iota(jnp.int32, (1, size), 1) + lo) % tok
            visible = visible & (u <= t + d * tok)
        return jnp.where(visible, s, NEG_BIG)

    def weight(s, part):
        return jnp.exp2(s * base2 - top[:, part])

    def find_top(d, own):
        k = k_ref[slots_of(d)[0]]
        for lo, size in split(WIDE):
            part = pl.ds(lo, size)
            s = scores(k, d, lo, size, own)
            top[:, part] = jnp.maximum(top[:, part], jnp.max(s, axis=0, keepdims=True))
            if keep:
                saved[0][rows(d), part] = s

    def find_total(d, own):
        k = None if keep else k_ref[slots_of(d)[0]]
        for lo, size in split(WIDE):
            part = pl.ds(lo, size)
            e = weight(saved[0][rows(d), part] if keep else scores(k, d, lo, size, own), part)
            tot[:, part] += jnp.sum(e, axis=0, keepdims=True)
            if keep:
                saved[0][rows(d), part] = e

    def forward(d, own):
        vt = v_ref[slots_of(d)[1]].T
        k = None if keep else k_ref[slots_of(d)[0]]
        for lo, size in split(CHUNK):
            part = pl.ds(lo, size)
            e = saved[0][rows(d), part] if keep else weight(scores(k, d, lo, size, own), part)
            p = (e * tot[:, part]).astype(BF16)
            if keep:
                saved[1][rows(d), part] = p
            o_t[:, part] += dot(vt, p)

    def outputs(d):
        buf = d % 2
        return [pltpu.make_async_copy(out.at[buf], ref.at[slot], out_sem.at[i, buf])
                for i, (out, ref, slot) in enumerate(zip((dk_out, dv_out), (dk_ref, dv_ref), slots_of(d)))]

    def backward(d, own):
        @pl.when(d > 1)
        def _():
            for c in outputs(d - 2):
                c.wait()

        k, v = k_ref[slots_of(d)[0]], v_ref[slots_of(d)[1]]
        kt = k.T
        dk = dv = jnp.zeros((tok, hd), F32)
        for lo, size in split(WIDE):
            part = pl.ds(lo, size)
            if keep:
                p = saved[1][rows(d), part]
            else:
                p = (weight(scores(k, d, lo, size, own), part) * tot[:, part]).astype(BF16)
            dp = dot(v, do_t[:, part])
            ds = (p.astype(F32) * (dp - delta[:, part])).astype(BF16)
            dq_t[:, part] += dot(kt, ds)
            dk += dot(ds, q_ref[part, :])
            dv += dot(p, do_ref[part, :])
        dk_out[d % 2] = dk * scale
        dv_out[d % 2] = dv
        for c in outputs(d):
            c.start()

    def over_blocks(step, first):
        def body(d, _):
            step(d, not first)
            return 0

        if first:
            step(0, True)
        lax.fori_loop(int(first), nd + 1, body, 0)

    over_blocks(find_top, keep)
    top[...] = top[...] * base2
    over_blocks(find_total, False)
    tot[...] = 1.0 / tot[...]
    over_blocks(forward, False)
    o_bf = o_t[...].astype(BF16)
    delta[...] = jnp.sum(o_bf.astype(F32) * do_t[...].astype(F32), axis=0, keepdims=True)
    o_ref[...] = o_bf.T
    over_blocks(backward, False)
    dq_ref[...] = (dq_t[...] * scale).astype(BF16).T

    @pl.when(nd > 0)
    def _():
        for c in outputs(nd - 1):
            c.wait()

    for c in outputs(nd):
        c.wait()
    each_empty(lambda c: c.wait())


class Scatter:
    def __init__(self, n, blk, reach, width, dk_ref, dv_ref, acc_k, acc_v, bufs, sems):
        place = blk % GROUP
        base = blk - place
        depth = reach + 1
        self.place, self.acc_k, self.acc_v = place, acc_k, acc_v
        self.rows = rows = (width + 3) // GROUP
        self.near_k, self.in_k, self.in_k1, self.in_k3, self.in_kx, self.side_v, self.in_v, self.in_v1, self.in_v3 = bufs
        self.m = m = Moves(*sems)

        def mate(r):
            return dev_of(base + (place + r) % GROUP, n)

        def earlier(dy):
            return dev_of(jnp.maximum(blk - GROUP * dy, 0), n)

        def down(dy):
            return blk - GROUP * dy >= 0

        def up(dy):
            return blk + GROUP * dy < n

        def need(dy, place):
            return GROUP * dy - width <= place

        def both_of(a, b):
            return b if a is None else a & b

        def asked(dy, r):
            return None if need(dy, 0) else need(dy, (place + r) % GROUP)

        both = up(1) & down(1)
        here, there = range(rows + 1), [(dy, j) for dy in range(3, rows + 1) for j in range(GROUP) if need(dy, j)]
        self.k_yy = {j: m.new(dk_ref.at[2 * GROUP + j], self.in_k.at[j], earlier(1), down(2), both)
                     for j in range(GROUP) if rows > 1 and need(2, j)}
        self.k_y = {(dy, j): m.new(dk_ref.at[GROUP * dy + j], self.in_k3.at[dy - 3, j], earlier(dy), down(dy), up(dy))
                    for dy, j in there}
        self.k_y1 = [m.new(self.near_k.at[j], self.in_k1.at[j], earlier(1), down(1), up(1)) for j in range(GROUP)]
        self.k_xx = m.new(acc_k.at[(place + 2) % GROUP], self.in_kx.at[0], mate(3))
        self.k_xu = m.new(acc_k.at[(place + 1) % GROUP], self.in_kx.at[1], mate(1))
        self.k_xd = m.new(acc_k.at[(place + 3) % GROUP], self.in_kx.at[2], mate(3))

        def term(r, dy):
            return dv_ref.at[((place + r) % GROUP) * depth + dy]

        self.v_xx = [m.new(term(2, dy), self.in_v.at[0, dy], mate(3), asked(dy, 2), asked(dy, 3)) for dy in here]
        self.v_xu = [m.new(term(1, dy), self.in_v.at[1, dy], mate(1), asked(dy, 1), asked(dy, 0)) for dy in here]
        self.v_xd = [m.new(self.side_v.at[dy], self.in_v.at[2, dy], mate(3), asked(dy, 3), asked(dy, 0)) for dy in here]
        self.v_y = {dy: m.new(acc_v.at[dy], self.in_v3.at[dy - 3], earlier(dy),
                              both_of(asked(dy, 0), down(dy)), both_of(asked(dy, 0), up(dy))) for dy in here[3:]}
        if rows > 1:
            self.v_yy = m.new(acc_v.at[2], self.in_v1.at[0], earlier(1), both_of(asked(2, 0), down(2)), both_of(asked(2, 0), both))
        self.v_y1 = m.new(acc_v.at[1], self.in_v1.at[1], earlier(1), down(1), up(1))
        self.order = [*here[2:], 1, 0]

    def start(self):
        m = self.m
        for dy in self.order:
            m.start(self.v_xx[dy])
            m.start(self.v_xu[dy])
        for i in (*self.k_yy.values(), *self.k_y.values()):
            m.start(i)

    def run(self):
        m, acc_k, acc_v = self.m, self.acc_k, self.acc_v

        def add(ref, at, buf, *slot):
            def act():
                ref[at] += buf[slot]
            return act

        for i in range(max(len(self.order), GROUP)):
            if i < len(self.order):
                dy = self.order[i]
                m.arrived(self.v_xx[dy], add(self.side_v, dy, self.in_v, 0, dy))
                m.start(self.v_xd[dy])
            if i < GROUP:
                if i in self.k_yy:
                    m.arrived(self.k_yy[i], add(self.near_k, i, self.in_k, i))
                m.start(self.k_y1[i])
        for i in range(max(len(self.order), GROUP)):
            if i < len(self.order):
                dy = self.order[i]
                m.arrived(self.v_xu[dy], add(acc_v, dy, self.in_v, 1, dy))
                m.arrived(self.v_xd[dy], add(acc_v, dy, self.in_v, 2, dy))
                if dy == 2:
                    m.start(self.v_yy)
                elif dy > 2:
                    m.start(self.v_y[dy])
            if i < GROUP:
                for (dy, j), move in self.k_y.items():
                    if j == i:
                        m.arrived(move, add(acc_k, j, self.in_k3, dy - 3, j))
                m.arrived(self.k_y1[i], add(acc_k, i, self.in_k1, i))
        m.start(self.k_xx)
        m.start(self.k_xu)
        if self.rows > 1:
            m.arrived(self.v_yy, add(acc_v, 1, self.in_v1, 0))
        m.start(self.v_y1)
        m.arrived(self.k_xx)
        acc_k[(self.place + 3) % GROUP] += self.in_kx[0]
        m.start(self.k_xd)
        for dy, move in self.v_y.items():
            m.arrived(move, add(acc_v, 0, self.in_v3, dy - 3))
        m.arrived(self.v_y1, add(acc_v, 0, self.in_v1, 1))
        m.arrived(self.k_xu)
        m.arrived(self.k_xd)
        return acc_k[self.place] + self.in_kx[1] + self.in_kx[2]


def scatter_bufs(width, tok, hd):
    rows = (width + 3) // GROUP
    more = max(rows - 2, 1)
    dma = pltpu.SemaphoreType.DMA
    shapes = [(GROUP,), (GROUP,), (GROUP,), (more, GROUP), (3,), (rows + 1,), (3, rows + 1), (2,), (more,)]
    return [pltpu.VMEM((*shape, tok, hd), F32) for shape in shapes] + [dma((8 * rows + 16,)), dma((8 * rows + 16,))]


def finish_kernel(n, reach, width, dk_ref, dv_ref, o_ref, dq_ref, wq_ref, wk_ref, wv_ref, wo_ref, y_ref, dx_ref,
                  acc_k, acc_v, o, dq, wq, wk, wv, wo, y_give, dx_give, dx_part, loc_sem, swap_send, swap_recv, *win):
    me = lax.axis_index('cp')
    core = me % 2
    partner = me + 1 - 2 * core
    blk = block_of(me, n)
    place = blk % GROUP
    base = blk - place
    tok = y_ref.shape[0]
    half = tok // 2
    heads, d_model, hd = wq_ref.shape
    rows = (width + 3) // GROUP
    depth = reach + 1
    mine = pl.ds(pl.multiple_of(core * half, half), half)
    if reach:
        bufs, sems = win[:9], win[9:]
        terms = [(dv_ref.at[pl.ds(((place + 3) % GROUP) * depth, rows + 1)], bufs[5]), (dk_ref.at[pl.ds(4, GROUP)], bufs[0]),
                 (dv_ref.at[pl.ds(place * depth, rows + 1)], acc_v), (dk_ref.at[pl.ds(0, GROUP)], acc_k)]
    else:
        terms = [(dv_ref, acc_v), (dk_ref, acc_k)]
    pairs = terms + [(o_ref, o), (wo_ref, wo), (dq_ref, dq), (wq_ref, wq), (wk_ref, wk), (wv_ref, wv)]
    loads = [pltpu.make_async_copy(src, dst, loc_sem.at[i]) for i, (src, dst) in enumerate(pairs)]
    for c in loads:
        c.start()
    barrier = pltpu.get_barrier_semaphore()
    signal(barrier, partner)
    if reach:
        for r in (1, 3):
            signal(barrier, dev_of(base + (place + r) % GROUP, n))
        column_signal(barrier, blk, n, rows)
        pl.semaphore_wait(barrier, 3 + column_size(blk, n, rows))
        scatter = Scatter(n, blk, reach, width, dk_ref, dv_ref, acc_k, acc_v, bufs, sems)
        scatter.start()
    else:
        pl.semaphore_wait(barrier, 1)
    for c in loads[-6:-4]:
        c.wait()
    o_cat = jnp.concatenate([o[pl.ds(h * tok, tok), :] for h in range(heads)], axis=1)
    y = dot(o_cat, wo[...]).astype(BF16)
    y_give[...] = y[half:]
    y_ref[mine, :] = y[:half]
    for c in loads[-4:-2]:
        c.wait()
    dx = dot_nt(dq[pl.ds(0, tok), :], wq[0])
    for h in range(1, heads):
        dx += dot_nt(dq[pl.ds(h * tok, tok), :], wq[h])
    dx_part[...] = dx
    swap_y = remote(y_give, y_ref.at[mine], swap_send.at[0], swap_recv.at[0], partner)
    swap_y.start()
    for c in loads[:-6] + loads[-2:]:
        c.wait()
    total_k = scatter.run() if reach else acc_k[0]
    dk = total_k.astype(BF16)
    dv = acc_v[0].astype(BF16)

    def dx_rows(lo):
        part = slice(lo, lo + half)
        return (dx_part[pl.ds(lo, half), :] + dot_nt(dk[part], wk[...]) + dot_nt(dv[part], wv[...])).astype(BF16)

    dx_give[...] = dx_rows(half)
    dx_ref[mine, :] = dx_rows(0)
    swap_dx = remote(dx_give, dx_ref.at[mine], swap_send.at[1], swap_recv.at[1], partner)
    swap_dx.start()
    if reach:
        scatter.m.sent()
    swap_y.wait()
    swap_dx.wait()


def copy_kernel(y_ref, dx_ref, y_out, dx_out, sem):
    copies = [pltpu.make_async_copy(y_ref, y_out, sem.at[0]), pltpu.make_async_copy(dx_ref, dx_out, sem.at[1])]
    for c in copies:
        c.start()
    for c in copies:
        c.wait()


def make_layer(n, widths, far):
    dma = pltpu.SemaphoreType.DMA
    near = widths[-1]

    def comm(cid):
        return pltpu.CompilerParams(collective_id=cid, has_side_effects=True, vmem_limit_bytes=VMEM_LIMIT)

    def local_layer(x_in, dy_in, doc_id, w_q, w_k, w_v, w_o):
        tok, d_model = x_in.shape
        heads, hd = w_q.shape[1], w_q.shape[2]
        cols = heads * tok
        me = lax.axis_index('cp')
        blk = block_of(me, n)
        place = blk % GROUP
        wq = jnp.transpose(w_q, (1, 0, 2))
        wk = w_k.reshape(d_model, hd)
        wv = w_v.reshape(d_model, hd)
        wo = w_o.reshape(heads * hd, d_model)
        n_stage = len(stages_of(n))
        reach = (near + 3) // GROUP

        def window(reach, dtype=BF16):
            return jax.ShapeDtypeStruct((GROUP * (reach + 1), tok, hd), dtype)

        q, do, k_win, v_win, rel, nd, which = pl.pallas_call(
            functools.partial(project_kernel, n, reach, (*widths, far)),
            out_shape=(jax.ShapeDtypeStruct((heads, tok, hd), BF16), jax.ShapeDtypeStruct((heads, tok, hd), BF16),
                       window(reach), window(reach), jax.ShapeDtypeStruct((1, cols), jnp.int32),
                       jax.ShapeDtypeStruct((2,), jnp.int32), jax.ShapeDtypeStruct((1,), jnp.int32)),
            in_specs=[HBM, HBM, VMEM, HBM, HBM, HBM, HBM],
            out_specs=(VMEM, VMEM, VMEM, VMEM, VMEM, SMEM, SMEM),
            scratch_shapes=[pltpu.VMEM((tok, d_model), BF16), pltpu.VMEM((tok, d_model), BF16),
                            pltpu.VMEM(wq.shape, BF16), pltpu.VMEM(wk.shape, BF16), pltpu.VMEM(wv.shape, BF16),
                            pltpu.VMEM(wo.shape, BF16), pltpu.VMEM((2, tok, hd), BF16),
                            pltpu.VMEM((heads, tok, hd), BF16), pltpu.VMEM((heads, tok, hd), BF16),
                            pltpu.VMEM((n, 1, 128), jnp.int32), dma((6,)), dma((4,)), dma((4,)), dma((8 * n_stage,)), dma((8 * n_stage,))] + gather_sems(reach),
            compiler_params=comm(0),
            name='project',
        )(x_in, dy_in, doc_id.reshape(1, tok), wq, wk, wv, wo)
        q, do = q.reshape(cols, hd), do.reshape(cols, hd)

        def attend(k, v, width, reach):
            saved = []
            if width:
                saved = [pltpu.VMEM(((width + 1) * tok, cols), F32), pltpu.VMEM(((width + 1) * tok, cols), BF16)]
            row = pltpu.VMEM((1, cols), F32)
            return pl.pallas_call(
                functools.partial(attend_kernel, reach, bool(width)),
                out_shape=(jax.ShapeDtypeStruct((cols, hd), BF16), jax.ShapeDtypeStruct((cols, hd), BF16),
                           jax.ShapeDtypeStruct(k.shape, F32), jax.ShapeDtypeStruct(k.shape, F32)),
                in_specs=[SMEM, VMEM, VMEM, VMEM, VMEM, VMEM],
                out_specs=(VMEM, VMEM, HBM, HBM),
                scratch_shapes=[pltpu.VMEM((hd, cols), BF16), pltpu.VMEM((hd, cols), BF16),
                                pltpu.VMEM((hd, cols), F32), pltpu.VMEM((hd, cols), F32),
                                row, row, row, pltpu.VMEM((tok, hd), F32), pltpu.VMEM((2, tok, hd), F32),
                                pltpu.VMEM((2, tok, hd), F32), dma((2, 2)), dma] + saved,
                compiler_params=pltpu.CompilerParams(vmem_limit_bytes=VMEM_LIMIT),
                name='attend',
            )(nd, rel, q, do, k, v)

        def finish(dk, dv, o, dq, reach, width, cid):
            rows = (width + 3) // GROUP
            win = scatter_bufs(width, tok, hd) if reach else []
            results = pl.pallas_call(
                functools.partial(finish_kernel, n, reach, width),
                out_shape=(jax.ShapeDtypeStruct((tok, d_model), BF16), jax.ShapeDtypeStruct((tok, d_model), BF16)),
                in_specs=[HBM] * 8,
                out_specs=(VMEM, VMEM),
                scratch_shapes=[pltpu.VMEM((4 if reach else 1, tok, hd), F32), pltpu.VMEM((rows + 1, tok, hd), F32),
                                pltpu.VMEM((cols, hd), BF16), pltpu.VMEM((cols, hd), BF16),
                                pltpu.VMEM(wq.shape, BF16), pltpu.VMEM(wk.shape, BF16), pltpu.VMEM(wv.shape, BF16),
                                pltpu.VMEM(wo.shape, BF16), pltpu.VMEM((tok // 2, d_model), BF16),
                                pltpu.VMEM((tok // 2, d_model), BF16), pltpu.VMEM((tok, d_model), F32),
                                dma((10,)), dma((2,)), dma((2,))] + win,
                compiler_params=comm(cid),
                name='finish',
            )(dk, dv, o, dq, wq, wk, wv, wo)
            return pl.pallas_call(
                copy_kernel, out_shape=(jax.ShapeDtypeStruct((tok, d_model), BF16),) * 2,
                in_specs=[VMEM] * 2, out_specs=(HBM, HBM), scratch_shapes=[dma((2,))], name='copy')(*results)

        def with_near(width, cid):
            def run(k, v):
                o, dq, dk, dv = attend(k, v, near, reach)
                return finish(dk, dv, o, dq, reach, width, cid)
            return run

        def own(k, v):
            return (lax.dynamic_index_in_dim(k, place, 0, keepdims=False),
                    lax.dynamic_index_in_dim(v, place * (reach + 1), 0, keepdims=False))

        def with_far(k, v):
            reach = (far + 3) // GROUP
            k, v = pl.pallas_call(
                functools.partial(gather_kernel, n, reach),
                out_shape=(window(reach), window(reach)),
                in_specs=[HBM, HBM], out_specs=(HBM, HBM),
                scratch_shapes=[dma((2,))] + gather_sems(reach),
                compiler_params=comm(1),
                name='gather',
            )(*own(k, v))
            o, dq, dk, dv = attend(k, v, far, reach)
            return finish(dk, dv, o, dq, reach, far, 2)

        order = [2 * b if b < n // 2 else 2 * (n - 1 - b) + 1 for b in range(n)]
        up = [(order[b], order[(b + 1) % n]) for b in range(n)]
        down = [(dst, src) for src, dst in up]

        def with_all(k, v):
            def pull(d, state):
                held, k, v = state
                held = lax.ppermute(held, 'cp', up)
                return held, k.at[d].set(held[0]), v.at[d].set(held[1])

            held = jnp.stack(own(k, v))
            empty = jnp.zeros((n, tok, hd), BF16)
            _, k, v = lax.fori_loop(1, n, pull, (held, empty.at[0].set(held[0]), empty.at[0].set(held[1])))
            o, dq, dk, dv = attend(k, v, 0, 0)

            def push(step, acc):
                d = n - 1 - step
                acc = acc + jnp.stack([lax.dynamic_index_in_dim(dk, d, 0, keepdims=False),
                                       lax.dynamic_index_in_dim(dv, d, 0, keepdims=False)])
                return lax.ppermute(acc, 'cp', down)

            acc = lax.fori_loop(0, n - 1, push, jnp.zeros((2, tok, hd), F32))
            return finish((acc[0] + dk[0])[None], (acc[1] + dv[0])[None], o, dq, 0, 0, 3)

        branches = [with_near(w, 4 + i) for i, w in enumerate(widths)] + [with_far, with_all]
        return lax.switch(which[0], branches, k_win, v_win)

    return local_layer


def solution(mesh, widths=WIDTHS, far=FAR):
    n = mesh.shape['cp']
    row_spec = P(('dp', 'cp'))
    full_spec = P()
    return jax.shard_map(make_layer(n, widths, far), mesh=mesh,
                         in_specs=(row_spec, row_spec, row_spec, full_spec, full_spec, full_spec, full_spec),
                         out_specs=(row_spec, row_spec), check_vma=False)
```

```python
import functools

import jax
import jax.numpy as jnp
from jax import lax
from jax.experimental import pallas as pl
from jax.experimental.pallas import tpu as pltpu
from jax.sharding import PartitionSpec as P

NEG_BIG = -1.0e30
GROUP = 4
MESH = pl.DeviceIdType.MESH
WIDTHS, FAR, CHUNK = (8, 9, 10, 12), 24, 256
LOG2_E = 1.4426950408889634
F32, BF16 = jnp.float32, jnp.bfloat16
HBM = pl.BlockSpec(memory_space=pl.ANY)
VMEM = pl.BlockSpec(memory_space=pltpu.VMEM)
SMEM = pl.BlockSpec(memory_space=pltpu.SMEM)
MIB = 1 << 20


def dot(a, b):
    return jnp.dot(a, b, preferred_element_type=F32)


def dot_nt(a, b):
    return lax.dot_general(a, b, (((1,), (1,)), ((), ())), preferred_element_type=F32)


def dot_tn(a, b):
    return lax.dot_general(a, b, (((0,), (0,)), ((), ())), preferred_element_type=F32)


def block_of(dev, n):
    return jnp.where(dev % 2 == 0, dev // 2, n - 1 - dev // 2)


def dev_of(blk, n):
    return jnp.where(blk < n // 2, 2 * blk, 2 * (n - 1 - blk) + 1)


def at(dev):
    return (lax.axis_index('dp'), dev)


def stages_of(n):
    out, stride = [(1, min(n, 8))], min(n, 8)
    while stride < n:
        size = min(4, n // stride)
        out.append((stride, size))
        stride *= size
    return out


def peer_of(me, stride, size, j):
    idx = (me // stride) % size
    return me - idx * stride + ((idx + j) % size) * stride


def remote(src, dst, send, recv, dev):
    return pltpu.make_async_remote_copy(src_ref=src, dst_ref=dst, send_sem=send, recv_sem=recv,
                                        device_id=at(dev), device_id_type=MESH)


def column(blk, n, reach):
    out = []
    for dy in range(1, reach + 1):
        out.append((blk - GROUP * dy, blk - GROUP * dy >= 0))
        out.append((blk + GROUP * dy, blk + GROUP * dy < n))
    return out


def signal(barrier, dev):
    pl.semaphore_signal(barrier, inc=1, device_id=at(dev), device_id_type=MESH)


def column_signal(barrier, blk, n, reach):
    for other, there in column(blk, n, reach):
        @pl.when(there)
        def _():
            signal(barrier, dev_of(other, n))


def column_size(blk, n, reach):
    return jnp.minimum((n - 1 - blk) // GROUP, reach) + jnp.minimum(blk // GROUP, reach)


class Moves:
    def __init__(self, send, recv):
        self.sems, self.copies = (send, recv), []

    def new(self, src, dst, dev, go=None, come=None):
        i = len(self.copies)
        self.copies.append((remote(src, dst, self.sems[0].at[i], self.sems[1].at[i], dev), go, come))
        return i

    def when(self, cond, act):
        if cond is None:
            act()
        else:
            pl.when(cond)(act)

    def start(self, i):
        copy, go, _ = self.copies[i]
        self.when(go, copy.start)

    def arrived(self, i, then=None):
        copy, _, come = self.copies[i]

        def act():
            copy.wait_recv()
            if then is not None:
                then()
        self.when(come, act)

    def sent(self):
        for copy, go, _ in self.copies:
            self.when(go, copy.wait_send)


class Gather:
    def __init__(self, n, blk, reach, k_ref, v_ref, send, recv):
        place = blk % GROUP
        base = blk - place
        depth = reach + 1
        self.m = m = Moves(send, recv)

        def mate(r):
            return dev_of(base + (place + r) % GROUP, n)

        def later(dy):
            return dev_of(jnp.minimum(blk + GROUP * dy, n - 1), n)

        def k_at(dy, r):
            return k_ref.at[GROUP * dy + (place + r) % GROUP]

        def v_at(r, dy):
            return v_ref.at[((place + r) % GROUP) * depth + dy]

        def up(dy):
            return blk + GROUP * dy < n

        def down(dy):
            return blk - GROUP * dy >= 0

        both = up(1) & down(1)
        mid = down(2)
        self.straight = [dy for dy in range(1, reach + 1) if dy != 2]
        self.k_x = {r: m.new(k_at(0, 0), k_at(0, 0), mate(r)) for r in (1, 3, 2)}
        self.k_y = {(dy, r): m.new(k_at(0, r), k_at(dy, r), later(dy), up(dy), down(dy)) for dy in self.straight for r in range(GROUP)}
        self.v_y = {dy: m.new(v_at(0, 0), v_at(0, dy), later(dy), up(dy), down(dy)) for dy in (*self.straight, *range(2, min(reach, 2) + 1))}
        rows = [(0, None)] + [(dy, down(dy)) for dy in range(1, reach + 1)]
        self.v_x = {(dy, r): m.new(v_at(0, dy), v_at(0, dy), mate(r), c, c) for dy, c in rows for r in (1, 3)}
        self.v_xx = {dy: m.new(v_at(3, dy), v_at(3, dy), mate(1), c, c) for dy, c in rows}
        if reach > 1:
            self.k_yy = {r: m.new(k_at(1, r), k_at(2, r), later(1), both, mid) for r in range(GROUP)}
        self.reach = reach

    def own(self):
        m = self.m
        for i in self.k_x.values():
            m.start(i)
        self.k_on(0)
        for i in self.v_y.values():
            m.start(i)
        self.v_on(0)

    def k_on(self, r):
        for dy in self.straight:
            self.m.start(self.k_y[dy, r])

    def v_on(self, dy):
        for r in (1, 3):
            self.m.start(self.v_x[dy, r])

    def hand_on(self):
        m = self.m
        m.arrived(self.k_x[1])
        self.k_on(3)
        m.arrived(self.v_y[1])
        self.v_on(1)
        m.arrived(self.k_x[3])
        self.k_on(1)
        for dy in self.straight[1:]:
            m.arrived(self.v_y[dy])
            self.v_on(dy)
        m.arrived(self.v_x[0, 1])
        m.start(self.v_xx[0])
        m.arrived(self.k_y[1, 0])
        if self.reach > 1:
            m.start(self.k_yy[0])
        m.arrived(self.k_x[2])
        self.k_on(2)
        if self.reach > 1:
            m.arrived(self.v_y[2])
            self.v_on(2)

    def rest(self):
        m = self.m
        order = [1] + self.straight[1:] + ([2] if self.reach > 1 else [])
        for i in range(max(len(order), 3)):
            if i < len(order):
                m.arrived(self.v_x[order[i], 1])
                m.start(self.v_xx[order[i]])
            if i < 3:
                r = (3, 1, 2)[i]
                m.arrived(self.k_y[1, r])
                if self.reach > 1:
                    m.start(self.k_yy[r])

    def finish(self):
        m = self.m
        for dy in self.straight[1:]:
            for r in range(GROUP):
                m.arrived(self.k_y[dy, r])
        for dy in range(self.reach + 1):
            m.arrived(self.v_x[dy, 3])
            m.arrived(self.v_xx[dy])
        if self.reach > 1:
            for r in range(GROUP):
                m.arrived(self.k_yy[r])
        m.sent()


def gather_sems(reach):
    dma = pltpu.SemaphoreType.DMA
    return [dma((9 * reach + 12,)), dma((9 * reach + 12,))]


def place_documents(tab_ref, doc_ref, me):
    docs, tok = tab_ref.shape[-1], doc_ref.shape[-1]
    earlier = doc_ref[...] < lax.broadcasted_iota(jnp.int32, (docs, tok), 0)
    count = dot_nt(jnp.ones((8, tok), BF16), jnp.where(earlier, 1.0, 0.0).astype(BF16))
    tab_ref[me] = count[:1].astype(jnp.int32)


def find_documents(tab_ref, rel_ref, near_ref, which_ref, blk, tok, limits):
    n, _, docs = tab_ref.shape
    starts = jnp.sum(tab_ref[...], axis=0).astype(F32)
    lane = lax.broadcasted_iota(jnp.int32, (1, docs), 1)
    ends = jnp.where(lane == docs - 1, float(n * tok), pltpu.roll(starts, docs - 1, 1))

    def block(pos):
        return jnp.floor((pos + 0.5) * (1.0 / tok))

    span = jnp.max(jnp.where(ends > starts, block(ends - 1.0) - block(starts), 0.0)).astype(jnp.int32)
    which = jnp.int32(0)
    for w in limits:
        which = which + jnp.where(span > w, 1, 0)
    which_ref[0] = which
    cols = rel_ref.shape[1]
    pos = (lax.broadcasted_iota(jnp.int32, (1, cols), 1) % tok + blk * tok).astype(F32)
    column = jnp.broadcast_to(starts, (docs, docs)).T[:, :1]
    first = jnp.max(jnp.where(column <= pos, column, 0.0), axis=0, keepdims=True)
    rel_ref[...] = first.astype(jnp.int32) - blk * tok
    near_ref[0] = blk - block(jnp.min(first)).astype(jnp.int32)
    near_ref[1] = blk % GROUP


def project_kernel(n, reach, limits, x_ref, dy_ref, doc_ref, wq_ref, wk_ref, wv_ref, wo_ref,
                   q_ref, do_ref, k_ref, v_ref, rel_ref, near_ref, which_ref,
                   xs, dys, wq, wk, wv, wo, own_kv, own_q, own_do, tab_ref, loc_sem, swap_send, swap_recv,
                   tab_send, tab_recv, *win):
    me = lax.axis_index('cp')
    core = me % 2
    partner = me + 1 - 2 * core
    blk = block_of(me, n)
    place = blk % GROUP
    tok = x_ref.shape[0]
    half = tok // 2
    heads, _, hd = wq_ref.shape
    depth = reach + 1
    keep = pl.ds(pl.multiple_of(core * half, half), half)
    give = pl.ds(pl.multiple_of((1 - core) * half, half), half)
    front, back = pl.ds(0, half), pl.ds(half, half)
    loads = [pltpu.make_async_copy(src, dst, loc_sem.at[i]) for i, (src, dst) in enumerate((
        (x_ref, xs), (wk_ref, wk), (wv_ref, wv), (wq_ref, wq), (dy_ref, dys), (wo_ref, wo)))]
    for c in loads:
        c.start()
    barrier = pltpu.get_barrier_semaphore()
    stages = stages_of(n)
    peers = 0
    for stride, size in stages:
        for j in range(1, size):
            signal(barrier, peer_of(me, stride, size, j))
            peers += 1
    column_signal(barrier, blk, n, reach)
    place_documents(tab_ref, doc_ref, me)

    def stage_copies(s):
        stride, size = stages[s]
        rows = pl.ds(me - me % stride, stride)
        return [remote(tab_ref.at[rows], tab_ref.at[rows], tab_send.at[8 * s + j], tab_recv.at[8 * s + j],
                       peer_of(me, stride, size, j)) for j in range(1, size)]

    def q_heads(some):
        for h in some:
            own_q[h] = dot(xs[...], wq[h]).astype(BF16)
            q_ref[h, front, :] = own_q[h, keep, :]

    tables = [stage_copies(s) for s in range(len(stages))]
    other = GROUP - 1 - place
    swaps = [remote(src, dst, swap_send.at[i], swap_recv.at[i], partner) for i, (src, dst) in enumerate((
        (own_kv.at[0, give], k_ref.at[other, back]), (own_kv.at[1, give], v_ref.at[other * depth, back]),
        (own_q.at[:, give], q_ref.at[:, back]), (own_do.at[:, give], do_ref.at[:, back])))]
    gather = Gather(n, blk, reach, k_ref, v_ref, *win)

    def next_table(s):
        if s < len(stages):
            for c in tables[s - 1]:
                c.wait()
            for c in tables[s]:
                c.start()

    for c in loads[:3]:
        c.wait()
    own_kv[0] = dot(xs[...], wk[...]).astype(BF16)
    own_kv[1] = dot(xs[...], wv[...]).astype(BF16)
    k_ref[place, front, :] = own_kv[0, keep, :]
    v_ref[place * depth, front, :] = own_kv[1, keep, :]
    loads[3].wait()
    q_heads(range(1))
    pl.semaphore_wait(barrier, peers + column_size(blk, n, reach))
    for c in swaps[:2] + tables[0]:
        c.start()
    q_heads(range(1, heads))
    for c in swaps[:2]:
        c.wait_recv()
    gather.own()
    loads[4].wait()
    loads[5].wait()
    for h in range(heads):
        own_do[h] = dot_nt(dys[...], wo[pl.ds(h * hd, hd), :]).astype(BF16)
        do_ref[h, front, :] = own_do[h, keep, :]
    swaps[2].start()
    next_table(1)
    gather.hand_on()
    swaps[3].start()
    next_table(2)
    gather.rest()
    for c in tables[-1]:
        c.wait()
    find_documents(tab_ref, rel_ref, near_ref, which_ref, blk, tok, limits)
    gather.finish()
    for c in swaps[2:]:
        c.wait_recv()
    for c in swaps:
        c.wait_send()


def gather_kernel(n, reach, k_own_ref, v_own_ref, k_ref, v_ref, loc_sem, *win):
    me = lax.axis_index('cp')
    blk = block_of(me, n)
    place = blk % GROUP
    own = [pltpu.make_async_copy(k_own_ref, k_ref.at[place], loc_sem.at[0]),
           pltpu.make_async_copy(v_own_ref, v_ref.at[place * (reach + 1)], loc_sem.at[1])]
    for c in own:
        c.start()
    barrier = pltpu.get_barrier_semaphore()
    for m in range(1, GROUP):
        signal(barrier, dev_of(blk - place + (place + m) % GROUP, n))
    column_signal(barrier, blk, n, reach)
    pl.semaphore_wait(barrier, 3 + column_size(blk, n, reach))
    for c in own:
        c.wait()
    gather = Gather(n, blk, reach, k_ref, v_ref, *win)
    gather.own()
    gather.hand_on()
    gather.rest()
    gather.finish()


def attend_kernel(reach, keep, nd_ref, start_ref, q_ref, do_ref, k_ref, v_ref, o_ref, dq_ref, dk_ref, dv_ref,
                  q_t, do_t, o_t, dq_t, ds_t, top, tot, delta, zero, dk_out, dv_out, out_sem, zero_sem, *saved):
    nd = nd_ref[0]
    place = nd_ref[1]
    slots, tok, hd = k_ref.shape
    cols = q_ref.shape[0]
    scale = hd ** -0.5
    base2 = scale * LOG2_E

    def slots_of(d):
        if not reach:
            return d, d
        back = (d + GROUP - 1 - place) // GROUP
        spot = place - d + GROUP * back
        return GROUP * back + spot, spot * (reach + 1) + back

    def rows(d):
        return pl.ds(pl.multiple_of(d * tok, tok), tok)

    zero[...] = jnp.zeros_like(zero)

    def each_empty(act):
        def step(i, _):
            if reach:
                d = place + GROUP * (i // GROUP) - i % GROUP
                empty = (d < 0) | (d > nd)
                where = (i, (i % GROUP) * (reach + 1) + i // GROUP)
            else:
                empty = i > nd
                where = (i, i)

            @pl.when(empty)
            def _():
                for ref, slot in zip((dk_ref, dv_ref), where):
                    act(pltpu.make_async_copy(zero, ref.at[slot], zero_sem))
            return 0
        lax.fori_loop(0, slots, step, 0)

    each_empty(lambda c: c.start())
    q_t[...] = q_ref[...].T
    do_t[...] = do_ref[...].T
    top[...] = jnp.full_like(top, NEG_BIG)
    tot[...] = jnp.zeros_like(tot)
    o_t[...] = jnp.zeros_like(o_t)
    dq_t[...] = jnp.zeros_like(dq_t)

    def split(size):
        return [(lo, min(size, cols - lo)) for lo in range(0, cols, size)]

    def scores(k, d, lo, size, own):
        part = pl.ds(lo, size)
        s = dot(k, q_t[:, part])
        u = lax.broadcasted_iota(jnp.int32, (tok, size), 0)
        visible = u >= start_ref[:, part] + d * tok
        if own:
            t = (lax.broadcasted_iota(jnp.int32, (1, size), 1) + lo) % tok
            visible = visible & (u <= t + d * tok)
        return jnp.where(visible, s, NEG_BIG)

    def weight(s, part):
        return jnp.exp2(s * base2 - top[:, part])

    def find_top(d, own):
        k = k_ref[slots_of(d)[0]]
        for lo, size in split(CHUNK):
            part = pl.ds(lo, size)
            s = scores(k, d, lo, size, own)
            top[:, part] = jnp.maximum(top[:, part], jnp.max(s, axis=0, keepdims=True))
            if keep:
                saved[0][rows(d), part] = s

    def find_total(d, own):
        k = None if keep else k_ref[slots_of(d)[0]]
        for lo, size in split(CHUNK):
            part = pl.ds(lo, size)
            e = weight(saved[0][rows(d), part] if keep else scores(k, d, lo, size, own), part)
            tot[:, part] += jnp.sum(e, axis=0, keepdims=True)
            if keep:
                saved[0][rows(d), part] = e

    def forward(d, own):
        vt = v_ref[slots_of(d)[1]].T
        k = None if keep else k_ref[slots_of(d)[0]]
        for lo, size in split(CHUNK):
            part = pl.ds(lo, size)
            e = saved[0][rows(d), part] if keep else weight(scores(k, d, lo, size, own), part)
            p = (e * tot[:, part]).astype(BF16)
            if keep:
                saved[1][rows(d), part] = p
            o_t[:, part] += dot(vt, p)

    def outputs(d):
        buf = d % 2
        return [pltpu.make_async_copy(out.at[buf], ref.at[slot], out_sem.at[i, buf])
                for i, (out, ref, slot) in enumerate(zip((dk_out, dv_out), (dk_ref, dv_ref), slots_of(d)))]

    def backward(d, own):
        @pl.when(d > 1)
        def _():
            for c in outputs(d - 2):
                c.wait()

        k, v = k_ref[slots_of(d)[0]], v_ref[slots_of(d)[1]]
        kt = k.T
        buf = d % 2
        p_all = saved[1].at[rows(d)] if keep else saved[0]
        for lo, size in split(CHUNK):
            part = pl.ds(lo, size)
            if not keep:
                p_all[:, part] = (weight(scores(k, d, lo, size, own), part) * tot[:, part]).astype(BF16)
            dp = dot(v, do_t[:, part])
            ds_t[:, part] = (p_all[:, part].astype(F32) * (dp - delta[:, part])).astype(BF16)
        dq_t[...] += dot(kt, ds_t[...])
        dk_out[buf] = dot(ds_t[...], q_ref[...]) * scale
        dv_out[buf] = dot(p_all[...], do_ref[...])
        for c in outputs(d):
            c.start()

    def over_blocks(step, first):
        def body(d, _):
            step(d, not first)
            return 0

        if first:
            step(0, True)
        lax.fori_loop(int(first), nd + 1, body, 0)

    over_blocks(find_top, keep)
    top[...] = top[...] * base2
    over_blocks(find_total, False)
    tot[...] = 1.0 / tot[...]
    over_blocks(forward, False)
    o_bf = o_t[...].astype(BF16)
    delta[...] = jnp.sum(o_bf.astype(F32) * do_t[...].astype(F32), axis=0, keepdims=True)
    o_ref[...] = o_bf.T
    over_blocks(backward, False)
    dq_ref[...] = (dq_t[...] * scale).astype(BF16).T

    @pl.when(nd > 0)
    def _():
        for c in outputs(nd - 1):
            c.wait()

    for c in outputs(nd):
        c.wait()
    each_empty(lambda c: c.wait())


class Scatter:
    def __init__(self, n, blk, reach, width, dk_ref, dv_ref, acc_k, acc_v, bufs, sems):
        place = blk % GROUP
        base = blk - place
        depth = reach + 1
        self.place, self.acc_k, self.acc_v = place, acc_k, acc_v
        self.rows = rows = (width + 3) // GROUP
        self.near_k, self.in_k, self.in_k1, self.in_k3, self.in_kx, self.side_v, self.in_v, self.in_v1 = bufs
        self.m = m = Moves(*sems)

        def mate(r):
            return dev_of(base + (place + r) % GROUP, n)

        def earlier(dy):
            return dev_of(jnp.maximum(blk - GROUP * dy, 0), n)

        def down(dy):
            return blk - GROUP * dy >= 0

        def up(dy):
            return blk + GROUP * dy < n

        def need(dy, place):
            return GROUP * dy - width <= place

        def both_of(a, b):
            return b if a is None else a & b

        def asked(dy, r):
            return None if need(dy, 0) else need(dy, (place + r) % GROUP)

        both = up(1) & down(1)
        here, there = range(rows + 1), [(dy, j) for dy in range(3, rows + 1) for j in range(GROUP) if need(dy, j)]
        self.k_yy = {j: m.new(dk_ref.at[2 * GROUP + j], self.in_k.at[j], earlier(1), down(2), both)
                     for j in range(GROUP) if rows > 1 and need(2, j)}
        self.k_y = {(dy, j): m.new(dk_ref.at[GROUP * dy + j], self.in_k3.at[dy - 3, j], earlier(dy), down(dy), up(dy))
                    for dy, j in there}
        self.k_y1 = [m.new(self.near_k.at[j], self.in_k1.at[j], earlier(1), down(1), up(1)) for j in range(GROUP)]
        self.k_x = [m.new(acc_k.at[(place + r) % GROUP], self.in_kx.at[r - 1], mate(r)) for r in (2, 1, 3)]

        def term(r, dy):
            return dv_ref.at[((place + r) % GROUP) * depth + dy]

        self.v_xx = [m.new(term(2, dy), self.in_v.at[0, dy], mate(3), asked(dy, 2), asked(dy, 3)) for dy in here]
        self.v_xu = [m.new(term(1, dy), self.in_v.at[1, dy], mate(1), asked(dy, 1), asked(dy, 0)) for dy in here]
        self.v_xd = [m.new(self.side_v.at[dy], self.in_v.at[2, dy], mate(3), asked(dy, 3), asked(dy, 0)) for dy in here]
        self.v_y = {dy: m.new(acc_v.at[dy], self.in_v1.at[dy - 1], earlier(dy),
                              both_of(asked(dy, 0), down(dy)), both_of(asked(dy, 0), up(dy))) for dy in here[1:]}
        self.order = [*here[2:], 1, 0]

    def start(self):
        m = self.m
        for dy in self.order:
            m.start(self.v_xx[dy])
            m.start(self.v_xu[dy])
        for i in (*self.k_yy.values(), *self.k_y.values()):
            m.start(i)

    def add(self, ref, at, buf, *slot):
        def act():
            ref[at] += buf[slot]
        return act

    def first_half(self):
        m, add = self.m, self.add
        for i in range(max(len(self.order), GROUP)):
            if i < len(self.order):
                dy = self.order[i]
                m.arrived(self.v_xx[dy], add(self.side_v, dy, self.in_v, 0, dy))
                m.start(self.v_xd[dy])
            if i < GROUP:
                if i in self.k_yy:
                    m.arrived(self.k_yy[i], add(self.near_k, i, self.in_k, i))
                m.start(self.k_y1[i])

    def second_half(self):
        m, add, acc_k, acc_v = self.m, self.add, self.acc_k, self.acc_v
        for i in range(max(len(self.order), GROUP)):
            if i < len(self.order):
                dy = self.order[i]
                m.arrived(self.v_xu[dy], add(acc_v, dy, self.in_v, 1, dy))
                m.arrived(self.v_xd[dy], add(acc_v, dy, self.in_v, 2, dy))
                if dy:
                    m.start(self.v_y[dy])
            if i < GROUP:
                for (dy, j), move in self.k_y.items():
                    if j == i:
                        m.arrived(move, add(acc_k, j, self.in_k3, dy - 3, j))
                m.arrived(self.k_y1[i], add(acc_k, i, self.in_k1, i))
        for i in self.k_x:
            m.start(i)
        for dy, move in self.v_y.items():
            m.arrived(move, add(acc_v, 0, self.in_v1, dy - 1))
        for i in self.k_x:
            m.arrived(i)
        return acc_k[self.place] + self.in_kx[0] + self.in_kx[1] + self.in_kx[2]


def scatter_bufs(width, tok, hd):
    rows = (width + 3) // GROUP
    more = max(rows - 2, 1)
    dma = pltpu.SemaphoreType.DMA
    shapes = [(GROUP,), (GROUP,), (GROUP,), (more, GROUP), (3,), (rows + 1,), (3, rows + 1), (rows,)]
    return [pltpu.VMEM((*shape, tok, hd), F32) for shape in shapes] + [dma((8 * rows + 16,)), dma((8 * rows + 16,))]


def finish_kernel(n, reach, width, dk_ref, dv_ref, o_ref, dq_ref, wq_ref, wk_ref, wv_ref, wo_ref, y_ref, dx_ref,
                  acc_k, acc_v, o, dq, wq, wk, wv, wo, y_give, dx_give, dx_part, loc_sem, swap_send, swap_recv, *win):
    me = lax.axis_index('cp')
    core = me % 2
    partner = me + 1 - 2 * core
    blk = block_of(me, n)
    place = blk % GROUP
    base = blk - place
    tok = y_ref.shape[0]
    half = tok // 2
    heads, d_model, hd = wq_ref.shape
    rows = (width + 3) // GROUP
    depth = reach + 1
    mine = pl.ds(pl.multiple_of(core * half, half), half)
    if reach:
        bufs, sems = win[:-2], win[-2:]
        terms = [(dv_ref.at[pl.ds(((place + 3) % GROUP) * depth, rows + 1)], bufs[5]), (dk_ref.at[pl.ds(4, GROUP)], bufs[0]),
                 (dv_ref.at[pl.ds(place * depth, rows + 1)], acc_v), (dk_ref.at[pl.ds(0, GROUP)], acc_k)]
    else:
        terms = [(dv_ref, acc_v), (dk_ref, acc_k)]
    pairs = terms + [(o_ref, o), (wo_ref, wo), (dq_ref, dq), (wq_ref, wq), (wk_ref, wk), (wv_ref, wv)]
    loads = [pltpu.make_async_copy(src, dst, loc_sem.at[i]) for i, (src, dst) in enumerate(pairs)]
    for c in loads:
        c.start()
    barrier = pltpu.get_barrier_semaphore()
    signal(barrier, partner)
    if reach:
        for r in range(1, GROUP):
            signal(barrier, dev_of(base + (place + r) % GROUP, n))
        column_signal(barrier, blk, n, rows)
        pl.semaphore_wait(barrier, GROUP + column_size(blk, n, rows))
        scatter = Scatter(n, blk, reach, width, dk_ref, dv_ref, acc_k, acc_v, bufs, sems)
        scatter.start()
    else:
        pl.semaphore_wait(barrier, 1)
    for c in loads[:-6]:
        c.wait()
    if reach:
        scatter.first_half()
    for c in loads[-6:-4]:
        c.wait()
    o_cat = jnp.concatenate([o[pl.ds(h * tok, tok), :] for h in range(heads)], axis=1)
    y = dot(o_cat, wo[...]).astype(BF16)
    y_give[...] = y[half:]
    y_ref[mine, :] = y[:half]
    for c in loads[-4:-2]:
        c.wait()
    dx = dot_nt(dq[pl.ds(0, tok), :], wq[0])
    for h in range(1, heads):
        dx += dot_nt(dq[pl.ds(h * tok, tok), :], wq[h])
    dx_part[...] = dx
    swap_y = remote(y_give, y_ref.at[mine], swap_send.at[0], swap_recv.at[0], partner)
    swap_y.start()
    for c in loads[-2:]:
        c.wait()
    total_k = scatter.second_half() if reach else acc_k[0]
    dk = total_k.astype(BF16)
    dv = acc_v[0].astype(BF16)

    def dx_rows(lo):
        part = slice(lo, lo + half)
        return (dx_part[pl.ds(lo, half), :] + dot_nt(dk[part], wk[...]) + dot_nt(dv[part], wv[...])).astype(BF16)

    dx_give[...] = dx_rows(half)
    dx_ref[mine, :] = dx_rows(0)
    swap_dx = remote(dx_give, dx_ref.at[mine], swap_send.at[1], swap_recv.at[1], partner)
    swap_dx.start()
    if reach:
        scatter.m.sent()
    swap_y.wait()
    swap_dx.wait()


def copy_kernel(y_ref, dx_ref, y_out, dx_out, sem):
    copies = [pltpu.make_async_copy(y_ref, y_out, sem.at[0]), pltpu.make_async_copy(dx_ref, dx_out, sem.at[1])]
    for c in copies:
        c.start()
    for c in copies:
        c.wait()


def make_layer(n, widths, far):
    dma = pltpu.SemaphoreType.DMA
    near = widths[-1]

    def comm(cid, mib=28):
        return pltpu.CompilerParams(collective_id=cid, has_side_effects=True, vmem_limit_bytes=mib * MIB)

    def local_layer(x_in, dy_in, doc_id, w_q, w_k, w_v, w_o):
        tok, d_model = x_in.shape
        heads, hd = w_q.shape[1], w_q.shape[2]
        cols = heads * tok
        me = lax.axis_index('cp')
        blk = block_of(me, n)
        place = blk % GROUP
        wq = jnp.transpose(w_q, (1, 0, 2))
        wk = w_k.reshape(d_model, hd)
        wv = w_v.reshape(d_model, hd)
        wo = w_o.reshape(heads * hd, d_model)
        n_stage = len(stages_of(n))
        reach = (near + 3) // GROUP

        def window(reach, dtype=BF16):
            return jax.ShapeDtypeStruct((GROUP * (reach + 1), tok, hd), dtype)

        q, do, k_win, v_win, rel, nd, which = pl.pallas_call(
            functools.partial(project_kernel, n, reach, (*widths, far)),
            out_shape=(jax.ShapeDtypeStruct((heads, tok, hd), BF16), jax.ShapeDtypeStruct((heads, tok, hd), BF16),
                       window(reach), window(reach), jax.ShapeDtypeStruct((1, cols), jnp.int32),
                       jax.ShapeDtypeStruct((2,), jnp.int32), jax.ShapeDtypeStruct((1,), jnp.int32)),
            in_specs=[HBM, HBM, VMEM, HBM, HBM, HBM, HBM],
            out_specs=(VMEM, VMEM, VMEM, VMEM, VMEM, SMEM, SMEM),
            scratch_shapes=[pltpu.VMEM((tok, d_model), BF16), pltpu.VMEM((tok, d_model), BF16),
                            pltpu.VMEM(wq.shape, BF16), pltpu.VMEM(wk.shape, BF16), pltpu.VMEM(wv.shape, BF16),
                            pltpu.VMEM(wo.shape, BF16), pltpu.VMEM((2, tok, hd), BF16),
                            pltpu.VMEM((heads, tok, hd), BF16), pltpu.VMEM((heads, tok, hd), BF16),
                            pltpu.VMEM((n, 1, 128), jnp.int32), dma((6,)), dma((4,)), dma((4,)), dma((8 * n_stage,)), dma((8 * n_stage,))] + gather_sems(reach),
            compiler_params=comm(0),
            name='project',
        )(x_in, dy_in, doc_id.reshape(1, tok), wq, wk, wv, wo)
        q, do = q.reshape(cols, hd), do.reshape(cols, hd)

        def attend(k, v, width, reach):
            saved = [pltpu.VMEM((tok, cols), BF16)]
            if width:
                saved = [pltpu.VMEM(((width + 1) * tok, cols), F32), pltpu.VMEM(((width + 1) * tok, cols), BF16)]
            row = pltpu.VMEM((1, cols), F32)
            return pl.pallas_call(
                functools.partial(attend_kernel, reach, bool(width)),
                out_shape=(jax.ShapeDtypeStruct((cols, hd), BF16), jax.ShapeDtypeStruct((cols, hd), BF16),
                           jax.ShapeDtypeStruct(k.shape, F32), jax.ShapeDtypeStruct(k.shape, F32)),
                in_specs=[SMEM, VMEM, VMEM, VMEM, VMEM, VMEM],
                out_specs=(VMEM, VMEM, HBM, HBM),
                scratch_shapes=[pltpu.VMEM((hd, cols), BF16), pltpu.VMEM((hd, cols), BF16),
                                pltpu.VMEM((hd, cols), F32), pltpu.VMEM((hd, cols), F32), pltpu.VMEM((tok, cols), BF16),
                                row, row, row, pltpu.VMEM((tok, hd), F32), pltpu.VMEM((2, tok, hd), F32),
                                pltpu.VMEM((2, tok, hd), F32), dma((2, 2)), dma] + saved,
                compiler_params=pltpu.CompilerParams(vmem_limit_bytes=(36 if width == near else 60) * MIB),
                name='attend',
            )(nd, rel, q, do, k, v)

        def finish(dk, dv, o, dq, reach, width, cid):
            rows = (width + 3) // GROUP
            win = scatter_bufs(width, tok, hd) if reach else []
            results = pl.pallas_call(
                functools.partial(finish_kernel, n, reach, width),
                out_shape=(jax.ShapeDtypeStruct((tok, d_model), BF16), jax.ShapeDtypeStruct((tok, d_model), BF16)),
                in_specs=[HBM] * 8,
                out_specs=(VMEM, VMEM),
                scratch_shapes=[pltpu.VMEM((4 if reach else 1, tok, hd), F32), pltpu.VMEM((rows + 1, tok, hd), F32),
                                pltpu.VMEM((cols, hd), BF16), pltpu.VMEM((cols, hd), BF16),
                                pltpu.VMEM(wq.shape, BF16), pltpu.VMEM(wk.shape, BF16), pltpu.VMEM(wv.shape, BF16),
                                pltpu.VMEM(wo.shape, BF16), pltpu.VMEM((tok // 2, d_model), BF16),
                                pltpu.VMEM((tok // 2, d_model), BF16), pltpu.VMEM((tok, d_model), F32),
                                dma((10,)), dma((2,)), dma((2,))] + win,
                compiler_params=comm(cid, 60 if width == far else 28),
                name='finish',
            )(dk, dv, o, dq, wq, wk, wv, wo)
            return pl.pallas_call(
                copy_kernel, out_shape=(jax.ShapeDtypeStruct((tok, d_model), BF16),) * 2,
                in_specs=[VMEM] * 2, out_specs=(HBM, HBM), scratch_shapes=[dma((2,))],
                compiler_params=pltpu.CompilerParams(vmem_limit_bytes=4 * MIB), name='copy')(*results)

        def with_near(width, cid):
            def run(k, v):
                o, dq, dk, dv = attend(k, v, near, reach)
                return finish(dk, dv, o, dq, reach, width, cid)
            return run

        def own(k, v):
            return (lax.dynamic_index_in_dim(k, place, 0, keepdims=False),
                    lax.dynamic_index_in_dim(v, place * (reach + 1), 0, keepdims=False))

        def with_far(k, v):
            reach = (far + 3) // GROUP
            k, v = pl.pallas_call(
                functools.partial(gather_kernel, n, reach),
                out_shape=(window(reach), window(reach)),
                in_specs=[HBM, HBM], out_specs=(HBM, HBM),
                scratch_shapes=[dma((2,))] + gather_sems(reach),
                compiler_params=comm(1),
                name='gather',
            )(*own(k, v))
            o, dq, dk, dv = attend(k, v, far, reach)
            return finish(dk, dv, o, dq, reach, far, 2)

        order = [2 * b if b < n // 2 else 2 * (n - 1 - b) + 1 for b in range(n)]
        up = [(order[b], order[(b + 1) % n]) for b in range(n)]
        down = [(dst, src) for src, dst in up]

        def with_all(k, v):
            def pull(d, state):
                held, k, v = state
                held = lax.ppermute(held, 'cp', up)
                return held, k.at[d].set(held[0]), v.at[d].set(held[1])

            held = jnp.stack(own(k, v))
            empty = jnp.zeros((n, tok, hd), BF16)
            _, k, v = lax.fori_loop(1, n, pull, (held, empty.at[0].set(held[0]), empty.at[0].set(held[1])))
            o, dq, dk, dv = attend(k, v, 0, 0)

            def push(step, acc):
                d = n - 1 - step
                acc = acc + jnp.stack([lax.dynamic_index_in_dim(dk, d, 0, keepdims=False),
                                       lax.dynamic_index_in_dim(dv, d, 0, keepdims=False)])
                return lax.ppermute(acc, 'cp', down)

            acc = lax.fori_loop(0, n - 1, push, jnp.zeros((2, tok, hd), F32))
            return finish((acc[0] + dk[0])[None], (acc[1] + dv[0])[None], o, dq, 0, 0, 3)

        branches = [with_near(w, 4 + i) for i, w in enumerate(widths)] + [with_far, with_all]
        return lax.switch(which[0], branches, k_win, v_win)

    return local_layer


def solution(mesh, widths=WIDTHS, far=FAR):
    n = mesh.shape['cp']
    row_spec = P(('dp', 'cp'))
    full_spec = P()
    return jax.shard_map(make_layer(n, widths, far), mesh=mesh,
                         in_specs=(row_spec, row_spec, row_spec, full_spec, full_spec, full_spec, full_spec),
                         out_specs=(row_spec, row_spec), check_vma=False)
```

```python
import functools

import jax
import jax.numpy as jnp
from jax import lax
from jax.experimental import pallas as pl
from jax.experimental.pallas import tpu as pltpu
from jax.sharding import PartitionSpec as P

NEG_BIG = -1.0e30
GROUP = 4
MESH = pl.DeviceIdType.MESH
WIDTHS, FAR, CHUNK = (8, 9, 10, 12), 24, 256
LOG2_E = 1.4426950408889634
F32, BF16 = jnp.float32, jnp.bfloat16
ANY = pl.BlockSpec(memory_space=pl.ANY)
HBM = pl.BlockSpec(memory_space=pltpu.HBM)
VMEM = pl.BlockSpec(memory_space=pltpu.VMEM)
SMEM = pl.BlockSpec(memory_space=pltpu.SMEM)
MIB = 1 << 20


def dot(a, b):
    return jnp.dot(a, b, preferred_element_type=F32)


def dot_nt(a, b):
    return lax.dot_general(a, b, (((1,), (1,)), ((), ())), preferred_element_type=F32)


def dot_tn(a, b):
    return lax.dot_general(a, b, (((0,), (0,)), ((), ())), preferred_element_type=F32)


def block_of(dev, n):
    return jnp.where(dev % 2 == 0, dev // 2, n - 1 - dev // 2)


def dev_of(blk, n):
    return jnp.where(blk < n // 2, 2 * blk, 2 * (n - 1 - blk) + 1)


def at(dev):
    return (lax.axis_index('dp'), dev)


def stages_of(n):
    out, stride = [(1, min(n, 8))], min(n, 8)
    while stride < n:
        size = min(4, n // stride)
        out.append((stride, size))
        stride *= size
    return out


def peer_of(me, stride, size, j):
    idx = (me // stride) % size
    return me - idx * stride + ((idx + j) % size) * stride


def remote(src, dst, send, recv, dev):
    return pltpu.make_async_remote_copy(src_ref=src, dst_ref=dst, send_sem=send, recv_sem=recv,
                                        device_id=at(dev), device_id_type=MESH)


def column(blk, n, reach):
    out = []
    for dy in range(1, reach + 1):
        out.append((blk - GROUP * dy, blk - GROUP * dy >= 0))
        out.append((blk + GROUP * dy, blk + GROUP * dy < n))
    return out


def signal(barrier, dev):
    pl.semaphore_signal(barrier, inc=1, device_id=at(dev), device_id_type=MESH)


def column_signal(barrier, blk, n, reach):
    for other, there in column(blk, n, reach):
        @pl.when(there)
        def _():
            signal(barrier, dev_of(other, n))


def column_size(blk, n, reach):
    return jnp.minimum((n - 1 - blk) // GROUP, reach) + jnp.minimum(blk // GROUP, reach)


class Moves:
    def __init__(self, send, recv):
        self.sems, self.copies = (send, recv), []

    def new(self, src, dst, dev, go=None, come=None):
        i = len(self.copies)
        self.copies.append((remote(src, dst, self.sems[0].at[i], self.sems[1].at[i], dev), go, come))
        return i

    def when(self, cond, act):
        if cond is None:
            act()
        else:
            pl.when(cond)(act)

    def start(self, i):
        copy, go, _ = self.copies[i]
        self.when(go, copy.start)

    def arrived(self, i, then=None):
        copy, _, come = self.copies[i]

        def act():
            copy.wait_recv()
            if then is not None:
                then()
        self.when(come, act)

    def sent(self):
        for copy, go, _ in self.copies:
            self.when(go, copy.wait_send)


class Gather:
    def __init__(self, n, blk, reach, k_ref, v_ref, send, recv):
        place = blk % GROUP
        base = blk - place
        depth = reach + 1
        self.m = m = Moves(send, recv)

        def mate(r):
            return dev_of(base + (place + r) % GROUP, n)

        def later(dy):
            return dev_of(jnp.minimum(blk + GROUP * dy, n - 1), n)

        def k_at(dy, r):
            return k_ref.at[GROUP * dy + (place + r) % GROUP]

        def v_at(r, dy):
            return v_ref.at[((place + r) % GROUP) * depth + dy]

        def up(dy):
            return blk + GROUP * dy < n

        def down(dy):
            return blk - GROUP * dy >= 0

        both = up(1) & down(1)
        mid = down(2)
        self.straight = [dy for dy in range(1, reach + 1) if dy != 2]
        self.k_x = {r: m.new(k_at(0, 0), k_at(0, 0), mate(r)) for r in (1, 3, 2)}
        self.k_y = {(dy, r): m.new(k_at(0, r), k_at(dy, r), later(dy), up(dy), down(dy)) for dy in self.straight for r in range(GROUP)}
        self.v_y = {dy: m.new(v_at(0, 0), v_at(0, dy), later(dy), up(dy), down(dy)) for dy in (*self.straight, *range(2, min(reach, 2) + 1))}
        rows = [(0, None)] + [(dy, down(dy)) for dy in range(1, reach + 1)]
        self.v_x = {(dy, r): m.new(v_at(0, dy), v_at(0, dy), mate(r), c, c) for dy, c in rows for r in (1, 3)}
        self.v_xx = {dy: m.new(v_at(3, dy), v_at(3, dy), mate(1), c, c) for dy, c in rows}
        if reach > 1:
            self.k_yy = {r: m.new(k_at(1, r), k_at(2, r), later(1), both, mid) for r in range(GROUP)}
        self.reach = reach

    def own(self):
        m = self.m
        for i in self.k_x.values():
            m.start(i)
        self.k_on(0)
        for i in self.v_y.values():
            m.start(i)
        self.v_on(0)

    def k_on(self, r):
        for dy in self.straight:
            self.m.start(self.k_y[dy, r])

    def v_on(self, dy):
        for r in (1, 3):
            self.m.start(self.v_x[dy, r])

    def hand_on(self):
        m = self.m
        m.arrived(self.k_x[1])
        self.k_on(3)
        m.arrived(self.v_y[1])
        self.v_on(1)
        m.arrived(self.k_x[3])
        self.k_on(1)
        for dy in self.straight[1:]:
            m.arrived(self.v_y[dy])
            self.v_on(dy)
        m.arrived(self.v_x[0, 1])
        m.start(self.v_xx[0])
        m.arrived(self.k_y[1, 0])
        if self.reach > 1:
            m.start(self.k_yy[0])
        m.arrived(self.k_x[2])
        self.k_on(2)
        if self.reach > 1:
            m.arrived(self.v_y[2])
            self.v_on(2)

    def rest(self):
        m = self.m
        order = [1] + self.straight[1:] + ([2] if self.reach > 1 else [])
        for i in range(max(len(order), 3)):
            if i < len(order):
                m.arrived(self.v_x[order[i], 1])
                m.start(self.v_xx[order[i]])
            if i < 3:
                r = (3, 1, 2)[i]
                m.arrived(self.k_y[1, r])
                if self.reach > 1:
                    m.start(self.k_yy[r])

    def finish(self):
        m = self.m
        for dy in self.straight[1:]:
            for r in range(GROUP):
                m.arrived(self.k_y[dy, r])
        for dy in range(self.reach + 1):
            m.arrived(self.v_x[dy, 3])
            m.arrived(self.v_xx[dy])
        if self.reach > 1:
            for r in range(GROUP):
                m.arrived(self.k_yy[r])
        m.sent()


def gather_sems(reach):
    dma = pltpu.SemaphoreType.DMA
    return [dma((9 * reach + 12,)), dma((9 * reach + 12,))]


def place_documents(tab_ref, doc_ref, me):
    docs, tok = tab_ref.shape[-1], doc_ref.shape[-1]
    earlier = doc_ref[...] < lax.broadcasted_iota(jnp.int32, (docs, tok), 0)
    count = dot_nt(jnp.ones((8, tok), BF16), jnp.where(earlier, 1.0, 0.0).astype(BF16))
    tab_ref[me] = count[:1].astype(jnp.int32)


def find_documents(tab_ref, rel_ref, near_ref, which_ref, blk, tok, limits):
    n, _, docs = tab_ref.shape
    starts = jnp.sum(tab_ref[...], axis=0).astype(F32)
    lane = lax.broadcasted_iota(jnp.int32, (1, docs), 1)
    ends = jnp.where(lane == docs - 1, float(n * tok), pltpu.roll(starts, docs - 1, 1))

    def block(pos):
        return jnp.floor((pos + 0.5) * (1.0 / tok))

    span = jnp.max(jnp.where(ends > starts, block(ends - 1.0) - block(starts), 0.0)).astype(jnp.int32)
    which = jnp.int32(0)
    for w in limits:
        which = which + jnp.where(span > w, 1, 0)
    which_ref[0] = which
    cols = rel_ref.shape[1]
    pos = (lax.broadcasted_iota(jnp.int32, (1, cols), 1) % tok + blk * tok).astype(F32)
    column = jnp.broadcast_to(starts, (docs, docs)).T[:, :1]
    first = jnp.max(jnp.where(column <= pos, column, 0.0), axis=0, keepdims=True)
    rel_ref[...] = first.astype(jnp.int32) - blk * tok
    near_ref[0] = blk - block(jnp.min(first)).astype(jnp.int32)
    near_ref[1] = blk % GROUP


def project_kernel(n, reach, limits, x_ref, dy_ref, doc_ref, wq_ref, wk_ref, wv_ref, wo_ref,
                   q_ref, do_ref, k_ref, v_ref, rel_ref, near_ref, which_ref,
                   xs, dys, wq, wk, wv, wo, own_kv, own_q, own_do, tab_ref, loc_sem, swap_send, swap_recv,
                   tab_send, tab_recv, *win):
    me = lax.axis_index('cp')
    core = me % 2
    partner = me + 1 - 2 * core
    blk = block_of(me, n)
    place = blk % GROUP
    tok = x_ref.shape[0]
    half = tok // 2
    heads, _, hd = wq_ref.shape
    depth = reach + 1
    keep = pl.ds(pl.multiple_of(core * half, half), half)
    give = pl.ds(pl.multiple_of((1 - core) * half, half), half)
    front, back = pl.ds(0, half), pl.ds(half, half)
    loads = [pltpu.make_async_copy(src, dst, loc_sem.at[i]) for i, (src, dst) in enumerate((
        (x_ref, xs), (wk_ref, wk), (wv_ref, wv), (wq_ref, wq), (dy_ref, dys), (wo_ref, wo)))]
    for c in loads:
        c.start()
    barrier = pltpu.get_barrier_semaphore()
    stages = stages_of(n)
    peers = 0
    for stride, size in stages:
        for j in range(1, size):
            signal(barrier, peer_of(me, stride, size, j))
            peers += 1
    column_signal(barrier, blk, n, reach)
    place_documents(tab_ref, doc_ref, me)

    def stage_copies(s):
        stride, size = stages[s]
        rows = pl.ds(me - me % stride, stride)
        return [remote(tab_ref.at[rows], tab_ref.at[rows], tab_send.at[8 * s + j], tab_recv.at[8 * s + j],
                       peer_of(me, stride, size, j)) for j in range(1, size)]

    def q_heads(some):
        for h in some:
            own_q[h] = dot(xs[...], wq[h]).astype(BF16)
            q_ref[h, front, :] = own_q[h, keep, :]

    tables = [stage_copies(s) for s in range(len(stages))]
    other = GROUP - 1 - place
    swaps = [remote(src, dst, swap_send.at[i], swap_recv.at[i], partner) for i, (src, dst) in enumerate((
        (own_kv.at[0, give], k_ref.at[other, back]), (own_kv.at[1, give], v_ref.at[other * depth, back]),
        (own_q.at[:, give], q_ref.at[:, back]), (own_do.at[:, give], do_ref.at[:, back])))]
    gather = Gather(n, blk, reach, k_ref, v_ref, *win)

    def next_table(s):
        if s < len(stages):
            for c in tables[s - 1]:
                c.wait()
            for c in tables[s]:
                c.start()

    for c in loads[:3]:
        c.wait()
    own_kv[0] = dot(xs[...], wk[...]).astype(BF16)
    own_kv[1] = dot(xs[...], wv[...]).astype(BF16)
    k_ref[place, front, :] = own_kv[0, keep, :]
    v_ref[place * depth, front, :] = own_kv[1, keep, :]
    loads[3].wait()
    q_heads(range(1))
    pl.semaphore_wait(barrier, peers + column_size(blk, n, reach))
    for c in swaps[:2] + tables[0]:
        c.start()
    q_heads(range(1, heads))
    for c in swaps[:2]:
        c.wait_recv()
    gather.own()
    loads[4].wait()
    loads[5].wait()
    for h in range(heads):
        own_do[h] = dot_nt(dys[...], wo[pl.ds(h * hd, hd), :]).astype(BF16)
        do_ref[h, front, :] = own_do[h, keep, :]
    swaps[2].start()
    next_table(1)
    gather.hand_on()
    swaps[3].start()
    next_table(2)
    gather.rest()
    for c in tables[-1]:
        c.wait()
    find_documents(tab_ref, rel_ref, near_ref, which_ref, blk, tok, limits)
    gather.finish()
    for c in swaps[2:]:
        c.wait_recv()
    for c in swaps:
        c.wait_send()


def gather_kernel(n, reach, k_own_ref, v_own_ref, k_ref, v_ref, loc_sem, *win):
    me = lax.axis_index('cp')
    blk = block_of(me, n)
    place = blk % GROUP
    own = [pltpu.make_async_copy(k_own_ref, k_ref.at[place], loc_sem.at[0]),
           pltpu.make_async_copy(v_own_ref, v_ref.at[place * (reach + 1)], loc_sem.at[1])]
    for c in own:
        c.start()
    barrier = pltpu.get_barrier_semaphore()
    for m in range(1, GROUP):
        signal(barrier, dev_of(blk - place + (place + m) % GROUP, n))
    column_signal(barrier, blk, n, reach)
    pl.semaphore_wait(barrier, 3 + column_size(blk, n, reach))
    for c in own:
        c.wait()
    gather = Gather(n, blk, reach, k_ref, v_ref, *win)
    gather.own()
    gather.hand_on()
    gather.rest()
    gather.finish()


def attend_kernel(reach, keep, nd_ref, start_ref, q_ref, do_ref, k_ref, v_ref, o_ref, dq_ref, dk_ref, dv_ref,
                  q_t, do_t, o_t, dq_t, ds_t, top, tot, delta, *saved):
    nd = nd_ref[0]
    place = nd_ref[1]
    slots, tok, hd = k_ref.shape
    cols = q_ref.shape[0]
    scale = hd ** -0.5
    base2 = scale * LOG2_E

    def slots_of(d):
        if not reach:
            return d, d
        back = (d + GROUP - 1 - place) // GROUP
        spot = place - d + GROUP * back
        return GROUP * back + spot, spot * (reach + 1) + back

    def rows(d):
        return pl.ds(pl.multiple_of(d * tok, tok), tok)

    def clear(i, _):
        if reach:
            d = place + GROUP * (i // GROUP) - i % GROUP
            empty = (d < 0) | (d > nd)
            where = (i, (i % GROUP) * (reach + 1) + i // GROUP)
        else:
            empty, where = i > nd, (i, i)

        @pl.when(empty)
        def _():
            for ref, slot in zip((dk_ref, dv_ref), where):
                ref[slot] = jnp.zeros((tok, hd), F32)
        return 0

    lax.fori_loop(0, slots, clear, 0)
    q_t[...] = q_ref[...].T
    do_t[...] = do_ref[...].T
    top[...] = jnp.full_like(top, NEG_BIG)
    tot[...] = jnp.zeros_like(tot)
    o_t[...] = jnp.zeros_like(o_t)
    dq_t[...] = jnp.zeros_like(dq_t)

    def split(size):
        return [(lo, min(size, cols - lo)) for lo in range(0, cols, size)]

    def scores(k, d, lo, size, own):
        part = pl.ds(lo, size)
        s = dot(k, q_t[:, part])
        u = lax.broadcasted_iota(jnp.int32, (tok, size), 0)
        visible = u >= start_ref[:, part] + d * tok
        if own:
            t = (lax.broadcasted_iota(jnp.int32, (1, size), 1) + lo) % tok
            visible = visible & (u <= t + d * tok)
        return jnp.where(visible, s, NEG_BIG)

    def weight(s, part):
        return jnp.exp2(s * base2 - top[:, part])

    def find_top(d, own):
        k = k_ref[slots_of(d)[0]]
        for lo, size in split(CHUNK):
            part = pl.ds(lo, size)
            s = scores(k, d, lo, size, own)
            top[:, part] = jnp.maximum(top[:, part], jnp.max(s, axis=0, keepdims=True))
            if keep:
                saved[0][rows(d), part] = s

    def find_total(d, own):
        k = None if keep else k_ref[slots_of(d)[0]]
        for lo, size in split(CHUNK):
            part = pl.ds(lo, size)
            e = weight(saved[0][rows(d), part] if keep else scores(k, d, lo, size, own), part)
            tot[:, part] += jnp.sum(e, axis=0, keepdims=True)
            if keep:
                saved[0][rows(d), part] = e

    def forward(d, own):
        vt = v_ref[slots_of(d)[1]].T
        k = None if keep else k_ref[slots_of(d)[0]]
        for lo, size in split(CHUNK):
            part = pl.ds(lo, size)
            e = saved[0][rows(d), part] if keep else weight(scores(k, d, lo, size, own), part)
            p = (e * tot[:, part]).astype(BF16)
            if keep:
                saved[1][rows(d), part] = p
            o_t[:, part] += dot(vt, p)

    def backward(d, own):
        at_k, at_v = slots_of(d)
        k, v = k_ref[at_k], v_ref[at_v]
        kt = k.T
        p_all = saved[1].at[rows(d)] if keep else saved[0]
        for lo, size in split(CHUNK):
            part = pl.ds(lo, size)
            if not keep:
                p_all[:, part] = (weight(scores(k, d, lo, size, own), part) * tot[:, part]).astype(BF16)
            dp = dot(v, do_t[:, part])
            ds_t[:, part] = (p_all[:, part].astype(F32) * (dp - delta[:, part])).astype(BF16)
        dq_t[...] += dot(kt, ds_t[...])
        dk_ref[at_k] = dot(ds_t[...], q_ref[...]) * scale
        dv_ref[at_v] = dot(p_all[...], do_ref[...])

    def over_blocks(step, first):
        def body(d, _):
            step(d, not first)
            return 0

        if first:
            step(0, True)
        lax.fori_loop(int(first), nd + 1, body, 0)

    over_blocks(find_top, keep)
    top[...] = top[...] * base2
    over_blocks(find_total, False)
    tot[...] = 1.0 / tot[...]
    over_blocks(forward, False)
    o_bf = o_t[...].astype(BF16)
    delta[...] = jnp.sum(o_bf.astype(F32) * do_t[...].astype(F32), axis=0, keepdims=True)
    o_ref[...] = o_bf.T
    over_blocks(backward, False)
    dq_ref[...] = (dq_t[...] * scale).astype(BF16).T


class Scatter:
    def __init__(self, n, blk, reach, width, dk_ref, dv_ref, acc_k, acc_v, bufs, sems):
        place = blk % GROUP
        base = blk - place
        depth = reach + 1
        self.place, self.acc_k, self.acc_v = place, acc_k, acc_v
        self.rows = rows = (width + 3) // GROUP
        self.near_k, self.in_k, self.in_k1, self.in_k3, self.in_kx, self.side_v, self.in_v, self.in_v1 = bufs
        self.m = m = Moves(*sems)

        def mate(r):
            return dev_of(base + (place + r) % GROUP, n)

        def earlier(dy):
            return dev_of(jnp.maximum(blk - GROUP * dy, 0), n)

        def down(dy):
            return blk - GROUP * dy >= 0

        def up(dy):
            return blk + GROUP * dy < n

        def need(dy, place):
            return GROUP * dy - width <= place

        def both_of(a, b):
            return b if a is None else a & b

        def asked(dy, r):
            return None if need(dy, 0) else need(dy, (place + r) % GROUP)

        both = up(1) & down(1)
        here, there = range(rows + 1), [(dy, j) for dy in range(3, rows + 1) for j in range(GROUP) if need(dy, j)]
        self.k_yy = {j: m.new(dk_ref.at[2 * GROUP + j], self.in_k.at[j], earlier(1), down(2), both)
                     for j in range(GROUP) if rows > 1 and need(2, j)}
        self.k_y = {(dy, j): m.new(dk_ref.at[GROUP * dy + j], self.in_k3.at[dy - 3, j], earlier(dy), down(dy), up(dy))
                    for dy, j in there}
        self.k_y1 = [m.new(self.near_k.at[j], self.in_k1.at[j], earlier(1), down(1), up(1)) for j in range(GROUP)]
        self.k_x = [m.new(acc_k.at[(place + r) % GROUP], self.in_kx.at[r - 1], mate(r)) for r in (2, 1, 3)]

        def term(r, dy):
            return dv_ref.at[((place + r) % GROUP) * depth + dy]

        self.v_xx = [m.new(term(2, dy), self.in_v.at[0, dy], mate(3), asked(dy, 2), asked(dy, 3)) for dy in here]
        self.v_xu = [m.new(term(1, dy), self.in_v.at[1, dy], mate(1), asked(dy, 1), asked(dy, 0)) for dy in here]
        self.v_xd = [m.new(self.side_v.at[dy], self.in_v.at[2, dy], mate(3), asked(dy, 3), asked(dy, 0)) for dy in here]
        self.v_y = {dy: m.new(acc_v.at[dy], self.in_v1.at[dy - 1], earlier(dy),
                              both_of(asked(dy, 0), down(dy)), both_of(asked(dy, 0), up(dy))) for dy in here[1:]}
        self.order = [*here[2:], 1, 0]

    def start(self):
        m = self.m
        for dy in self.order:
            m.start(self.v_xx[dy])
            m.start(self.v_xu[dy])
        for i in (*self.k_yy.values(), *self.k_y.values()):
            m.start(i)

    def add(self, ref, at, buf, *slot):
        def act():
            ref[at] += buf[slot]
        return act

    def first_half(self):
        m, add = self.m, self.add
        for i in range(max(len(self.order), GROUP)):
            if i < len(self.order):
                dy = self.order[i]
                m.arrived(self.v_xx[dy], add(self.side_v, dy, self.in_v, 0, dy))
                m.start(self.v_xd[dy])
            if i < GROUP:
                if i in self.k_yy:
                    m.arrived(self.k_yy[i], add(self.near_k, i, self.in_k, i))
                m.start(self.k_y1[i])

    def second_half(self):
        m, add, acc_k, acc_v = self.m, self.add, self.acc_k, self.acc_v
        for i in range(max(len(self.order), GROUP)):
            if i < len(self.order):
                dy = self.order[i]
                m.arrived(self.v_xu[dy], add(acc_v, dy, self.in_v, 1, dy))
                m.arrived(self.v_xd[dy], add(acc_v, dy, self.in_v, 2, dy))
                if dy:
                    m.start(self.v_y[dy])
            if i < GROUP:
                for (dy, j), move in self.k_y.items():
                    if j == i:
                        m.arrived(move, add(acc_k, j, self.in_k3, dy - 3, j))
                m.arrived(self.k_y1[i], add(acc_k, i, self.in_k1, i))
        for i in self.k_x:
            m.start(i)
        for dy, move in self.v_y.items():
            m.arrived(move, add(acc_v, 0, self.in_v1, dy - 1))
        for i in self.k_x:
            m.arrived(i)
        return acc_k[self.place] + self.in_kx[0] + self.in_kx[1] + self.in_kx[2]


def scatter_bufs(width, tok, hd):
    rows = (width + 3) // GROUP
    more = max(rows - 2, 1)
    dma = pltpu.SemaphoreType.DMA
    shapes = [(GROUP,), (GROUP,), (GROUP,), (more, GROUP), (3,), (rows + 1,), (3, rows + 1), (rows,)]
    return [pltpu.VMEM((*shape, tok, hd), F32) for shape in shapes] + [dma((8 * rows + 16,)), dma((8 * rows + 16,))]


def finish_kernel(n, reach, width, dk_ref, dv_ref, o, dq, wq, wk, wv, wo_ref, y_ref, dx_ref,
                  acc_k, acc_v, wo, wo_sem, y_give, dx_give, dx_part, swap_send, swap_recv, *win):
    me = lax.axis_index('cp')
    core = me % 2
    partner = me + 1 - 2 * core
    blk = block_of(me, n)
    place = blk % GROUP
    base = blk - place
    tok = y_ref.shape[0]
    half = tok // 2
    heads, d_model, hd = wq.shape
    rows = (width + 3) // GROUP
    depth = reach + 1
    mine = pl.ds(pl.multiple_of(core * half, half), half)
    load = pltpu.make_async_copy(wo_ref, wo, wo_sem)
    load.start()
    barrier = pltpu.get_barrier_semaphore()
    signal(barrier, partner)
    if reach:
        for r in range(1, GROUP):
            signal(barrier, dev_of(base + (place + r) % GROUP, n))
        column_signal(barrier, blk, n, rows)
        pl.semaphore_wait(barrier, GROUP + column_size(blk, n, rows))
        bufs, sems = win[:-2], win[-2:]
        scatter = Scatter(n, blk, reach, width, dk_ref, dv_ref, acc_k, acc_v, bufs, sems)
        scatter.start()
        scatter.side_v[...] = dv_ref[pl.ds(((place + 3) % GROUP) * depth, rows + 1)]
        scatter.near_k[...] = dk_ref[pl.ds(GROUP, GROUP)]
        acc_v[...] = dv_ref[pl.ds(place * depth, rows + 1)]
        acc_k[...] = dk_ref[pl.ds(0, GROUP)]
        scatter.first_half()
    else:
        pl.semaphore_wait(barrier, 1)
        acc_v[...], acc_k[...] = dv_ref[...], dk_ref[...]
    load.wait()
    o_cat = jnp.concatenate([o[pl.ds(h * tok, tok), :] for h in range(heads)], axis=1)
    y = dot(o_cat, wo[...]).astype(BF16)
    y_give[...] = y[half:]
    y_ref[mine, :] = y[:half]
    dx = dot_nt(dq[pl.ds(0, tok), :], wq[0])
    for h in range(1, heads):
        dx += dot_nt(dq[pl.ds(h * tok, tok), :], wq[h])
    dx_part[...] = dx
    swap_y = remote(y_give, y_ref.at[mine], swap_send.at[0], swap_recv.at[0], partner)
    swap_y.start()
    total_k = scatter.second_half() if reach else acc_k[0]
    dk = total_k.astype(BF16)
    dv = acc_v[0].astype(BF16)

    def dx_rows(lo):
        part = slice(lo, lo + half)
        return (dx_part[pl.ds(lo, half), :] + dot_nt(dk[part], wk[...]) + dot_nt(dv[part], wv[...])).astype(BF16)

    dx_give[...] = dx_rows(half)
    dx_ref[mine, :] = dx_rows(0)
    swap_dx = remote(dx_give, dx_ref.at[mine], swap_send.at[1], swap_recv.at[1], partner)
    swap_dx.start()
    if reach:
        scatter.m.sent()
    swap_y.wait()
    swap_dx.wait()


def copy_kernel(y_ref, dx_ref, y_out, dx_out, sem):
    copies = [pltpu.make_async_copy(y_ref, y_out, sem.at[0]), pltpu.make_async_copy(dx_ref, dx_out, sem.at[1])]
    for c in copies:
        c.start()
    for c in copies:
        c.wait()


def make_layer(n, widths, far):
    dma = pltpu.SemaphoreType.DMA
    near = widths[-1]

    def comm(cid, mib=28):
        return pltpu.CompilerParams(collective_id=cid, has_side_effects=True, vmem_limit_bytes=mib * MIB)

    def local_layer(x_in, dy_in, doc_id, w_q, w_k, w_v, w_o):
        tok, d_model = x_in.shape
        heads, hd = w_q.shape[1], w_q.shape[2]
        cols = heads * tok
        me = lax.axis_index('cp')
        blk = block_of(me, n)
        place = blk % GROUP
        wq = jnp.transpose(w_q, (1, 0, 2))
        wk = w_k.reshape(d_model, hd)
        wv = w_v.reshape(d_model, hd)
        wo = w_o.reshape(heads * hd, d_model)
        n_stage = len(stages_of(n))
        reach = (near + 3) // GROUP

        def window(reach, dtype=BF16):
            return jax.ShapeDtypeStruct((GROUP * (reach + 1), tok, hd), dtype)

        q, do, k_win, v_win, rel, nd, which = pl.pallas_call(
            functools.partial(project_kernel, n, reach, (*widths, far)),
            out_shape=(jax.ShapeDtypeStruct((heads, tok, hd), BF16), jax.ShapeDtypeStruct((heads, tok, hd), BF16),
                       window(reach), window(reach), jax.ShapeDtypeStruct((1, cols), jnp.int32),
                       jax.ShapeDtypeStruct((2,), jnp.int32), jax.ShapeDtypeStruct((1,), jnp.int32)),
            in_specs=[HBM, HBM, VMEM, HBM, HBM, HBM, HBM],
            out_specs=(VMEM, VMEM, VMEM, VMEM, VMEM, SMEM, SMEM),
            scratch_shapes=[pltpu.VMEM((tok, d_model), BF16), pltpu.VMEM((tok, d_model), BF16),
                            pltpu.VMEM(wq.shape, BF16), pltpu.VMEM(wk.shape, BF16), pltpu.VMEM(wv.shape, BF16),
                            pltpu.VMEM(wo.shape, BF16), pltpu.VMEM((2, tok, hd), BF16),
                            pltpu.VMEM((heads, tok, hd), BF16), pltpu.VMEM((heads, tok, hd), BF16),
                            pltpu.VMEM((n, 1, 128), jnp.int32), dma((6,)), dma((4,)), dma((4,)), dma((8 * n_stage,)), dma((8 * n_stage,))] + gather_sems(reach),
            compiler_params=comm(0, 60),
            name='project',
        )(x_in, dy_in, doc_id.reshape(1, tok), wq, wk, wv, wo)
        q, do = q.reshape(cols, hd), do.reshape(cols, hd)

        def attend(k, v, width, reach):
            saved = [pltpu.VMEM((tok, cols), BF16)]
            if width:
                saved = [pltpu.VMEM(((width + 1) * tok, cols), F32), pltpu.VMEM(((width + 1) * tok, cols), BF16)]
            row = pltpu.VMEM((1, cols), F32)
            return pl.pallas_call(
                functools.partial(attend_kernel, reach, bool(width)),
                out_shape=(jax.ShapeDtypeStruct((cols, hd), BF16), jax.ShapeDtypeStruct((cols, hd), BF16),
                           jax.ShapeDtypeStruct(k.shape, F32), jax.ShapeDtypeStruct(k.shape, F32)),
                in_specs=[SMEM, VMEM, VMEM, VMEM, VMEM, VMEM],
                out_specs=(VMEM, VMEM, VMEM, VMEM),
                scratch_shapes=[pltpu.VMEM((hd, cols), BF16), pltpu.VMEM((hd, cols), BF16),
                                pltpu.VMEM((hd, cols), F32), pltpu.VMEM((hd, cols), F32), pltpu.VMEM((tok, cols), BF16),
                                row, row, row] + saved,
                compiler_params=pltpu.CompilerParams(vmem_limit_bytes=(36 if width == near else 60) * MIB),
                name='attend',
            )(nd, rel, q, do, k, v)

        def finish(dk, dv, o, dq, reach, width, cid):
            rows = (width + 3) // GROUP
            win = scatter_bufs(width, tok, hd) if reach else []
            results = pl.pallas_call(
                functools.partial(finish_kernel, n, reach, width),
                out_shape=(jax.ShapeDtypeStruct((tok, d_model), BF16), jax.ShapeDtypeStruct((tok, d_model), BF16)),
                in_specs=[VMEM] * 7 + [ANY],
                out_specs=(VMEM, VMEM),
                scratch_shapes=[pltpu.VMEM((4 if reach else 1, tok, hd), F32), pltpu.VMEM((rows + 1, tok, hd), F32),
                                pltpu.VMEM(wo.shape, BF16), dma, pltpu.VMEM((tok // 2, d_model), BF16), pltpu.VMEM((tok // 2, d_model), BF16),
                                pltpu.VMEM((tok, d_model), F32), dma((2,)), dma((2,))] + win,
                compiler_params=comm(cid, 60 if width == far else 28),
                name='finish',
            )(dk, dv, o, dq, wq, wk, wv, wo)
            return pl.pallas_call(
                copy_kernel, out_shape=(jax.ShapeDtypeStruct((tok, d_model), BF16),) * 2,
                in_specs=[VMEM] * 2, out_specs=(ANY, ANY), scratch_shapes=[dma((2,))],
                compiler_params=pltpu.CompilerParams(vmem_limit_bytes=4 * MIB), name='copy')(*results)

        def with_near(width, cid):
            def run(k, v):
                o, dq, dk, dv = attend(k, v, near, reach)
                return finish(dk, dv, o, dq, reach, width, cid)
            return run

        def own(k, v):
            return (lax.dynamic_index_in_dim(k, place, 0, keepdims=False),
                    lax.dynamic_index_in_dim(v, place * (reach + 1), 0, keepdims=False))

        def with_far(k, v):
            reach = (far + 3) // GROUP
            k, v = pl.pallas_call(
                functools.partial(gather_kernel, n, reach),
                out_shape=(window(reach), window(reach)),
                in_specs=[ANY, ANY], out_specs=(ANY, ANY),
                scratch_shapes=[dma((2,))] + gather_sems(reach),
                compiler_params=comm(1),
                name='gather',
            )(*own(k, v))
            o, dq, dk, dv = attend(k, v, far, reach)
            return finish(dk, dv, o, dq, reach, far, 2)

        order = [2 * b if b < n // 2 else 2 * (n - 1 - b) + 1 for b in range(n)]
        up = [(order[b], order[(b + 1) % n]) for b in range(n)]
        down = [(dst, src) for src, dst in up]

        def with_all(k, v):
            def pull(d, state):
                held, k, v = state
                held = lax.ppermute(held, 'cp', up)
                return held, k.at[d].set(held[0]), v.at[d].set(held[1])

            held = jnp.stack(own(k, v))
            empty = jnp.zeros((n, tok, hd), BF16)
            _, k, v = lax.fori_loop(1, n, pull, (held, empty.at[0].set(held[0]), empty.at[0].set(held[1])))
            o, dq, dk, dv = attend(k, v, 0, 0)

            def push(step, acc):
                d = n - 1 - step
                acc = acc + jnp.stack([lax.dynamic_index_in_dim(dk, d, 0, keepdims=False),
                                       lax.dynamic_index_in_dim(dv, d, 0, keepdims=False)])
                return lax.ppermute(acc, 'cp', down)

            acc = lax.fori_loop(0, n - 1, push, jnp.zeros((2, tok, hd), F32))
            return finish((acc[0] + dk[0])[None], (acc[1] + dv[0])[None], o, dq, 0, 0, 3)

        branches = [with_near(w, 4 + i) for i, w in enumerate(widths)] + [with_far, with_all]
        return lax.switch(which[0], branches, k_win, v_win)

    return local_layer


def solution(mesh, widths=WIDTHS, far=FAR):
    n = mesh.shape['cp']
    row_spec = P(('dp', 'cp'))
    full_spec = P()
    return jax.shard_map(make_layer(n, widths, far), mesh=mesh,
                         in_specs=(row_spec, row_spec, row_spec, full_spec, full_spec, full_spec, full_spec),
                         out_specs=(row_spec, row_spec), check_vma=False)
```

```python
import functools

import jax
import jax.numpy as jnp
from jax import lax
from jax.experimental import pallas as pl
from jax.experimental.pallas import tpu as pltpu
from jax.sharding import PartitionSpec as P

NEG_BIG = -1.0e30
GROUP = 4
MESH = pl.DeviceIdType.MESH
WIDTHS, FAR, CHUNK = (8, 9, 10, 12), 24, 256
LOG2_E = 1.4426950408889634
F32, BF16 = jnp.float32, jnp.bfloat16
ANY = pl.BlockSpec(memory_space=pl.ANY)
HBM = pl.BlockSpec(memory_space=pltpu.HBM)
VMEM = pl.BlockSpec(memory_space=pltpu.VMEM)
SMEM = pl.BlockSpec(memory_space=pltpu.SMEM)
MIB = 1 << 20


def dot(a, b):
    return jnp.dot(a, b, preferred_element_type=F32)


def dot_nt(a, b):
    return lax.dot_general(a, b, (((1,), (1,)), ((), ())), preferred_element_type=F32)


def dot_tn(a, b):
    return lax.dot_general(a, b, (((0,), (0,)), ((), ())), preferred_element_type=F32)


def block_of(dev, n):
    return jnp.where(dev % 2 == 0, dev // 2, n - 1 - dev // 2)


def dev_of(blk, n):
    return jnp.where(blk < n // 2, 2 * blk, 2 * (n - 1 - blk) + 1)


def at(dev):
    return (lax.axis_index('dp'), dev)


def stages_of(n):
    out, stride = [(1, min(n, 8))], min(n, 8)
    while stride < n:
        size = min(4, n // stride)
        out.append((stride, size))
        stride *= size
    return out


def peer_of(me, stride, size, j):
    idx = (me // stride) % size
    return me - idx * stride + ((idx + j) % size) * stride


def remote(src, dst, send, recv, dev):
    return pltpu.make_async_remote_copy(src_ref=src, dst_ref=dst, send_sem=send, recv_sem=recv,
                                        device_id=at(dev), device_id_type=MESH)


def column(blk, n, reach):
    out = []
    for dy in range(1, reach + 1):
        out.append((blk - GROUP * dy, blk - GROUP * dy >= 0))
        out.append((blk + GROUP * dy, blk + GROUP * dy < n))
    return out


def signal(barrier, dev):
    pl.semaphore_signal(barrier, inc=1, device_id=at(dev), device_id_type=MESH)


def column_signal(barrier, blk, n, reach):
    for other, there in column(blk, n, reach):
        @pl.when(there)
        def _():
            signal(barrier, dev_of(other, n))


def column_size(blk, n, reach):
    return jnp.minimum((n - 1 - blk) // GROUP, reach) + jnp.minimum(blk // GROUP, reach)


class Moves:
    def __init__(self, send, recv):
        self.sems, self.copies = (send, recv), []

    def new(self, src, dst, dev, go=None, come=None):
        i = len(self.copies)
        self.copies.append((remote(src, dst, self.sems[0].at[i], self.sems[1].at[i], dev), go, come))
        return i

    def when(self, cond, act):
        if cond is None:
            act()
        else:
            pl.when(cond)(act)

    def start(self, i):
        copy, go, _ = self.copies[i]
        self.when(go, copy.start)

    def arrived(self, i, then=None):
        copy, _, come = self.copies[i]

        def act():
            copy.wait_recv()
            if then is not None:
                then()
        self.when(come, act)

    def sent(self):
        for copy, go, _ in self.copies:
            self.when(go, copy.wait_send)


class Gather:
    def __init__(self, n, blk, reach, k_ref, v_ref, send, recv):
        place = blk % GROUP
        base = blk - place
        depth = reach + 1
        self.m = m = Moves(send, recv)

        def mate(r):
            return dev_of(base + (place + r) % GROUP, n)

        def later(dy):
            return dev_of(jnp.minimum(blk + GROUP * dy, n - 1), n)

        def k_at(dy, r):
            return k_ref.at[GROUP * dy + (place + r) % GROUP]

        def v_at(r, dy):
            return v_ref.at[((place + r) % GROUP) * depth + dy]

        def up(dy):
            return blk + GROUP * dy < n

        def down(dy):
            return blk - GROUP * dy >= 0

        both = up(1) & down(1)
        mid = down(2)
        self.straight = [dy for dy in range(1, reach + 1) if dy != 2]
        self.k_x = {r: m.new(k_at(0, 0), k_at(0, 0), mate(r)) for r in (1, 3, 2)}
        self.k_y = {(dy, r): m.new(k_at(0, r), k_at(dy, r), later(dy), up(dy), down(dy)) for dy in self.straight for r in range(GROUP)}
        self.v_y = {dy: m.new(v_at(0, 0), v_at(0, dy), later(dy), up(dy), down(dy)) for dy in (*self.straight, *range(2, min(reach, 2) + 1))}
        rows = [(0, None)] + [(dy, down(dy)) for dy in range(1, reach + 1)]
        self.v_x = {(dy, r): m.new(v_at(0, dy), v_at(0, dy), mate(r), c, c) for dy, c in rows for r in (1, 3)}
        self.v_xx = {dy: m.new(v_at(0, 2), v_at(0, 2), mate(2), c, c) if dy == 2 else
                     m.new(v_at(3, dy), v_at(3, dy), mate(1), c, c) for dy, c in rows}
        if reach > 1:
            self.k_yy = {r: m.new(k_at(0, 2), k_at(2, 2), later(2), up(2), mid) if r == 2 else
                         m.new(k_at(1, r), k_at(2, r), later(1), both, mid) for r in range(GROUP)}
        self.reach = reach

    def own(self):
        m = self.m
        for i in self.k_x.values():
            m.start(i)
        self.k_on(0)
        for i in self.v_y.values():
            m.start(i)
        self.v_on(0)

    def k_on(self, r):
        for dy in self.straight:
            self.m.start(self.k_y[dy, r])
        if r == 2 and self.reach > 1:
            self.m.start(self.k_yy[r])

    def v_on(self, dy):
        for r in (1, 3):
            self.m.start(self.v_x[dy, r])
        if dy == 2:
            self.m.start(self.v_xx[dy])

    def hand_on(self):
        m = self.m
        m.arrived(self.k_x[1])
        self.k_on(3)
        m.arrived(self.v_y[1])
        self.v_on(1)
        m.arrived(self.k_x[3])
        self.k_on(1)
        for dy in self.straight[1:]:
            m.arrived(self.v_y[dy])
            self.v_on(dy)
        m.arrived(self.v_x[0, 1])
        m.start(self.v_xx[0])
        m.arrived(self.k_y[1, 0])
        if self.reach > 1:
            m.start(self.k_yy[0])
        m.arrived(self.k_x[2])
        self.k_on(2)
        if self.reach > 1:
            m.arrived(self.v_y[2])
            self.v_on(2)

    def rest(self):
        m = self.m
        order = [1] + self.straight[1:] + ([2] if self.reach > 1 else [])
        for i in range(max(len(order), 3)):
            if i < len(order):
                m.arrived(self.v_x[order[i], 1])
                if order[i] != 2:
                    m.start(self.v_xx[order[i]])
            if i < 3:
                r = (3, 1, 2)[i]
                m.arrived(self.k_y[1, r])
                if self.reach > 1 and r != 2:
                    m.start(self.k_yy[r])

    def finish(self):
        m = self.m
        for dy in self.straight[1:]:
            for r in range(GROUP):
                m.arrived(self.k_y[dy, r])
        for dy in range(self.reach + 1):
            m.arrived(self.v_x[dy, 3])
            m.arrived(self.v_xx[dy])
        if self.reach > 1:
            for r in range(GROUP):
                m.arrived(self.k_yy[r])
        m.sent()


def gather_sems(reach):
    dma = pltpu.SemaphoreType.DMA
    return [dma((9 * reach + 12,)), dma((9 * reach + 12,))]


def place_documents(tab_ref, doc_ref, me):
    docs, tok = tab_ref.shape[-1], doc_ref.shape[-1]
    earlier = doc_ref[...] < lax.broadcasted_iota(jnp.int32, (docs, tok), 0)
    count = dot_nt(jnp.ones((8, tok), BF16), jnp.where(earlier, 1.0, 0.0).astype(BF16))
    tab_ref[me] = count[:1].astype(jnp.int32)


def find_documents(tab_ref, rel_ref, near_ref, which_ref, blk, tok, limits):
    n, _, docs = tab_ref.shape
    starts = jnp.sum(tab_ref[...], axis=0).astype(F32)
    lane = lax.broadcasted_iota(jnp.int32, (1, docs), 1)
    ends = jnp.where(lane == docs - 1, float(n * tok), pltpu.roll(starts, docs - 1, 1))

    def block(pos):
        return jnp.floor((pos + 0.5) * (1.0 / tok))

    span = jnp.max(jnp.where(ends > starts, block(ends - 1.0) - block(starts), 0.0)).astype(jnp.int32)
    which = jnp.int32(0)
    for w in limits:
        which = which + jnp.where(span > w, 1, 0)
    which_ref[0] = which
    cols = rel_ref.shape[1]
    pos = (lax.broadcasted_iota(jnp.int32, (1, cols), 1) % tok + blk * tok).astype(F32)
    column = jnp.broadcast_to(starts, (docs, docs)).T[:, :1]
    first = jnp.max(jnp.where(column <= pos, column, 0.0), axis=0, keepdims=True)
    rel_ref[...] = first.astype(jnp.int32) - blk * tok
    near_ref[0] = blk - block(jnp.min(first)).astype(jnp.int32)
    near_ref[1] = blk % GROUP


def project_kernel(n, reach, limits, x_ref, dy_ref, doc_ref, wq_ref, wk_ref, wv_ref, wo_ref,
                   q_ref, do_ref, k_ref, v_ref, rel_ref, near_ref, which_ref,
                   xs, dys, wq, wk, wv, wo, own_kv, own_q, own_do, tab_ref, loc_sem, swap_send, swap_recv,
                   tab_send, tab_recv, *win):
    me = lax.axis_index('cp')
    core = me % 2
    partner = me + 1 - 2 * core
    blk = block_of(me, n)
    place = blk % GROUP
    tok = x_ref.shape[0]
    half = tok // 2
    heads, _, hd = wq_ref.shape
    depth = reach + 1
    keep = pl.ds(pl.multiple_of(core * half, half), half)
    give = pl.ds(pl.multiple_of((1 - core) * half, half), half)
    front, back = pl.ds(0, half), pl.ds(half, half)
    loads = [pltpu.make_async_copy(src, dst, loc_sem.at[i]) for i, (src, dst) in enumerate((
        (x_ref, xs), (wk_ref, wk), (wv_ref, wv), (wq_ref, wq), (dy_ref, dys), (wo_ref, wo)))]
    for c in loads:
        c.start()
    barrier = pltpu.get_barrier_semaphore()
    stages = stages_of(n)
    peers = 0
    for stride, size in stages:
        for j in range(1, size):
            signal(barrier, peer_of(me, stride, size, j))
            peers += 1
    column_signal(barrier, blk, n, reach)
    place_documents(tab_ref, doc_ref, me)

    def stage_copies(s):
        stride, size = stages[s]
        rows = pl.ds(me - me % stride, stride)
        return [remote(tab_ref.at[rows], tab_ref.at[rows], tab_send.at[8 * s + j], tab_recv.at[8 * s + j],
                       peer_of(me, stride, size, j)) for j in range(1, size)]

    def q_heads(some):
        for h in some:
            own_q[h] = dot(xs[...], wq[h]).astype(BF16)
            q_ref[h, front, :] = own_q[h, keep, :]

    tables = [stage_copies(s) for s in range(len(stages))]
    other = GROUP - 1 - place
    swaps = [remote(src, dst, swap_send.at[i], swap_recv.at[i], partner) for i, (src, dst) in enumerate((
        (own_kv.at[0, give], k_ref.at[other, back]), (own_kv.at[1, give], v_ref.at[other * depth, back]),
        (own_q.at[:, give], q_ref.at[:, back]), (own_do.at[:, give], do_ref.at[:, back])))]
    gather = Gather(n, blk, reach, k_ref, v_ref, *win)

    def next_table(s):
        if s < len(stages):
            for c in tables[s - 1]:
                c.wait()
            for c in tables[s]:
                c.start()

    for c in loads[:3]:
        c.wait()
    own_kv[0] = dot(xs[...], wk[...]).astype(BF16)
    own_kv[1] = dot(xs[...], wv[...]).astype(BF16)
    k_ref[place, front, :] = own_kv[0, keep, :]
    v_ref[place * depth, front, :] = own_kv[1, keep, :]
    loads[3].wait()
    q_heads(range(1))
    pl.semaphore_wait(barrier, peers + column_size(blk, n, reach))
    for c in swaps[:2] + tables[0]:
        c.start()
    q_heads(range(1, heads))
    for c in swaps[:2]:
        c.wait_recv()
    gather.own()
    loads[4].wait()
    loads[5].wait()
    for h in range(heads):
        own_do[h] = dot_nt(dys[...], wo[pl.ds(h * hd, hd), :]).astype(BF16)
        do_ref[h, front, :] = own_do[h, keep, :]
    swaps[2].start()
    next_table(1)
    gather.hand_on()
    swaps[3].start()
    next_table(2)
    gather.rest()
    for c in tables[-1]:
        c.wait()
    find_documents(tab_ref, rel_ref, near_ref, which_ref, blk, tok, limits)
    gather.finish()
    for c in swaps[2:]:
        c.wait_recv()
    for c in swaps:
        c.wait_send()


def gather_kernel(n, reach, k_own_ref, v_own_ref, k_ref, v_ref, loc_sem, *win):
    me = lax.axis_index('cp')
    blk = block_of(me, n)
    place = blk % GROUP
    own = [pltpu.make_async_copy(k_own_ref, k_ref.at[place], loc_sem.at[0]),
           pltpu.make_async_copy(v_own_ref, v_ref.at[place * (reach + 1)], loc_sem.at[1])]
    for c in own:
        c.start()
    barrier = pltpu.get_barrier_semaphore()
    for m in range(1, GROUP):
        signal(barrier, dev_of(blk - place + (place + m) % GROUP, n))
    column_signal(barrier, blk, n, reach)
    pl.semaphore_wait(barrier, 3 + column_size(blk, n, reach))
    for c in own:
        c.wait()
    gather = Gather(n, blk, reach, k_ref, v_ref, *win)
    gather.own()
    gather.hand_on()
    gather.rest()
    gather.finish()


def attend_kernel(reach, keep, nd_ref, start_ref, q_ref, do_ref, k_far, v_far, o_ref, dq_ref, dk_ref, dv_ref,
                  k_ref, v_ref, load_sem, q_t, do_t, o_t, dq_t, ds_t, top, tot, delta, *saved):
    nd = nd_ref[0]
    place = nd_ref[1]
    slots, tok, hd = k_ref.shape
    cols = q_ref.shape[0]
    scale = hd ** -0.5
    base2 = scale * LOG2_E

    def slots_of(d):
        if not reach:
            return d, d
        back = (d + GROUP - 1 - place) // GROUP
        spot = place - d + GROUP * back
        return GROUP * back + spot, spot * (reach + 1) + back

    def rows(d):
        return pl.ds(pl.multiple_of(d * tok, tok), tok)

    loads = [pltpu.make_async_copy(k_far, k_ref, load_sem.at[0]), pltpu.make_async_copy(v_far, v_ref, load_sem.at[1])]
    for c in loads:
        c.start()

    def clear(i, _):
        if reach:
            d = place + GROUP * (i // GROUP) - i % GROUP
            empty = (d < 0) | (d > nd)
            where = (i, (i % GROUP) * (reach + 1) + i // GROUP)
        else:
            empty, where = i > nd, (i, i)

        @pl.when(empty)
        def _():
            for ref, slot in zip((dk_ref, dv_ref), where):
                ref[slot] = jnp.zeros((tok, hd), F32)
        return 0

    lax.fori_loop(0, slots, clear, 0)
    q_t[...] = q_ref[...].T
    do_t[...] = do_ref[...].T
    top[...] = jnp.full_like(top, NEG_BIG)
    tot[...] = jnp.zeros_like(tot)
    o_t[...] = jnp.zeros_like(o_t)
    dq_t[...] = jnp.zeros_like(dq_t)
    for c in loads:
        c.wait()

    def split(size):
        return [(lo, min(size, cols - lo)) for lo in range(0, cols, size)]

    def scores(k, d, lo, size, own):
        part = pl.ds(lo, size)
        s = dot(k, q_t[:, part])
        u = lax.broadcasted_iota(jnp.int32, (tok, size), 0)
        visible = u >= start_ref[:, part] + d * tok
        if own:
            t = (lax.broadcasted_iota(jnp.int32, (1, size), 1) + lo) % tok
            visible = visible & (u <= t + d * tok)
        return jnp.where(visible, s, NEG_BIG)

    def weight(s, part):
        return jnp.exp2(s * base2 - top[:, part])

    def find_top(d, own):
        k = k_ref[slots_of(d)[0]]
        for lo, size in split(CHUNK):
            part = pl.ds(lo, size)
            s = scores(k, d, lo, size, own)
            top[:, part] = jnp.maximum(top[:, part], jnp.max(s, axis=0, keepdims=True))
            if keep:
                saved[0][rows(d), part] = s

    def find_total(d, own):
        k = None if keep else k_ref[slots_of(d)[0]]
        for lo, size in split(CHUNK):
            part = pl.ds(lo, size)
            e = weight(saved[0][rows(d), part] if keep else scores(k, d, lo, size, own), part)
            tot[:, part] += jnp.sum(e, axis=0, keepdims=True)
            if keep:
                saved[0][rows(d), part] = e

    def forward(d, own):
        vt = v_ref[slots_of(d)[1]].T
        k = None if keep else k_ref[slots_of(d)[0]]
        for lo, size in split(CHUNK):
            part = pl.ds(lo, size)
            e = saved[0][rows(d), part] if keep else weight(scores(k, d, lo, size, own), part)
            p = (e * tot[:, part]).astype(BF16)
            if keep:
                saved[1][rows(d), part] = p
            o_t[:, part] += dot(vt, p)

    def backward(d, own):
        at_k, at_v = slots_of(d)
        k, v = k_ref[at_k], v_ref[at_v]
        kt = k.T
        p_all = saved[1].at[rows(d)] if keep else saved[0]
        for lo, size in split(CHUNK):
            part = pl.ds(lo, size)
            if not keep:
                p_all[:, part] = (weight(scores(k, d, lo, size, own), part) * tot[:, part]).astype(BF16)
            dp = dot(v, do_t[:, part])
            ds_t[:, part] = (p_all[:, part].astype(F32) * (dp - delta[:, part])).astype(BF16)
        dq_t[...] += dot(kt, ds_t[...])
        dk_ref[at_k] = dot(ds_t[...], q_ref[...]) * scale
        dv_ref[at_v] = dot(p_all[...], do_ref[...])

    def over_blocks(step, first):
        def body(d, _):
            step(d, not first)
            return 0

        if first:
            step(0, True)
        lax.fori_loop(int(first), nd + 1, body, 0)

    over_blocks(find_top, keep)
    top[...] = top[...] * base2
    over_blocks(find_total, False)
    tot[...] = 1.0 / tot[...]
    over_blocks(forward, False)
    o_bf = o_t[...].astype(BF16)
    delta[...] = jnp.sum(o_bf.astype(F32) * do_t[...].astype(F32), axis=0, keepdims=True)
    o_ref[...] = o_bf.T
    over_blocks(backward, False)
    dq_ref[...] = (dq_t[...] * scale).astype(BF16).T


class Scatter:
    def __init__(self, n, blk, reach, width, dk_ref, dv_ref, acc_k, acc_v, bufs, sems):
        place = blk % GROUP
        base = blk - place
        depth = reach + 1
        self.place, self.acc_k, self.acc_v = place, acc_k, acc_v
        self.rows = rows = (width + 3) // GROUP
        self.near_k, self.in_k, self.in_k1, self.in_k3, self.in_kx, self.side_v, self.in_v, self.in_v1 = bufs
        self.m = m = Moves(*sems)

        def mate(r):
            return dev_of(base + (place + r) % GROUP, n)

        def earlier(dy):
            return dev_of(jnp.maximum(blk - GROUP * dy, 0), n)

        def down(dy):
            return blk - GROUP * dy >= 0

        def up(dy):
            return blk + GROUP * dy < n

        def need(dy, place):
            return GROUP * dy - width <= place

        def both_of(a, b):
            return b if a is None else a & b

        def asked(dy, r):
            return None if need(dy, 0) else need(dy, (place + r) % GROUP)

        both = up(1) & down(1)
        here, there = range(rows + 1), [(dy, j) for dy in range(3, rows + 1) for j in range(GROUP) if need(dy, j)]
        self.k_yy = {j: m.new(dk_ref.at[2 * GROUP + j], self.in_k.at[j], earlier(1), down(2), both)
                     for j in range(GROUP) if rows > 1 and need(2, j)}
        self.k_y = {(dy, j): m.new(dk_ref.at[GROUP * dy + j], self.in_k3.at[dy - 3, j], earlier(dy), down(dy), up(dy))
                    for dy, j in there}
        self.k_y1 = [m.new(self.near_k.at[j], self.in_k1.at[j], earlier(1), down(1), up(1)) for j in range(GROUP)]
        self.k_x = [m.new(acc_k.at[(place + r) % GROUP], self.in_kx.at[r - 1], mate(r)) for r in (2, 1, 3)]

        def term(r, dy):
            return dv_ref.at[((place + r) % GROUP) * depth + dy]

        self.v_xx = [m.new(term(2, dy), self.in_v.at[0, dy], mate(3), asked(dy, 2), asked(dy, 3)) for dy in here]
        self.v_xu = [m.new(term(1, dy), self.in_v.at[1, dy], mate(1), asked(dy, 1), asked(dy, 0)) for dy in here]
        self.v_xd = [m.new(self.side_v.at[dy], self.in_v.at[2, dy], mate(3), asked(dy, 3), asked(dy, 0)) for dy in here]
        self.v_y = {dy: m.new(acc_v.at[dy], self.in_v1.at[dy - 1], earlier(dy),
                              both_of(asked(dy, 0), down(dy)), both_of(asked(dy, 0), up(dy))) for dy in here[1:]}
        self.order = [*here[2:], 1, 0]

    def start(self):
        m = self.m
        for dy in self.order:
            m.start(self.v_xx[dy])
            m.start(self.v_xu[dy])
        for i in (*self.k_yy.values(), *self.k_y.values()):
            m.start(i)

    def add(self, ref, at, buf, *slot):
        def act():
            ref[at] += buf[slot]
        return act

    def first_half(self):
        m, add = self.m, self.add
        for i in range(max(len(self.order), GROUP)):
            if i < len(self.order):
                dy = self.order[i]
                m.arrived(self.v_xx[dy], add(self.side_v, dy, self.in_v, 0, dy))
                m.start(self.v_xd[dy])
            if i < GROUP:
                if i in self.k_yy:
                    m.arrived(self.k_yy[i], add(self.near_k, i, self.in_k, i))
                m.start(self.k_y1[i])

    def second_half(self):
        m, add, acc_k, acc_v = self.m, self.add, self.acc_k, self.acc_v
        for i in range(max(len(self.order), GROUP)):
            if i < len(self.order):
                dy = self.order[i]
                m.arrived(self.v_xu[dy], add(acc_v, dy, self.in_v, 1, dy))
                m.arrived(self.v_xd[dy], add(acc_v, dy, self.in_v, 2, dy))
                if dy:
                    m.start(self.v_y[dy])
            if i < GROUP:
                for (dy, j), move in self.k_y.items():
                    if j == i:
                        m.arrived(move, add(acc_k, j, self.in_k3, dy - 3, j))
                m.arrived(self.k_y1[i], add(acc_k, i, self.in_k1, i))
        for i in self.k_x:
            m.start(i)
        for dy, move in self.v_y.items():
            m.arrived(move, add(acc_v, 0, self.in_v1, dy - 1))
        for i in self.k_x:
            m.arrived(i)
        return acc_k[self.place] + self.in_kx[0] + self.in_kx[1] + self.in_kx[2]


def scatter_bufs(width, tok, hd):
    rows = (width + 3) // GROUP
    more = max(rows - 2, 1)
    dma = pltpu.SemaphoreType.DMA
    shapes = [(GROUP,), (GROUP,), (GROUP,), (more, GROUP), (3,), (rows + 1,), (3, rows + 1), (rows,)]
    return [pltpu.VMEM((*shape, tok, hd), F32) for shape in shapes] + [dma((8 * rows + 16,)), dma((8 * rows + 16,))]


def finish_kernel(n, reach, width, dk_ref, dv_ref, o, dq, wq, wk, wv, wo_ref, y_ref, dx_ref,
                  acc_k, acc_v, wo, wo_sem, y_give, dx_give, dx_part, swap_send, swap_recv, *win):
    me = lax.axis_index('cp')
    core = me % 2
    partner = me + 1 - 2 * core
    blk = block_of(me, n)
    place = blk % GROUP
    base = blk - place
    tok = y_ref.shape[0]
    half = tok // 2
    heads, d_model, hd = wq.shape
    rows = (width + 3) // GROUP
    depth = reach + 1
    mine = pl.ds(pl.multiple_of(core * half, half), half)
    load = pltpu.make_async_copy(wo_ref, wo, wo_sem)
    load.start()
    barrier = pltpu.get_barrier_semaphore()
    signal(barrier, partner)
    if reach:
        for r in range(1, GROUP):
            signal(barrier, dev_of(base + (place + r) % GROUP, n))
        column_signal(barrier, blk, n, rows)
        pl.semaphore_wait(barrier, GROUP + column_size(blk, n, rows))
        bufs, sems = win[:-2], win[-2:]
        scatter = Scatter(n, blk, reach, width, dk_ref, dv_ref, acc_k, acc_v, bufs, sems)
        scatter.start()
        scatter.side_v[...] = dv_ref[pl.ds(((place + 3) % GROUP) * depth, rows + 1)]
        scatter.near_k[...] = dk_ref[pl.ds(GROUP, GROUP)]
        acc_v[...] = dv_ref[pl.ds(place * depth, rows + 1)]
        acc_k[...] = dk_ref[pl.ds(0, GROUP)]
        scatter.first_half()
    else:
        pl.semaphore_wait(barrier, 1)
        acc_v[...], acc_k[...] = dv_ref[...], dk_ref[...]
    load.wait()
    o_cat = jnp.concatenate([o[pl.ds(h * tok, tok), :] for h in range(heads)], axis=1)
    y = dot(o_cat, wo[...]).astype(BF16)
    y_give[...] = y[half:]
    y_ref[mine, :] = y[:half]
    dx = dot_nt(dq[pl.ds(0, tok), :], wq[0])
    for h in range(1, heads):
        dx += dot_nt(dq[pl.ds(h * tok, tok), :], wq[h])
    dx_part[...] = dx
    swap_y = remote(y_give, y_ref.at[mine], swap_send.at[0], swap_recv.at[0], partner)
    swap_y.start()
    total_k = scatter.second_half() if reach else acc_k[0]
    dk = total_k.astype(BF16)
    dv = acc_v[0].astype(BF16)

    def dx_rows(lo):
        part = slice(lo, lo + half)
        return (dx_part[pl.ds(lo, half), :] + dot_nt(dk[part], wk[...]) + dot_nt(dv[part], wv[...])).astype(BF16)

    dx_give[...] = dx_rows(half)
    dx_ref[mine, :] = dx_rows(0)
    swap_dx = remote(dx_give, dx_ref.at[mine], swap_send.at[1], swap_recv.at[1], partner)
    swap_dx.start()
    if reach:
        scatter.m.sent()
    swap_y.wait()
    swap_dx.wait()


def copy_kernel(y_ref, dx_ref, y_out, dx_out, sem):
    copies = [pltpu.make_async_copy(y_ref, y_out, sem.at[0]), pltpu.make_async_copy(dx_ref, dx_out, sem.at[1])]
    for c in copies:
        c.start()
    for c in copies:
        c.wait()


def make_layer(n, widths, far):
    dma = pltpu.SemaphoreType.DMA
    near = widths[-1]

    def comm(cid, mib=28):
        return pltpu.CompilerParams(collective_id=cid, has_side_effects=True, vmem_limit_bytes=mib * MIB)

    def local_layer(x_in, dy_in, doc_id, w_q, w_k, w_v, w_o):
        tok, d_model = x_in.shape
        heads, hd = w_q.shape[1], w_q.shape[2]
        cols = heads * tok
        me = lax.axis_index('cp')
        blk = block_of(me, n)
        place = blk % GROUP
        wq = jnp.transpose(w_q, (1, 0, 2))
        wk = w_k.reshape(d_model, hd)
        wv = w_v.reshape(d_model, hd)
        wo = w_o.reshape(heads * hd, d_model)
        n_stage = len(stages_of(n))
        reach = (near + 3) // GROUP

        def window(reach, dtype=BF16):
            return jax.ShapeDtypeStruct((GROUP * (reach + 1), tok, hd), dtype)

        q, do, k_win, v_win, rel, nd, which = pl.pallas_call(
            functools.partial(project_kernel, n, reach, (*widths, far)),
            out_shape=(jax.ShapeDtypeStruct((heads, tok, hd), BF16), jax.ShapeDtypeStruct((heads, tok, hd), BF16),
                       window(reach), window(reach), jax.ShapeDtypeStruct((1, cols), jnp.int32),
                       jax.ShapeDtypeStruct((2,), jnp.int32), jax.ShapeDtypeStruct((1,), jnp.int32)),
            in_specs=[HBM, HBM, VMEM, HBM, HBM, HBM, HBM],
            out_specs=(VMEM, VMEM, VMEM, VMEM, VMEM, SMEM, SMEM),
            scratch_shapes=[pltpu.VMEM((tok, d_model), BF16), pltpu.VMEM((tok, d_model), BF16),
                            pltpu.VMEM(wq.shape, BF16), pltpu.VMEM(wk.shape, BF16), pltpu.VMEM(wv.shape, BF16),
                            pltpu.VMEM(wo.shape, BF16), pltpu.VMEM((2, tok, hd), BF16),
                            pltpu.VMEM((heads, tok, hd), BF16), pltpu.VMEM((heads, tok, hd), BF16),
                            pltpu.VMEM((n, 1, 128), jnp.int32), dma((6,)), dma((4,)), dma((4,)), dma((8 * n_stage,)), dma((8 * n_stage,))] + gather_sems(reach),
            compiler_params=comm(0, 60),
            name='project',
        )(x_in, dy_in, doc_id.reshape(1, tok), wq, wk, wv, wo)
        q, do = q.reshape(cols, hd), do.reshape(cols, hd)

        def attend(k, v, width, reach):
            saved = [pltpu.VMEM((tok, cols), BF16)]
            if width:
                saved = [pltpu.VMEM(((width + 1) * tok, cols), F32), pltpu.VMEM(((width + 1) * tok, cols), BF16)]
            row = pltpu.VMEM((1, cols), F32)
            return pl.pallas_call(
                functools.partial(attend_kernel, reach, bool(width)),
                out_shape=(jax.ShapeDtypeStruct((cols, hd), BF16), jax.ShapeDtypeStruct((cols, hd), BF16),
                           jax.ShapeDtypeStruct(k.shape, F32), jax.ShapeDtypeStruct(k.shape, F32)),
                in_specs=[SMEM, VMEM, VMEM, VMEM, ANY, ANY],
                out_specs=(VMEM, VMEM, VMEM, VMEM),
                scratch_shapes=[pltpu.VMEM(k.shape, BF16), pltpu.VMEM(k.shape, BF16), dma((2,)),
                                pltpu.VMEM((hd, cols), BF16), pltpu.VMEM((hd, cols), BF16),
                                pltpu.VMEM((hd, cols), F32), pltpu.VMEM((hd, cols), F32), pltpu.VMEM((tok, cols), BF16),
                                row, row, row] + saved,
                compiler_params=pltpu.CompilerParams(vmem_limit_bytes=(36 if width == near else 60) * MIB),
                name='attend',
            )(nd, rel, q, do, k, v)

        def finish(dk, dv, o, dq, reach, width, cid):
            rows = (width + 3) // GROUP
            win = scatter_bufs(width, tok, hd) if reach else []
            results = pl.pallas_call(
                functools.partial(finish_kernel, n, reach, width),
                out_shape=(jax.ShapeDtypeStruct((tok, d_model), BF16), jax.ShapeDtypeStruct((tok, d_model), BF16)),
                in_specs=[VMEM] * 7 + [ANY],
                out_specs=(VMEM, VMEM),
                scratch_shapes=[pltpu.VMEM((4 if reach else 1, tok, hd), F32), pltpu.VMEM((rows + 1, tok, hd), F32),
                                pltpu.VMEM(wo.shape, BF16), dma, pltpu.VMEM((tok // 2, d_model), BF16), pltpu.VMEM((tok // 2, d_model), BF16),
                                pltpu.VMEM((tok, d_model), F32), dma((2,)), dma((2,))] + win,
                compiler_params=comm(cid, 60 if width == far else 28),
                name='finish',
            )(dk, dv, o, dq, wq, wk, wv, wo)
            return pl.pallas_call(
                copy_kernel, out_shape=(jax.ShapeDtypeStruct((tok, d_model), BF16),) * 2,
                in_specs=[VMEM] * 2, out_specs=(ANY, ANY), scratch_shapes=[dma((2,))],
                compiler_params=pltpu.CompilerParams(vmem_limit_bytes=4 * MIB), name='copy')(*results)

        def with_near(width, cid):
            def run(k, v):
                o, dq, dk, dv = attend(k, v, near, reach)
                return finish(dk, dv, o, dq, reach, width, cid)
            return run

        def own(k, v):
            return (lax.dynamic_index_in_dim(k, place, 0, keepdims=False),
                    lax.dynamic_index_in_dim(v, place * (reach + 1), 0, keepdims=False))

        def with_far(k, v):
            reach = (far + 3) // GROUP
            k, v = pl.pallas_call(
                functools.partial(gather_kernel, n, reach),
                out_shape=(window(reach), window(reach)),
                in_specs=[ANY, ANY], out_specs=(ANY, ANY),
                scratch_shapes=[dma((2,))] + gather_sems(reach),
                compiler_params=comm(1),
                name='gather',
            )(*own(k, v))
            o, dq, dk, dv = attend(k, v, far, reach)
            return finish(dk, dv, o, dq, reach, far, 2)

        order = [2 * b if b < n // 2 else 2 * (n - 1 - b) + 1 for b in range(n)]
        up = [(order[b], order[(b + 1) % n]) for b in range(n)]
        down = [(dst, src) for src, dst in up]

        def with_all(k, v):
            def pull(d, state):
                held, k, v = state
                held = lax.ppermute(held, 'cp', up)
                return held, k.at[d].set(held[0]), v.at[d].set(held[1])

            held = jnp.stack(own(k, v))
            empty = jnp.zeros((n, tok, hd), BF16)
            _, k, v = lax.fori_loop(1, n, pull, (held, empty.at[0].set(held[0]), empty.at[0].set(held[1])))
            o, dq, dk, dv = attend(k, v, 0, 0)

            def push(step, acc):
                d = n - 1 - step
                acc = acc + jnp.stack([lax.dynamic_index_in_dim(dk, d, 0, keepdims=False),
                                       lax.dynamic_index_in_dim(dv, d, 0, keepdims=False)])
                return lax.ppermute(acc, 'cp', down)

            acc = lax.fori_loop(0, n - 1, push, jnp.zeros((2, tok, hd), F32))
            return finish((acc[0] + dk[0])[None], (acc[1] + dv[0])[None], o, dq, 0, 0, 3)

        branches = [with_near(w, 4 + i) for i, w in enumerate(widths)] + [with_far, with_all]
        return lax.switch(which[0], branches, k_win, v_win)

    return local_layer


def solution(mesh, widths=WIDTHS, far=FAR):
    n = mesh.shape['cp']
    row_spec = P(('dp', 'cp'))
    full_spec = P()
    return jax.shard_map(make_layer(n, widths, far), mesh=mesh,
                         in_specs=(row_spec, row_spec, row_spec, full_spec, full_spec, full_spec, full_spec),
                         out_specs=(row_spec, row_spec), check_vma=False)
```

```python
import functools

import jax
import jax.numpy as jnp
from jax import lax
from jax.experimental import pallas as pl
from jax.experimental.pallas import tpu as pltpu
from jax.sharding import PartitionSpec as P

NEG_BIG = -1.0e30
GROUP = 4
MESH = pl.DeviceIdType.MESH
WIDTHS, FAR, CHUNK = (8, 9, 10, 12), 24, 256
LOG2_E = 1.4426950408889634
F32, BF16 = jnp.float32, jnp.bfloat16
ANY = pl.BlockSpec(memory_space=pl.ANY)
HBM = pl.BlockSpec(memory_space=pltpu.HBM)
VMEM = pl.BlockSpec(memory_space=pltpu.VMEM)
SMEM = pl.BlockSpec(memory_space=pltpu.SMEM)
MIB = 1 << 20


def dot(a, b):
    return jnp.dot(a, b, preferred_element_type=F32)


def dot_nt(a, b):
    return lax.dot_general(a, b, (((1,), (1,)), ((), ())), preferred_element_type=F32)


def dot_tn(a, b):
    return lax.dot_general(a, b, (((0,), (0,)), ((), ())), preferred_element_type=F32)


def block_of(dev, n):
    return jnp.where(dev % 2 == 0, dev // 2, n - 1 - dev // 2)


def dev_of(blk, n):
    return jnp.where(blk < n // 2, 2 * blk, 2 * (n - 1 - blk) + 1)


def at(dev):
    return (lax.axis_index('dp'), dev)


def stages_of(n):
    out, stride = [(1, min(n, 8))], min(n, 8)
    while stride < n:
        size = min(4, n // stride)
        out.append((stride, size))
        stride *= size
    return out


def peer_of(me, stride, size, j):
    idx = (me // stride) % size
    return me - idx * stride + ((idx + j) % size) * stride


def remote(src, dst, send, recv, dev):
    return pltpu.make_async_remote_copy(src_ref=src, dst_ref=dst, send_sem=send, recv_sem=recv,
                                        device_id=at(dev), device_id_type=MESH)


def column(blk, n, reach):
    out = []
    for dy in range(1, reach + 1):
        out.append((blk - GROUP * dy, blk - GROUP * dy >= 0))
        out.append((blk + GROUP * dy, blk + GROUP * dy < n))
    return out


def signal(barrier, dev):
    pl.semaphore_signal(barrier, inc=1, device_id=at(dev), device_id_type=MESH)


def column_signal(barrier, blk, n, reach):
    for other, there in column(blk, n, reach):
        @pl.when(there)
        def _():
            signal(barrier, dev_of(other, n))


def column_size(blk, n, reach):
    return jnp.minimum((n - 1 - blk) // GROUP, reach) + jnp.minimum(blk // GROUP, reach)


class Moves:
    def __init__(self, send, recv):
        self.sems, self.copies = (send, recv), []

    def new(self, src, dst, dev, go=None, come=None):
        i = len(self.copies)
        self.copies.append((remote(src, dst, self.sems[0].at[i], self.sems[1].at[i], dev), go, come))
        return i

    def when(self, cond, act):
        if cond is None:
            act()
        else:
            pl.when(cond)(act)

    def start(self, i):
        copy, go, _ = self.copies[i]
        self.when(go, copy.start)

    def arrived(self, i, then=None):
        copy, _, come = self.copies[i]

        def act():
            copy.wait_recv()
            if then is not None:
                then()
        self.when(come, act)

    def sent(self):
        for copy, go, _ in self.copies:
            self.when(go, copy.wait_send)


class Gather:
    def __init__(self, n, blk, reach, k_ref, v_ref, send, recv):
        place = blk % GROUP
        base = blk - place
        depth = reach + 1
        self.m = m = Moves(send, recv)

        def mate(r):
            return dev_of(base + (place + r) % GROUP, n)

        def later(dy):
            return dev_of(jnp.minimum(blk + GROUP * dy, n - 1), n)

        def k_at(dy, r):
            return k_ref.at[GROUP * dy + (place + r) % GROUP]

        def v_at(r, dy):
            return v_ref.at[((place + r) % GROUP) * depth + dy]

        def up(dy):
            return blk + GROUP * dy < n

        def down(dy):
            return blk - GROUP * dy >= 0

        both = up(1) & down(1)
        mid = down(2)
        self.straight = [dy for dy in range(1, reach + 1) if dy != 2]
        self.k_x = {r: m.new(k_at(0, 0), k_at(0, 0), mate(r)) for r in (1, 3, 2)}
        self.k_y = {(dy, r): m.new(k_at(0, r), k_at(dy, r), later(dy), up(dy), down(dy)) for dy in self.straight for r in range(GROUP)}
        self.v_y = {dy: m.new(v_at(0, 0), v_at(0, dy), later(dy), up(dy), down(dy)) for dy in (*self.straight, *range(2, min(reach, 2) + 1))}
        rows = [(0, None)] + [(dy, down(dy)) for dy in range(1, reach + 1)]
        self.v_x = {(dy, r): m.new(v_at(0, dy), v_at(0, dy), mate(r), c, c) for dy, c in rows for r in (1, 3)}
        self.v_xx = {dy: m.new(v_at(0, 2), v_at(0, 2), mate(2), c, c) if dy == 2 else
                     m.new(v_at(3, dy), v_at(3, dy), mate(1), c, c) for dy, c in rows}
        if reach > 1:
            self.k_yy = {r: m.new(k_at(0, 2), k_at(2, 2), later(2), up(2), mid) if r == 2 else
                         m.new(k_at(1, r), k_at(2, r), later(1), both, mid) for r in range(GROUP)}
        self.reach = reach

    def own(self):
        m = self.m
        for i in self.k_x.values():
            m.start(i)
        self.k_on(0)
        for i in self.v_y.values():
            m.start(i)
        self.v_on(0)

    def k_on(self, r):
        for dy in self.straight:
            self.m.start(self.k_y[dy, r])
        if r == 2 and self.reach > 1:
            self.m.start(self.k_yy[r])

    def v_on(self, dy):
        for r in (1, 3):
            self.m.start(self.v_x[dy, r])
        if dy == 2:
            self.m.start(self.v_xx[dy])

    def hand_on(self):
        m = self.m
        m.arrived(self.k_x[1])
        self.k_on(3)
        m.arrived(self.v_y[1])
        self.v_on(1)
        m.arrived(self.k_x[3])
        self.k_on(1)
        for dy in self.straight[1:]:
            m.arrived(self.v_y[dy])
            self.v_on(dy)
        m.arrived(self.v_x[0, 1])
        m.start(self.v_xx[0])
        m.arrived(self.k_y[1, 0])
        if self.reach > 1:
            m.start(self.k_yy[0])
        m.arrived(self.k_x[2])
        self.k_on(2)
        if self.reach > 1:
            m.arrived(self.v_y[2])
            self.v_on(2)

    def rest(self):
        m = self.m
        order = [1] + self.straight[1:] + ([2] if self.reach > 1 else [])
        for i in range(max(len(order), 3)):
            if i < len(order):
                m.arrived(self.v_x[order[i], 1])
                if order[i] != 2:
                    m.start(self.v_xx[order[i]])
            if i < 3:
                r = (3, 1, 2)[i]
                m.arrived(self.k_y[1, r])
                if self.reach > 1 and r != 2:
                    m.start(self.k_yy[r])

    def finish(self):
        m = self.m
        for dy in self.straight[1:]:
            for r in range(GROUP):
                m.arrived(self.k_y[dy, r])
        for dy in range(self.reach + 1):
            m.arrived(self.v_x[dy, 3])
            m.arrived(self.v_xx[dy])
        if self.reach > 1:
            for r in range(GROUP):
                m.arrived(self.k_yy[r])
        m.sent()


def gather_sems(reach):
    dma = pltpu.SemaphoreType.DMA
    return [dma((9 * reach + 12,)), dma((9 * reach + 12,))]


def place_documents(tab_ref, doc_ref, me):
    docs, tok = tab_ref.shape[-1], doc_ref.shape[-1]
    earlier = doc_ref[...] < lax.broadcasted_iota(jnp.int32, (docs, tok), 0)
    count = dot_nt(jnp.ones((8, tok), BF16), jnp.where(earlier, 1.0, 0.0).astype(BF16))
    tab_ref[me] = count[:1].astype(jnp.int32)


def find_documents(tab_ref, rel_ref, near_ref, which_ref, blk, tok, limits):
    n, _, docs = tab_ref.shape
    starts = jnp.sum(tab_ref[...], axis=0).astype(F32)
    lane = lax.broadcasted_iota(jnp.int32, (1, docs), 1)
    ends = jnp.where(lane == docs - 1, float(n * tok), pltpu.roll(starts, docs - 1, 1))

    def block(pos):
        return jnp.floor((pos + 0.5) * (1.0 / tok))

    span = jnp.max(jnp.where(ends > starts, block(ends - 1.0) - block(starts), 0.0)).astype(jnp.int32)
    which = jnp.int32(0)
    for w in limits:
        which = which + jnp.where(span > w, 1, 0)
    which_ref[0] = which
    cols = rel_ref.shape[1]
    pos = (lax.broadcasted_iota(jnp.int32, (1, cols), 1) % tok + blk * tok).astype(F32)
    column = jnp.broadcast_to(starts, (docs, docs)).T[:, :1]
    first = jnp.max(jnp.where(column <= pos, column, 0.0), axis=0, keepdims=True)
    rel_ref[...] = first.astype(jnp.int32) - blk * tok
    near_ref[0] = blk - block(jnp.min(first)).astype(jnp.int32)
    near_ref[1] = blk % GROUP


def project_kernel(n, reach, limits, x_ref, dy_ref, doc_ref, wq_ref, wk_ref, wv_ref, wo_ref,
                   q_ref, do_ref, k_ref, v_ref, rel_ref, near_ref, which_ref,
                   xs, dys, wq, wk, wv, wo, own_kv, own_q, own_do, tab_ref, loc_sem, swap_send, swap_recv,
                   tab_send, tab_recv, *win):
    me = lax.axis_index('cp')
    core = me % 2
    partner = me + 1 - 2 * core
    blk = block_of(me, n)
    place = blk % GROUP
    tok = x_ref.shape[0]
    half = tok // 2
    heads, _, hd = wq_ref.shape
    depth = reach + 1
    keep = pl.ds(pl.multiple_of(core * half, half), half)
    give = pl.ds(pl.multiple_of((1 - core) * half, half), half)
    front, back = pl.ds(0, half), pl.ds(half, half)
    loads = [pltpu.make_async_copy(src, dst, loc_sem.at[i]) for i, (src, dst) in enumerate((
        (x_ref, xs), (wk_ref, wk), (wv_ref, wv), (wq_ref, wq), (dy_ref, dys), (wo_ref, wo)))]
    for c in loads:
        c.start()
    barrier = pltpu.get_barrier_semaphore()
    stages = stages_of(n)
    peers = 0
    for stride, size in stages:
        for j in range(1, size):
            signal(barrier, peer_of(me, stride, size, j))
            peers += 1
    column_signal(barrier, blk, n, reach)
    place_documents(tab_ref, doc_ref, me)

    def stage_copies(s):
        stride, size = stages[s]
        rows = pl.ds(me - me % stride, stride)
        return [remote(tab_ref.at[rows], tab_ref.at[rows], tab_send.at[8 * s + j], tab_recv.at[8 * s + j],
                       peer_of(me, stride, size, j)) for j in range(1, size)]

    def q_heads(some):
        for h in some:
            own_q[h] = dot(xs[...], wq[h]).astype(BF16)
            q_ref[h, front, :] = own_q[h, keep, :]

    tables = [stage_copies(s) for s in range(len(stages))]
    other = GROUP - 1 - place
    swaps = [remote(src, dst, swap_send.at[i], swap_recv.at[i], partner) for i, (src, dst) in enumerate((
        (own_kv.at[0, give], k_ref.at[other, back]), (own_kv.at[1, give], v_ref.at[other * depth, back]),
        (own_q.at[:, give], q_ref.at[:, back]), (own_do.at[:, give], do_ref.at[:, back])))]
    gather = Gather(n, blk, reach, k_ref, v_ref, *win)

    def next_table(s):
        if s < len(stages):
            for c in tables[s - 1]:
                c.wait()
            for c in tables[s]:
                c.start()

    for c in loads[:3]:
        c.wait()
    own_kv[0] = dot(xs[...], wk[...]).astype(BF16)
    own_kv[1] = dot(xs[...], wv[...]).astype(BF16)
    k_ref[place, front, :] = own_kv[0, keep, :]
    v_ref[place * depth, front, :] = own_kv[1, keep, :]
    loads[3].wait()
    q_heads(range(1))
    pl.semaphore_wait(barrier, peers + column_size(blk, n, reach))
    for c in swaps[:2] + tables[0]:
        c.start()
    q_heads(range(1, heads))
    for c in swaps[:2]:
        c.wait_recv()
    gather.own()
    loads[4].wait()
    loads[5].wait()
    for h in range(heads):
        own_do[h] = dot_nt(dys[...], wo[pl.ds(h * hd, hd), :]).astype(BF16)
        do_ref[h, front, :] = own_do[h, keep, :]
    swaps[2].start()
    next_table(1)
    gather.hand_on()
    swaps[3].start()
    next_table(2)
    gather.rest()
    for c in tables[-1]:
        c.wait()
    find_documents(tab_ref, rel_ref, near_ref, which_ref, blk, tok, limits)
    gather.finish()
    for c in swaps[2:]:
        c.wait_recv()
    for c in swaps:
        c.wait_send()


def gather_kernel(n, reach, k_own_ref, v_own_ref, k_ref, v_ref, loc_sem, *win):
    me = lax.axis_index('cp')
    blk = block_of(me, n)
    place = blk % GROUP
    own = [pltpu.make_async_copy(k_own_ref, k_ref.at[place], loc_sem.at[0]),
           pltpu.make_async_copy(v_own_ref, v_ref.at[place * (reach + 1)], loc_sem.at[1])]
    for c in own:
        c.start()
    barrier = pltpu.get_barrier_semaphore()
    for m in range(1, GROUP):
        signal(barrier, dev_of(blk - place + (place + m) % GROUP, n))
    column_signal(barrier, blk, n, reach)
    pl.semaphore_wait(barrier, 3 + column_size(blk, n, reach))
    for c in own:
        c.wait()
    gather = Gather(n, blk, reach, k_ref, v_ref, *win)
    gather.own()
    gather.hand_on()
    gather.rest()
    gather.finish()


def attend_kernel(reach, keep, nd_ref, start_ref, q_ref, do_ref, k_ref, v_ref, o_ref, dq_ref, dk_ref, dv_ref,
                  q_t, do_t, o_t, dq_t, ds_t, top, tot, delta, *saved):
    nd = nd_ref[0]
    place = nd_ref[1]
    slots, tok, hd = k_ref.shape
    cols = q_ref.shape[0]
    scale = hd ** -0.5
    base2 = scale * LOG2_E

    def slots_of(d):
        if not reach:
            return d, d
        back = (d + GROUP - 1 - place) // GROUP
        spot = place - d + GROUP * back
        return GROUP * back + spot, spot * (reach + 1) + back

    def rows(d):
        return pl.ds(pl.multiple_of(d * tok, tok), tok)

    def clear(i, _):
        if reach:
            d = place + GROUP * (i // GROUP) - i % GROUP
            empty = (d < 0) | (d > nd)
            where = (i, (i % GROUP) * (reach + 1) + i // GROUP)
        else:
            empty, where = i > nd, (i, i)

        @pl.when(empty)
        def _():
            for ref, slot in zip((dk_ref, dv_ref), where):
                ref[slot] = jnp.zeros((tok, hd), F32)
        return 0

    lax.fori_loop(0, slots, clear, 0)
    q_t[...] = q_ref[...].T
    do_t[...] = do_ref[...].T
    top[...] = jnp.full_like(top, NEG_BIG)
    tot[...] = jnp.zeros_like(tot)
    o_t[...] = jnp.zeros_like(o_t)
    dq_t[...] = jnp.zeros_like(dq_t)

    def split(size):
        return [(lo, min(size, cols - lo)) for lo in range(0, cols, size)]

    def scores(k, d, lo, size, own):
        part = pl.ds(lo, size)
        s = dot(k, q_t[:, part])
        u = lax.broadcasted_iota(jnp.int32, (tok, size), 0)
        visible = u >= start_ref[:, part] + d * tok
        if own:
            t = (lax.broadcasted_iota(jnp.int32, (1, size), 1) + lo) % tok
            visible = visible & (u <= t + d * tok)
        return jnp.where(visible, s, NEG_BIG)

    def weight(s, part):
        return jnp.exp2(s * base2 - top[:, part])

    def find_top(d, own):
        k = k_ref[slots_of(d)[0]]
        for lo, size in split(CHUNK):
            part = pl.ds(lo, size)
            s = scores(k, d, lo, size, own)
            top[:, part] = jnp.maximum(top[:, part], jnp.max(s, axis=0, keepdims=True))
            if keep:
                saved[0][rows(d), part] = s

    def find_total(d, own):
        k = None if keep else k_ref[slots_of(d)[0]]
        for lo, size in split(CHUNK):
            part = pl.ds(lo, size)
            e = weight(saved[0][rows(d), part] if keep else scores(k, d, lo, size, own), part)
            tot[:, part] += jnp.sum(e, axis=0, keepdims=True)
            if keep:
                saved[0][rows(d), part] = e

    def forward(d, own):
        vt = v_ref[slots_of(d)[1]].T
        k = None if keep else k_ref[slots_of(d)[0]]
        for lo, size in split(CHUNK):
            part = pl.ds(lo, size)
            e = saved[0][rows(d), part] if keep else weight(scores(k, d, lo, size, own), part)
            p = (e * tot[:, part]).astype(BF16)
            if keep:
                saved[1][rows(d), part] = p
            o_t[:, part] += dot(vt, p)

    def backward(d, own):
        at_k, at_v = slots_of(d)
        k, v = k_ref[at_k], v_ref[at_v]
        kt = k.T
        p_all = saved[1].at[rows(d)] if keep else saved[0]
        for lo, size in split(CHUNK):
            part = pl.ds(lo, size)
            if not keep:
                p_all[:, part] = (weight(scores(k, d, lo, size, own), part) * tot[:, part]).astype(BF16)
            dp = dot(v, do_t[:, part])
            ds_t[:, part] = (p_all[:, part].astype(F32) * (dp - delta[:, part])).astype(BF16)
        dq_t[...] += dot(kt, ds_t[...])
        dk_ref[at_k] = dot(ds_t[...], q_ref[...]) * scale
        dv_ref[at_v] = dot(p_all[...], do_ref[...])

    def over_blocks(step, first):
        def body(d, _):
            step(d, not first)
            return 0

        if first:
            step(0, True)
        lax.fori_loop(int(first), nd + 1, body, 0)

    over_blocks(find_top, keep)
    top[...] = top[...] * base2
    over_blocks(find_total, False)
    tot[...] = 1.0 / tot[...]
    over_blocks(forward, False)
    o_bf = o_t[...].astype(BF16)
    delta[...] = jnp.sum(o_bf.astype(F32) * do_t[...].astype(F32), axis=0, keepdims=True)
    o_ref[...] = o_bf.T
    over_blocks(backward, False)
    dq_ref[...] = (dq_t[...] * scale).astype(BF16).T


class Scatter:
    def __init__(self, n, blk, reach, width, dk_ref, dv_ref, acc_k, acc_v, bufs, sems):
        place = blk % GROUP
        base = blk - place
        depth = reach + 1
        self.place, self.acc_k, self.acc_v = place, acc_k, acc_v
        self.rows = rows = (width + 3) // GROUP
        self.near_k, self.in_k, self.in_k1, self.in_k3, self.in_kx, self.side_v, self.in_v, self.in_v1 = bufs
        self.m = m = Moves(*sems)

        def mate(r):
            return dev_of(base + (place + r) % GROUP, n)

        def earlier(dy):
            return dev_of(jnp.maximum(blk - GROUP * dy, 0), n)

        def down(dy):
            return blk - GROUP * dy >= 0

        def up(dy):
            return blk + GROUP * dy < n

        def need(dy, place):
            return GROUP * dy - width <= place

        def both_of(a, b):
            return b if a is None else a & b

        def asked(dy, r):
            return None if need(dy, 0) else need(dy, (place + r) % GROUP)

        both = up(1) & down(1)
        here, there = range(rows + 1), [(dy, j) for dy in range(3, rows + 1) for j in range(GROUP) if need(dy, j)]
        self.k_yy = {j: m.new(dk_ref.at[2 * GROUP + j], self.in_k.at[j], earlier(1), down(2), both)
                     for j in range(GROUP) if rows > 1 and need(2, j)}
        self.k_y = {(dy, j): m.new(dk_ref.at[GROUP * dy + j], self.in_k3.at[dy - 3, j], earlier(dy), down(dy), up(dy))
                    for dy, j in there}
        self.k_y1 = [m.new(self.near_k.at[j], self.in_k1.at[j], earlier(1), down(1), up(1)) for j in range(GROUP)]
        self.k_x = [m.new(acc_k.at[(place + r) % GROUP], self.in_kx.at[r - 1], mate(r)) for r in (2, 1, 3)]

        def term(r, dy):
            return dv_ref.at[((place + r) % GROUP) * depth + dy]

        self.v_xx = [m.new(term(2, dy), self.in_v.at[0, dy], mate(3), asked(dy, 2), asked(dy, 3)) for dy in here]
        self.v_xu = [m.new(term(1, dy), self.in_v.at[1, dy], mate(1), asked(dy, 1), asked(dy, 0)) for dy in here]
        self.v_xd = [m.new(self.side_v.at[dy], self.in_v.at[2, dy], mate(3), asked(dy, 3), asked(dy, 0)) for dy in here]
        self.v_y = {dy: m.new(acc_v.at[dy], self.in_v1.at[dy - 1], earlier(dy),
                              both_of(asked(dy, 0), down(dy)), both_of(asked(dy, 0), up(dy))) for dy in here[1:]}
        self.order = [*here[2:], 1, 0]

    def start(self):
        m = self.m
        for dy in self.order:
            m.start(self.v_xx[dy])
            m.start(self.v_xu[dy])
        for i in (*self.k_yy.values(), *self.k_y.values()):
            m.start(i)

    def add(self, ref, at, buf, *slot):
        def act():
            ref[at] += buf[slot]
        return act

    def first_half(self):
        m, add = self.m, self.add
        for i in range(max(len(self.order), GROUP)):
            if i < len(self.order):
                dy = self.order[i]
                m.arrived(self.v_xx[dy], add(self.side_v, dy, self.in_v, 0, dy))
                m.start(self.v_xd[dy])
            if i < GROUP:
                if i in self.k_yy:
                    m.arrived(self.k_yy[i], add(self.near_k, i, self.in_k, i))
                m.start(self.k_y1[i])

    def second_half(self):
        m, add, acc_k, acc_v = self.m, self.add, self.acc_k, self.acc_v
        for i in range(max(len(self.order), GROUP)):
            if i < len(self.order):
                dy = self.order[i]
                m.arrived(self.v_xu[dy], add(acc_v, dy, self.in_v, 1, dy))
                m.arrived(self.v_xd[dy], add(acc_v, dy, self.in_v, 2, dy))
                if dy:
                    m.start(self.v_y[dy])
            if i < GROUP:
                for (dy, j), move in self.k_y.items():
                    if j == i:
                        m.arrived(move, add(acc_k, j, self.in_k3, dy - 3, j))
                m.arrived(self.k_y1[i], add(acc_k, i, self.in_k1, i))
        for i in self.k_x:
            m.start(i)
        for dy, move in self.v_y.items():
            m.arrived(move, add(acc_v, 0, self.in_v1, dy - 1))
        for i in self.k_x:
            m.arrived(i)
        return acc_k[self.place] + self.in_kx[0] + self.in_kx[1] + self.in_kx[2]


def scatter_bufs(width, tok, hd):
    rows = (width + 3) // GROUP
    more = max(rows - 2, 1)
    dma = pltpu.SemaphoreType.DMA
    shapes = [(GROUP,), (GROUP,), (GROUP,), (more, GROUP), (3,), (rows + 1,), (3, rows + 1), (rows,)]
    return [pltpu.VMEM((*shape, tok, hd), F32) for shape in shapes] + [dma((8 * rows + 16,)), dma((8 * rows + 16,))]


def finish_kernel(n, reach, width, dk_ref, dv_ref, o, dq, wq, wk, wv, wo_ref, y_ref, dx_ref,
                  acc_k, acc_v, wo, wo_sem, y_give, dx_give, dx_part, swap_send, swap_recv, *win):
    me = lax.axis_index('cp')
    core = me % 2
    partner = me + 1 - 2 * core
    blk = block_of(me, n)
    place = blk % GROUP
    base = blk - place
    tok = y_ref.shape[0]
    half = tok // 2
    heads, d_model, hd = wq.shape
    rows = (width + 3) // GROUP
    depth = reach + 1
    mine = pl.ds(pl.multiple_of(core * half, half), half)
    load = pltpu.make_async_copy(wo_ref, wo, wo_sem)
    load.start()
    barrier = pltpu.get_barrier_semaphore()
    signal(barrier, partner)
    if reach:
        for r in range(1, GROUP):
            signal(barrier, dev_of(base + (place + r) % GROUP, n))
        column_signal(barrier, blk, n, rows)
        pl.semaphore_wait(barrier, GROUP + column_size(blk, n, rows))
        bufs, sems = win[:-2], win[-2:]
        scatter = Scatter(n, blk, reach, width, dk_ref, dv_ref, acc_k, acc_v, bufs, sems)
        scatter.start()
        scatter.side_v[...] = dv_ref[pl.ds(((place + 3) % GROUP) * depth, rows + 1)]
        scatter.near_k[...] = dk_ref[pl.ds(GROUP, GROUP)]
        scatter.first_half()
        acc_v[...] = dv_ref[pl.ds(place * depth, rows + 1)]
        acc_k[...] = dk_ref[pl.ds(0, GROUP)]
    else:
        pl.semaphore_wait(barrier, 1)
        acc_v[...], acc_k[...] = dv_ref[...], dk_ref[...]
    load.wait()
    o_cat = jnp.concatenate([o[pl.ds(h * tok, tok), :] for h in range(heads)], axis=1)
    y = dot(o_cat, wo[...]).astype(BF16)
    y_give[...] = y[half:]
    y_ref[mine, :] = y[:half]
    dx = dot_nt(dq[pl.ds(0, tok), :], wq[0])
    for h in range(1, heads):
        dx += dot_nt(dq[pl.ds(h * tok, tok), :], wq[h])
    dx_part[...] = dx
    swap_y = remote(y_give, y_ref.at[mine], swap_send.at[0], swap_recv.at[0], partner)
    swap_y.start()
    total_k = scatter.second_half() if reach else acc_k[0]
    dk = total_k.astype(BF16)
    dv = acc_v[0].astype(BF16)

    def dx_rows(lo):
        part = slice(lo, lo + half)
        return (dx_part[pl.ds(lo, half), :] + dot_nt(dk[part], wk[...]) + dot_nt(dv[part], wv[...])).astype(BF16)

    dx_give[...] = dx_rows(half)
    dx_ref[mine, :] = dx_rows(0)
    swap_dx = remote(dx_give, dx_ref.at[mine], swap_send.at[1], swap_recv.at[1], partner)
    swap_dx.start()
    if reach:
        scatter.m.sent()
    swap_y.wait()
    swap_dx.wait()


def copy_kernel(y_ref, dx_ref, y_out, dx_out, sem):
    copies = [pltpu.make_async_copy(y_ref, y_out, sem.at[0]), pltpu.make_async_copy(dx_ref, dx_out, sem.at[1])]
    for c in copies:
        c.start()
    for c in copies:
        c.wait()


def make_layer(n, widths, far):
    dma = pltpu.SemaphoreType.DMA
    near = widths[-1]

    def comm(cid, mib=28):
        return pltpu.CompilerParams(collective_id=cid, has_side_effects=True, vmem_limit_bytes=mib * MIB)

    def local_layer(x_in, dy_in, doc_id, w_q, w_k, w_v, w_o):
        tok, d_model = x_in.shape
        heads, hd = w_q.shape[1], w_q.shape[2]
        cols = heads * tok
        me = lax.axis_index('cp')
        blk = block_of(me, n)
        place = blk % GROUP
        wq = jnp.transpose(w_q, (1, 0, 2))
        wk = w_k.reshape(d_model, hd)
        wv = w_v.reshape(d_model, hd)
        wo = w_o.reshape(heads * hd, d_model)
        n_stage = len(stages_of(n))
        reach = (near + 3) // GROUP

        def window(reach, dtype=BF16):
            return jax.ShapeDtypeStruct((GROUP * (reach + 1), tok, hd), dtype)

        q, do, k_win, v_win, rel, nd, which = pl.pallas_call(
            functools.partial(project_kernel, n, reach, (*widths, far)),
            out_shape=(jax.ShapeDtypeStruct((heads, tok, hd), BF16), jax.ShapeDtypeStruct((heads, tok, hd), BF16),
                       window(reach), window(reach), jax.ShapeDtypeStruct((1, cols), jnp.int32),
                       jax.ShapeDtypeStruct((2,), jnp.int32), jax.ShapeDtypeStruct((1,), jnp.int32)),
            in_specs=[HBM, HBM, VMEM, HBM, HBM, HBM, HBM],
            out_specs=(VMEM, VMEM, VMEM, VMEM, VMEM, SMEM, SMEM),
            scratch_shapes=[pltpu.VMEM((tok, d_model), BF16), pltpu.VMEM((tok, d_model), BF16),
                            pltpu.VMEM(wq.shape, BF16), pltpu.VMEM(wk.shape, BF16), pltpu.VMEM(wv.shape, BF16),
                            pltpu.VMEM(wo.shape, BF16), pltpu.VMEM((2, tok, hd), BF16),
                            pltpu.VMEM((heads, tok, hd), BF16), pltpu.VMEM((heads, tok, hd), BF16),
                            pltpu.VMEM((n, 1, 128), jnp.int32), dma((6,)), dma((4,)), dma((4,)), dma((8 * n_stage,)), dma((8 * n_stage,))] + gather_sems(reach),
            compiler_params=comm(0, 60),
            name='project',
        )(x_in, dy_in, doc_id.reshape(1, tok), wq, wk, wv, wo)
        q, do = q.reshape(cols, hd), do.reshape(cols, hd)

        def attend(k, v, width, reach):
            saved = [pltpu.VMEM((tok, cols), BF16)]
            if width:
                saved = [pltpu.VMEM(((width + 1) * tok, cols), F32), pltpu.VMEM(((width + 1) * tok, cols), BF16)]
            row = pltpu.VMEM((1, cols), F32)
            return pl.pallas_call(
                functools.partial(attend_kernel, reach, bool(width)),
                out_shape=(jax.ShapeDtypeStruct((cols, hd), BF16), jax.ShapeDtypeStruct((cols, hd), BF16),
                           jax.ShapeDtypeStruct(k.shape, F32), jax.ShapeDtypeStruct(k.shape, F32)),
                in_specs=[SMEM, VMEM, VMEM, VMEM, VMEM, VMEM],
                out_specs=(VMEM, VMEM, VMEM, VMEM),
                scratch_shapes=[pltpu.VMEM((hd, cols), BF16), pltpu.VMEM((hd, cols), BF16),
                                pltpu.VMEM((hd, cols), F32), pltpu.VMEM((hd, cols), F32), pltpu.VMEM((tok, cols), BF16),
                                row, row, row] + saved,
                compiler_params=pltpu.CompilerParams(vmem_limit_bytes=(36 if width == near else 60) * MIB),
                name='attend',
            )(nd, rel, q, do, k, v)

        def finish(dk, dv, o, dq, reach, width, cid):
            rows = (width + 3) // GROUP
            win = scatter_bufs(width, tok, hd) if reach else []
            results = pl.pallas_call(
                functools.partial(finish_kernel, n, reach, width),
                out_shape=(jax.ShapeDtypeStruct((tok, d_model), BF16), jax.ShapeDtypeStruct((tok, d_model), BF16)),
                in_specs=[VMEM] * 7 + [ANY],
                out_specs=(VMEM, VMEM),
                scratch_shapes=[pltpu.VMEM((4 if reach else 1, tok, hd), F32), pltpu.VMEM((rows + 1, tok, hd), F32),
                                pltpu.VMEM(wo.shape, BF16), dma, pltpu.VMEM((tok // 2, d_model), BF16), pltpu.VMEM((tok // 2, d_model), BF16),
                                pltpu.VMEM((tok, d_model), F32), dma((2,)), dma((2,))] + win,
                compiler_params=comm(cid, 60 if width == far else 28),
                name='finish',
            )(dk, dv, o, dq, wq, wk, wv, wo)
            return pl.pallas_call(
                copy_kernel, out_shape=(jax.ShapeDtypeStruct((tok, d_model), BF16),) * 2,
                in_specs=[VMEM] * 2, out_specs=(ANY, ANY), scratch_shapes=[dma((2,))],
                compiler_params=pltpu.CompilerParams(vmem_limit_bytes=4 * MIB), name='copy')(*results)

        def with_near(width, cid):
            def run(k, v):
                o, dq, dk, dv = attend(k, v, near, reach)
                return finish(dk, dv, o, dq, reach, width, cid)
            return run

        def own(k, v):
            return (lax.dynamic_index_in_dim(k, place, 0, keepdims=False),
                    lax.dynamic_index_in_dim(v, place * (reach + 1), 0, keepdims=False))

        def with_far(k, v):
            reach = (far + 3) // GROUP
            k, v = pl.pallas_call(
                functools.partial(gather_kernel, n, reach),
                out_shape=(window(reach), window(reach)),
                in_specs=[ANY, ANY], out_specs=(ANY, ANY),
                scratch_shapes=[dma((2,))] + gather_sems(reach),
                compiler_params=comm(1),
                name='gather',
            )(*own(k, v))
            o, dq, dk, dv = attend(k, v, far, reach)
            return finish(dk, dv, o, dq, reach, far, 2)

        order = [2 * b if b < n // 2 else 2 * (n - 1 - b) + 1 for b in range(n)]
        up = [(order[b], order[(b + 1) % n]) for b in range(n)]
        down = [(dst, src) for src, dst in up]

        def with_all(k, v):
            def pull(d, state):
                held, k, v = state
                held = lax.ppermute(held, 'cp', up)
                return held, k.at[d].set(held[0]), v.at[d].set(held[1])

            held = jnp.stack(own(k, v))
            empty = jnp.zeros((n, tok, hd), BF16)
            _, k, v = lax.fori_loop(1, n, pull, (held, empty.at[0].set(held[0]), empty.at[0].set(held[1])))
            o, dq, dk, dv = attend(k, v, 0, 0)

            def push(step, acc):
                d = n - 1 - step
                acc = acc + jnp.stack([lax.dynamic_index_in_dim(dk, d, 0, keepdims=False),
                                       lax.dynamic_index_in_dim(dv, d, 0, keepdims=False)])
                return lax.ppermute(acc, 'cp', down)

            acc = lax.fori_loop(0, n - 1, push, jnp.zeros((2, tok, hd), F32))
            return finish((acc[0] + dk[0])[None], (acc[1] + dv[0])[None], o, dq, 0, 0, 3)

        branches = [with_near(w, 4 + i) for i, w in enumerate(widths)] + [with_far, with_all]
        return lax.switch(which[0], branches, k_win, v_win)

    return local_layer


def solution(mesh, widths=WIDTHS, far=FAR):
    n = mesh.shape['cp']
    row_spec = P(('dp', 'cp'))
    full_spec = P()
    return jax.shard_map(make_layer(n, widths, far), mesh=mesh,
                         in_specs=(row_spec, row_spec, row_spec, full_spec, full_spec, full_spec, full_spec),
                         out_specs=(row_spec, row_spec), check_vma=False)
```
